32 devices in a mesh: gx: 2 (over y), gy: 4 (over x, core), gz: 4 (over z).
Axes of the slice: x: 2, y: 2, z: 4, core: 2. Of those that a mesh axis runs over, the one named last changes fastest.
Arguments:
- species: float32 [5, 8, 32, 512], P(None, 'gx', 'gy', 'gz'), may hold values from 0.09 to 0.6
- velocity_in: float32 [3, 8, 32, 512], P(None, 'gx', 'gy', 'gz'), may hold values from -3 to 3
- pressure_in: float32 [8, 32, 512], P('gx', 'gy', 'gz'), may hold values from 0.125 to 1
- wall_types: int32 [3, 2, 8, 128], P(None, 'gx', 'gy', 'gz'), may hold values 0 or 1
Outputs:
- new_state: float32 [9, 8, 32, 512], P(None, 'gx', 'gy', 'gz')
- blending: float32 [2, 8, 128], P('gx', 'gy', 'gz')
The draws below stay inside these ranges and needn't reach their ends.
All inputs are finite; a program needn't handle non-finite values. Where the reference program divides by a largest or mean magnitude, that divisor is 1e-20 or more. No bound on the sum of `wall_types` on one device may be relied on, other than what follows from the above.
Results may differ from the reference program's by a relative error of at most 0.0003.
Values sent between devices are 32-bit elements; how exact they have to be, the bound alone decides.
A program may use at most 64 MiB of HBM per device.

```python
import math
import jax
import jax.numpy as jnp
from jax import lax

SPECIES = 5
P_SIZE = 4
ITERS = 2
NX = 2
NY = 8
NZ = 128
MX = 8
MY = 32
MZ = 512


def element_factor(key, lowest):
    values = jax.random.uniform(key, (NX, NY, NZ), jnp.float32, math.log(lowest), 0.0)
    values = jnp.exp(values)
    values = jnp.repeat(values, P_SIZE, axis=0)
    values = jnp.repeat(values, P_SIZE, axis=1)
    return jnp.repeat(values, P_SIZE, axis=2)


def node_factor(key, shape, lowest, highest):
    logs = jax.random.uniform(key, shape, jnp.float32, math.log(lowest), math.log(highest))
    return jnp.exp(logs)


def draw_species(key, part):
    factor = element_factor(jax.random.fold_in(key, 11), 0.3)
    nodes = node_factor(jax.random.fold_in(key, 12), (SPECIES, MX, MY, MZ), 0.3, 0.6)
    return (nodes * factor[None]).astype(jnp.float32)


def draw_pressure_in(key, part):
    factor = element_factor(jax.random.fold_in(key, 21), 0.25)
    nodes = node_factor(jax.random.fold_in(key, 22), (MX, MY, MZ), 0.5, 1.0)
    return (nodes * factor).astype(jnp.float32)


def set_ends(drawn, own_key, least, largest):
    shape = drawn.shape
    place = [jax.random.randint(jax.random.fold_in(own_key, axis), (), 0, shape[axis]) for axis in range(len(shape))]
    drawn = drawn.at[tuple(place)].set(least)
    longest = shape.index(max(shape))
    place[longest] = (place[longest] + 1) % shape[longest]
    return drawn.at[tuple(place)].set(largest)


def levels(key, shape, pieces, least, high):
    def one(dim, blocks):
        heights = jax.random.uniform(jax.random.fold_in(jax.random.fold_in(key, 6), dim), (blocks,), jnp.float32, least / len(pieces), high / len(pieces))
        return jnp.repeat(jnp.exp(heights), shape[dim] // blocks).reshape((-1,) + (1,) * (len(shape) - dim - 1))

    gain = one(*pieces[0])
    for cut in pieces[1:]:
        gain = gain * one(*cut)
    return gain


def bell_draw(own_key, shape, deviation, limit, shards=(), held_as=jnp.bfloat16):
    entries = jax.random.normal(own_key, shape, jnp.float32) * deviation
    if len(shards) > 0:
        entries = levels(own_key, shape, shards, -0.22, 0.18) * entries
    return jnp.clip(entries, min=-limit, max=limit).astype(held_as)


def setup_inputs(seed: int = 0) -> dict:
    seeds = jax.random.split(jax.random.key(seed), 5)
    species = draw_species(jax.random.fold_in(seeds[4], 71), 0)
    velocity_in = bell_draw(seeds[1], (3, MX, MY, MZ), 0.5, 3.0, ((1, 2), (2, 4), (3, 4)), jnp.float32)
    pressure_in = draw_pressure_in(jax.random.fold_in(seeds[4], 71), 0)
    wall_types = set_ends((jax.random.randint(seeds[3], (3, NX, NY, NZ), 0, 4) < 1).astype(jnp.int32), jax.random.fold_in(seeds[3], 1), 0, 1)
    return {"species": species, "velocity_in": velocity_in, "pressure_in": pressure_in, "wall_types": wall_types}


GAMMA = 1.4
COURANT = 0.4
FLOOR = 0.1
SLOPE_FLOOR = 0.01
SPREAD = 0.002
RELAX = 0.1

def primitives(conserved):
    density = lax.optimization_barrier(jnp.sum(conserved[:SPECIES], axis=0))
    safe_rho = jnp.maximum(density, FLOOR)
    momentum = conserved[SPECIES:SPECIES + 3]
    velocity = momentum / safe_rho
    pressure = (GAMMA - 1.0) * (conserved[SPECIES + 3] - 0.5 * lax.optimization_barrier(jnp.sum(momentum * velocity, axis=0)))
    sound = jnp.sqrt(GAMMA * jnp.maximum(pressure, FLOOR) / safe_rho)
    return (density, safe_rho, velocity, pressure, sound)

def entropy(density, safe_rho, pressure):
    return density * (jnp.log(jnp.maximum(pressure, FLOOR)) - GAMMA * jnp.log(safe_rho))

def component_mask(target, length):
    component = lax.broadcasted_iota(jnp.int32, (length, 1, 1, 1), 0)
    return component == target

def node_flux(conserved, velocity, pressure, spatial):
    along = velocity[spatial]
    length = conserved.shape[0]
    normal = component_mask(SPECIES + spatial, length)
    energy_row = component_mask(SPECIES + 3, length)
    return conserved * along + jnp.where(normal, pressure, 0.0) + jnp.where(energy_row, pressure * along, 0.0)

def element_form(values):
    blocks = [extent // P_SIZE for extent in values.shape]
    return values.reshape(blocks[0], P_SIZE, blocks[1], P_SIZE, blocks[2], P_SIZE)

def element_min(values):
    return lax.optimization_barrier(jnp.min(element_form(values), axis=(1, 3, 5)))

def element_mean(values):
    return lax.optimization_barrier(jnp.mean(element_form(values), axis=(1, 3, 5)))

def to_nodes(values):
    blocks = values.shape
    wide = jnp.broadcast_to(values[:, None, :, None, :, None], (blocks[0], P_SIZE, blocks[1], P_SIZE, blocks[2], P_SIZE))
    return wide.reshape(blocks[0] * P_SIZE, blocks[1] * P_SIZE, blocks[2] * P_SIZE)

def neighbour_min(values):
    result = values
    for spatial in range(3):
        result = jnp.minimum(result, jnp.roll(values, 1, spatial))
        result = jnp.minimum(result, jnp.roll(values, -1, spatial))
    return result

def interface_pair(conserved, velocity, pressure, sound, wall_types, spatial):
    array_axis = spatial + 1
    terms = node_flux(conserved, velocity, pressure, spatial)
    right_terms = jnp.roll(terms, -1, array_axis)
    high_flux = (7.0 * (terms + right_terms) - (jnp.roll(terms, 1, array_axis) + jnp.roll(terms, -2, array_axis))) / 12.0
    wave_rate = jnp.abs(velocity[spatial]) + sound
    max_rate = jnp.maximum(wave_rate, jnp.roll(wave_rate, -1, spatial))
    low_flux = 0.5 * (terms + right_terms) - 0.5 * max_rate * (jnp.roll(conserved, -1, array_axis) - conserved)
    wall_flux = jnp.where(component_mask(SPECIES + spatial, conserved.shape[0]), 0.5 * (pressure + jnp.roll(pressure, -1, spatial)), 0.0)
    position = lax.broadcasted_iota(jnp.int32, pressure.shape, spatial)
    wall_flags = jnp.roll(to_nodes(wall_types[spatial]), -1, spatial)
    wall_face = (position % P_SIZE == P_SIZE - 1) & (wall_flags == 1)
    return (jnp.where(wall_face, wall_flux, low_flux), jnp.where(wall_face, wall_flux, high_flux))

def divergence(fluxes):
    result = fluxes[0] - jnp.roll(fluxes[0], 1, 1)
    for spatial in range(1, 3):
        result = result + fluxes[spatial] - jnp.roll(fluxes[spatial], 1, spatial + 1)
    return result

def newton_update(blending, delta, trial_rho, trial_vel, trial_p, residual, rho_bound, p_bound, lowest, mean_sq):
    node_blend = to_nodes(blending)
    rho_target = rho_bound - RELAX * jnp.maximum(rho_bound - lowest[0], 0.0)
    p_target = p_bound - RELAX * jnp.maximum(p_bound - lowest[1], 0.0)
    d_rho = lax.optimization_barrier(jnp.sum(delta[:SPECIES], axis=0))
    slope = (GAMMA - 1.0) * (delta[SPECIES + 3] - lax.optimization_barrier(jnp.sum(trial_vel * delta[SPECIES:SPECIES + 3], axis=0)) + 0.5 * lax.optimization_barrier(jnp.sum(trial_vel * trial_vel, axis=0)) * d_rho)
    t_rho = node_blend + jnp.minimum(trial_rho - to_nodes(rho_target), 0.0) / jnp.maximum(-d_rho, SLOPE_FLOOR)
    t_pres = node_blend + jnp.minimum(trial_p - to_nodes(p_target), 0.0) / jnp.maximum(-slope, SLOPE_FLOOR)
    cap = (mean_sq + SPREAD) / (mean_sq + SPREAD + element_mean(residual * residual))
    return jnp.maximum(jnp.minimum(cap, jnp.minimum(element_min(t_rho), element_min(t_pres))), 0.0)

def reference(species, velocity_in, pressure_in, wall_types):
    density_in = lax.optimization_barrier(jnp.sum(species, axis=0))
    momentum = density_in * velocity_in
    energy = pressure_in / (GAMMA - 1.0) + 0.5 * density_in * lax.optimization_barrier(jnp.sum(velocity_in * velocity_in, axis=0))
    conserved = jnp.concatenate([species, momentum, energy[None]], axis=0)
    density, safe_rho, velocity, pressure, sound = primitives(conserved)
    speed_max = jnp.max(lax.optimization_barrier(jnp.sum(jnp.abs(velocity), axis=0)) + 3.0 * sound)
    step_ratio = COURANT / speed_max
    flux_pairs = [interface_pair(conserved, velocity, pressure, sound, wall_types, spatial) for spatial in range(3)]
    low_state = conserved - step_ratio * divergence([pair[0] for pair in flux_pairs])
    high_state = conserved - step_ratio * divergence([pair[1] for pair in flux_pairs])
    delta = high_state - low_state
    rho_bound = neighbour_min(element_min(density))
    p_bound = neighbour_min(element_min(pressure))
    low_prims = primitives(low_state)
    low_sigma = entropy(low_prims[0], low_prims[1], low_prims[3])
    blending = jnp.ones(rho_bound.shape, jnp.float32)
    for newton in range(ITERS):
        trial_state = low_state + to_nodes(blending) * delta
        trial_prims = primitives(trial_state)
        residual = entropy(trial_prims[0], trial_prims[1], trial_prims[3]) - low_sigma
        lowest = jnp.stack([jnp.min(trial_prims[0]), jnp.min(trial_prims[3])])
        mean_sq = jnp.sum(residual * residual) / residual.size
        blending = newton_update(blending, delta, trial_prims[0], trial_prims[2], trial_prims[3], residual, rho_bound, p_bound, lowest, mean_sq)
    node_blend = to_nodes(blending)
    blended = []
    for spatial in range(3):
        face_theta = jnp.minimum(node_blend, jnp.roll(node_blend, -1, spatial))
        low_flux, high_flux = flux_pairs[spatial]
        blended.append(low_flux + face_theta * (high_flux - low_flux))
    new_state = conserved - step_ratio * divergence(blended)
    return (new_state, blending)
```

```python
import functools
import itertools

import jax
import jax.numpy as jnp
from jax import lax
from jax.experimental import pallas as pl
from jax.experimental.pallas import tpu as pltpu
from jax.sharding import PartitionSpec as P

SPECIES = 5
P_SIZE = 4
ITERS = 2
GAMMA = 1.4
COURANT = 0.4
FLOOR = 0.1
SLOPE_FLOOR = 0.01
SPREAD = 0.002
RELAX = 0.1

COMPS = SPECIES + 4
AXES = ("gx", "gy", "gz")
ROW = 128
DIRECT = 64
MESH = pl.DeviceIdType.MESH


def reduce_groups(sizes):
    if sizes[0] * sizes[1] * sizes[2] <= DIRECT:
        return [(0, 1, 2)]
    return [(2,), (1,), (0,)]


def group_offsets(sizes, group):
    spans = [range(sizes[d]) if d in group else (0,) for d in range(3)]
    far = lambda off: sum(min(off[d], sizes[d] - off[d]) for d in range(3))
    return sorted(itertools.product(*spans), key=far)


def halo_links(sizes):
    return [(d, k) for d in range(3) for k in ((1,) if sizes[d] == 2 else (1, -1))]


def conserved_of(inputs):
    species, velocity, pressure = inputs[:SPECIES], inputs[SPECIES : SPECIES + 3], inputs[-1]
    density = sum(species[1:], species[0])
    square = velocity[0] * velocity[0] + velocity[1] * velocity[1] + velocity[2] * velocity[2]
    energy = pressure * (1.0 / (GAMMA - 1.0)) + 0.5 * density * square
    return list(species) + [density * v for v in velocity] + [energy]


def primitives(cons):
    density = sum(cons[1:SPECIES], cons[0])
    safe = jnp.maximum(density, FLOOR)
    inverse = 1.0 / safe
    momentum = cons[SPECIES : SPECIES + 3]
    velocity = [m * inverse for m in momentum]
    kinetic = momentum[0] * velocity[0] + momentum[1] * velocity[1] + momentum[2] * velocity[2]
    pressure = (GAMMA - 1.0) * (cons[SPECIES + 3] - 0.5 * kinetic)
    return density, safe, inverse, velocity, pressure


def sound_of(inverse, pressure):
    return jnp.sqrt(GAMMA * jnp.maximum(pressure, FLOOR) * inverse)


def entropy(density, safe, pressure):
    return density * (jnp.log(jnp.maximum(pressure, FLOOR)) - GAMMA * jnp.log(safe))


def flux_term(cons, velocity, pressure, comp, d):
    term = cons[comp] * velocity[d]
    if comp == SPECIES + d:
        term = term + pressure
    if comp == SPECIES + 3:
        term = term + pressure * velocity[d]
    return term


def face_pair(mm, left, right, pp, jump, rate, wall, wall_value):
    both = left + right
    high = (7.0 * both - (mm + pp)) * (1.0 / 12.0)
    low = 0.5 * both - rate * jump
    keep = 0.0 if wall_value is None else wall_value
    diff = jnp.where(wall, 0.0, high - low)
    return jnp.where(wall, keep, low), diff


def kernel(
    sizes, sp_hbm, ve_hbm, pr_hbm, wa_hbm, out, bl, sp, ve, pr, wa, load_sem,
    xsp, xve, xpr, ys, yr, hy, zs, zr, es, er, pk, pn, pz, qz,
    dx, du, dw, lows, deltas, halo_send, halo_recv, near_sem, all_sem, *reduce_scratch
):
    X, Y, Z = pr.shape
    EX, EY, EZ = wa.shape[1:]
    loads = [
        pltpu.make_async_copy(source, target, load_sem.at[i])
        for i, (source, target) in enumerate(
            ((sp_hbm, sp), (ve_hbm, ve), (pr_hbm, pr), (wa_hbm, wa))
        )
    ]
    for copy in loads:
        copy.start()
    me = [lax.axis_index(name) for name in AXES]
    groups = reduce_groups(sizes)

    place = [[me[d]] + [lax.rem(me[d] + k, sizes[d]) for k in range(1, sizes[d])] for d in range(3)]

    def device(off):
        return tuple(place[d][off[d]] for d in range(3))

    def step(d, k):
        return tuple(k % sizes[d] if a == d else 0 for a in range(3))

    def traced(flag):
        return jnp.where(flag, 1, 0).astype(jnp.int32)

    links = halo_links(sizes)
    near = {link: near_sem.at[i] for i, link in enumerate(links)}

    def later(d, k):
        return me[d] != sizes[d] - 1 if k == 1 else me[d] == 0

    def neighbour(d, k):
        return device(step(d, k))

    corner = tuple(n - 1 for n in sizes)
    is_corner = (me[0] == corner[0]) & (me[1] == corner[1]) & (me[2] == corner[2])
    devices = sizes[0] * sizes[1] * sizes[2]
    barrier = pltpu.get_barrier_semaphore()

    @pl.when(jnp.logical_not(is_corner))
    def _():
        pl.semaphore_signal(barrier, inc=1, device_id=corner, device_id_type=MESH)

    expected = jnp.where(is_corner, devices - 1, 0).astype(jnp.int32)
    for d, k in links:

        @pl.when(later(d, k))
        def _(d=d, k=k):
            pl.semaphore_signal(barrier, inc=1, device_id=neighbour(d, k), device_id_type=MESH)

        expected = expected + 1 - traced(later(d, k))

    @pl.when(expected > 0)
    def _():
        pl.semaphore_wait(barrier, expected)

    for d, k in links:
        back = (d, k if sizes[d] == 2 else -k)

        @pl.when(jnp.logical_not(later(d, k)))
        def _(d=d, k=k, back=back):
            pl.semaphore_signal(
                near[back], inc=1, device_id=neighbour(d, k), device_id_type=MESH
            )

    @pl.when(is_corner)
    def _():
        def tell(i, carry):
            z = lax.rem(i, sizes[2])
            y = lax.rem(lax.div(i, sizes[2]), sizes[1])
            x = lax.div(i, sizes[2] * sizes[1])
            pl.semaphore_signal(all_sem, inc=1, device_id=(x, y, z), device_id_type=MESH)
            return carry

        if devices <= DIRECT:
            for at in itertools.product(*[range(n) for n in sizes]):
                if at != corner:
                    pl.semaphore_signal(all_sem, inc=1, device_id=at, device_id_type=MESH)
        else:
            lax.fori_loop(0, devices - 1, tell, 0)

    def await_near(d, k):
        @pl.when(later(d, k))
        def _():
            pl.semaphore_wait(near[d, k], 1)

    def await_all():
        @pl.when(jnp.logical_not(is_corner))
        def _():
            pl.semaphore_wait(all_sem, 1)

    for copy in loads:
        copy.wait()

    started = []

    def send(src, dst, slot, off):
        copy = pltpu.make_async_remote_copy(
            src_ref=src,
            dst_ref=dst,
            send_sem=halo_send.at[slot],
            recv_sem=halo_recv.at[slot],
            device_id=device(off),
            device_id_type=MESH,
        )
        copy.start()
        started.append(copy)
        return copy

    def spread_copy(turn, stage, i):
        base = 4 * (turn * len(groups) + stage)
        mine, buf, ssem, rsem = reduce_scratch[base : base + 4]
        group = groups[stage]
        off = group_offsets(sizes, group)[i]
        there = tuple(
            lax.rem(sizes[d] - 1 - me[d] + off[d], sizes[d]) if d in group else me[d]
            for d in range(3)
        )
        can_be_me = all((off[d] + 1 - sizes[d]) % 2 == 0 or sizes[d] % 2 for d in group)
        copy = pltpu.make_async_remote_copy(
            src_ref=mine,
            dst_ref=buf.at[pl.ds(i, 1)],
            send_sem=ssem,
            recv_sem=rsem,
            device_id=there,
            device_id_type=MESH,
        )
        return copy, can_be_me, functools.reduce(lambda a, b: a & b, [t == m for t, m in zip(there, me)])

    def spread_start(turn, stage, row):
        base = 4 * (turn * len(groups) + stage)
        mine, buf = reduce_scratch[base : base + 2]
        mine[...] = row
        for i in range(buf.shape[0]):
            copy, can_be_me, is_me = spread_copy(turn, stage, i)
            if not can_be_me:
                copy.start()
                continue

            @pl.when(jnp.logical_not(is_me))
            def _(copy=copy):
                copy.start()

            @pl.when(is_me)
            def _(i=i):
                buf[i : i + 1] = row

    def spread_whole(turn, stage):
        base = 4 * (turn * len(groups) + stage)
        _, buf, ssem, rsem = reduce_scratch[base : base + 4]
        rows = buf.at[pl.ds(0, buf.shape[0] - 1)]
        return pltpu.make_async_remote_copy(
            src_ref=rows,
            dst_ref=rows,
            send_sem=ssem,
            recv_sem=rsem,
            device_id=device((1, 1, 1)),
            device_id_type=MESH,
        )

    def spread_end(turn, combine):
        for stage in range(len(groups)):
            if stage > 0:
                spread_start(turn, stage, row)
            spread_whole(turn, stage).wait_recv()
            row = combine(reduce_scratch[4 * (turn * len(groups) + stage) + 1][...])
        return row

    def spread_sent(turn):
        for stage in range(len(groups)):
            spread_whole(turn, stage).wait_send()

    row_index = lax.broadcasted_iota(jnp.int32, (1, Y, Z), 1)
    lane_index = lax.broadcasted_iota(jnp.int32, (1, Y, Z), 2)
    index = {1: row_index, 2: lane_index}
    extent = {1: Y, 2: Z}

    def roll(value, shift, axis):
        return pltpu.roll(value, shift % value.shape[axis], axis)

    def mesh_group(value, axis, op):
        for s in (1, 2):
            low = (index[axis] & s) == 0
            value = op(value, jnp.where(low, roll(value, -s, axis), roll(value, s, axis)))
        return value

    def element(value, op):
        parts = value.reshape(EX, P_SIZE, Y, Z)
        value = op(op(parts[:, 0], parts[:, 1]), op(parts[:, 2], parts[:, 3]))
        return mesh_group(mesh_group(value, 1, op), 2, op)

    def nodes(value):
        return jnp.broadcast_to(value[:, None], (EX, P_SIZE, Y, Z)).reshape(X, Y, Z)

    def total(value, op):
        value = functools.reduce(op, [value[x] for x in range(X)])
        value = {jnp.minimum: jnp.min, jnp.maximum: jnp.max, jnp.add: jnp.sum}[op](
            value, axis=0, keepdims=True
        )
        return {jnp.minimum: jnp.min, jnp.maximum: jnp.max, jnp.add: jnp.sum}[op](
            value, axis=1, keepdims=True
        )

    def block(comp):
        if comp < SPECIES:
            return sp[comp]
        if comp < SPECIES + 3:
            return ve[comp - SPECIES]
        return pr[...]

    own_inputs = [block(c) for c in range(COMPS)]

    cons = conserved_of(own_inputs)
    density, _, inverse, velocity, pressure = primitives(cons)
    sound = sound_of(inverse, pressure)
    speed = jnp.abs(velocity[0]) + jnp.abs(velocity[1]) + jnp.abs(velocity[2]) + 3.0 * sound
    speed_row = jnp.broadcast_to(total(speed, jnp.maximum), (1, ROW))

    for c in range(COMPS):
        for x in range(X):
            ys[0, c, 2 * x : 2 * x + 2, :] = own_inputs[c][x, Y - 2 : Y, :]
            ys[1, c, 2 * x : 2 * x + 2, :] = own_inputs[c][x, 0:2, :]
    packs = zs.shape[0]
    per_pack = Z // (4 * X)
    for v in range(packs):
        packed = jnp.zeros((1, Y, Z), jnp.float32)
        for c in range(v * per_pack, min((v + 1) * per_pack, COMPS)):
            for x in range(X):
                at = ((c - v * per_pack) * X + x) * 4
                moved = roll(own_inputs[c][x : x + 1], at + 2, 2)
                packed = jnp.where((lane_index >= at) & (lane_index < at + 4), moved, packed)
        zs[v] = packed[0]

    rho_min = element(density, jnp.minimum)
    p_min = element(pressure, jnp.minimum)
    widen = (
        lax.broadcasted_iota(jnp.int32, (EZ, Z), 1) // P_SIZE
        == lax.broadcasted_iota(jnp.int32, (EZ, Z), 0)
    ).astype(jnp.float32)
    heighten = (
        lax.broadcasted_iota(jnp.int32, (Y, EY), 0) // P_SIZE
        == lax.broadcasted_iota(jnp.int32, (Y, EY), 1)
    ).astype(jnp.float32)
    walls = []
    for d in range(3):
        layers = []
        for e in range(EX):
            flags = wa[d, e].astype(jnp.float32)
            flags = jnp.dot(flags, widen, preferred_element_type=jnp.float32)
            layers.append(jnp.dot(heighten, flags, preferred_element_type=jnp.float32)[None])
        walls.append(jnp.concatenate(layers, axis=0))
        es[d, 0] = rho_min
        es[d, 1] = p_min
        es[d, 2] = walls[d]

    arrivals = {}

    def halo(key, src, dst, slot, off):
        copy = pltpu.make_async_remote_copy(
            src_ref=src,
            dst_ref=dst,
            send_sem=halo_send.at[slot],
            recv_sem=halo_recv.at[slot],
            device_id=device(off),
            device_id_type=MESH,
        )
        arrivals.setdefault(key, []).append(copy)
        started.append(copy)

    for side, k in ((0, 1), (1, -1)):
        at = X - 2 if side == 0 else 0
        halo(("x", side), sp.at[:, at : at + 2], xsp.at[side], 3 * side, step(0, k))
        halo(("x", side), ve.at[:, at : at + 2], xve.at[side], 3 * side + 1, step(0, k))
        halo(("x", side), pr.at[at : at + 2], xpr.at[side], 3 * side + 2, step(0, k))
        halo(("y", side), ys.at[side], yr.at[side], 6 + side, step(1, k))
        halo(("z", side), zs, zr.at[side], 8 + side, step(2, k))
        for d in range(3):
            halo(("e", d, side), es.at[d], er.at[side, d], 10 + 2 * d + side, step(d, k))

    def send_halo(d):
        for side, k in ((0, 1), (1, -1)):
            if (d, k) in links:
                await_near(d, k)
            for key in ((AXES[d][1], side), ("e", d, side)):
                for copy in arrivals[key]:
                    copy.start()

    late = me[2] == sizes[2] - 1

    @pl.when(jnp.logical_not(late))
    def _():
        send_halo(0)

    send_halo(1)
    send_halo(2)
    await_all()
    spread_start(0, 0, speed_row)

    @pl.when(late)
    def _():
        send_halo(0)

    def arrive(*key):
        for copy in arrivals[key]:
            copy.wait_recv()

    def cyclic_fluxes(d, halo_inputs, number):
        n = extent[d]
        ix = index[d]
        halo = conserved_of(halo_inputs)
        _, _, h_inv, h_vel, h_p = primitives(halo)
        h_rate = jnp.abs(h_vel[d]) + sound_of(h_inv, h_p)
        rate = jnp.abs(velocity[d]) + sound
        first, last = ix == 0, ix == n - 1
        two_first, two_last = ix < 2, ix >= n - 2

        def right_of(value, beyond):
            return roll(jnp.where(first, beyond, value), -1, d)

        arrive("e", d, 0)
        arrive("e", d, 1)
        flag = right_of(walls[d], er[1, d, 2])
        flag_low = roll(walls[d], -1, d)
        ends = (ix & (P_SIZE - 1)) == P_SIZE - 1
        wall = nodes(jnp.where(ends, flag, 0.0)) > 0.5
        wall_low = nodes(jnp.where(ends, flag_low, 0.0)) > 0.5
        half_rate = 0.5 * jnp.maximum(rate, right_of(rate, h_rate))
        half_low = 0.5 * jnp.maximum(h_rate, roll(rate, -1, d))
        wall_p = 0.5 * (pressure + right_of(pressure, h_p))
        wall_p_low = 0.5 * (h_p + roll(pressure, -1, d))
        for c in range(COMPS):
            f = flux_term(cons, velocity, pressure, c, d)
            h = flux_term(halo, h_vel, h_p, c, d)
            is_normal = c == SPECIES + d
            low, diff = face_pair(
                roll(jnp.where(last, h, f), 1, d),
                f,
                right_of(f, h),
                roll(jnp.where(two_first, h, f), -2, d),
                right_of(cons[c], halo[c]) - cons[c],
                half_rate,
                wall,
                wall_p if is_normal else None,
            )
            edge_low, edge_diff = face_pair(
                roll(h, 1, d),
                h,
                roll(f, -1, d),
                roll(f, -2, d),
                roll(cons[c], -1, d) - halo[c],
                half_low,
                wall_low,
                wall_p_low if is_normal else None,
            )
            before_low = roll(jnp.where(last, edge_low, low), 1, d)
            before_diff = roll(jnp.where(last, edge_diff, diff), 1, d)
            du[number, c] = diff
            dw[number, c] = before_diff
            if number == 0:
                lows[c] = low - before_low
                deltas[c] = diff - before_diff
            else:
                lows[c] += low - before_low
                deltas[c] += diff - before_diff

    arrive("z", 0)
    arrive("z", 1)
    merged = [
        jnp.where((lane_index & 3) < 2, zr[0, v][None], zr[1, v][None]) for v in range(packs)
    ]
    z_halo = []
    for c in range(COMPS):
        layers = []
        for x in range(X):
            at = ((c % per_pack) * X + x) * 4
            layers.append(roll(merged[c // per_pack], -(at + 2), 2))
        z_halo.append(jnp.concatenate(layers, axis=0))
    cyclic_fluxes(2, z_halo, 0)

    arrive("y", 0)
    arrive("y", 1)
    for c in range(COMPS):
        hy[c] = own_inputs[c]
        for x in range(X):
            hy[c, x, Y - 2 : Y, :] = yr[0, c, 2 * x : 2 * x + 2, :]
            hy[c, x, 0:2, :] = yr[1, c, 2 * x : 2 * x + 2, :]
    cyclic_fluxes(1, [hy[c] for c in range(COMPS)], 1)

    for side in (0, 1):
        arrive("x", side)
        arrive("e", 0, side)
    sides = []
    for side in (0, 1):
        inputs = [xsp[side, c] for c in range(SPECIES)]
        inputs += [xve[side, c] for c in range(3)]
        inputs.append(xpr[side])
        halo = conserved_of(inputs)
        _, _, h_inv, h_vel, h_p = primitives(halo)
        sides.append((halo, h_vel, h_p, jnp.abs(h_vel[0]) + sound_of(h_inv, h_p)))

    def joined(below, own, above):
        return jnp.concatenate([below, own, above], axis=0)

    rate = joined(sides[0][3], jnp.abs(velocity[0]) + sound, sides[1][3])
    p_ext = joined(sides[0][2], pressure, sides[1][2])
    half_rate = 0.5 * jnp.maximum(rate[1 : X + 2], rate[2 : X + 3])
    wall_p = 0.5 * (p_ext[1 : X + 2] + p_ext[2 : X + 3])
    planes = []
    for x in range(-1, X):
        if (x + 1) % P_SIZE:
            planes.append(jnp.zeros((1, Y, Z), jnp.float32))
        elif x == X - 1:
            planes.append(er[1, 0, 2, 0:1])
        else:
            e = (x + 1) // P_SIZE
            planes.append(walls[0][e : e + 1])
    wall = jnp.concatenate(planes, axis=0) > 0.5
    for c in range(COMPS):
        f = joined(
            flux_term(sides[0][0], sides[0][1], sides[0][2], c, 0),
            flux_term(cons, velocity, pressure, c, 0),
            flux_term(sides[1][0], sides[1][1], sides[1][2], c, 0),
        )
        u = joined(sides[0][0][c], cons[c], sides[1][0][c])
        low, diff = face_pair(
            f[0 : X + 1],
            f[1 : X + 2],
            f[2 : X + 3],
            f[3 : X + 4],
            u[2 : X + 3] - u[1 : X + 2],
            half_rate,
            wall,
            wall_p if c == SPECIES else None,
        )
        dx[c] = diff
        lows[c] += low[1:] - low[:-1]
        deltas[c] += diff[1:] - diff[:-1]

    def bound(own, which):
        best = own
        for d in (1, 2):
            n = extent[d]
            up = jnp.where(index[d] < P_SIZE, er[1, d, which], own)
            down = jnp.where(index[d] >= n - P_SIZE, er[0, d, which], own)
            best = jnp.minimum(best, jnp.minimum(roll(up, -P_SIZE, d), roll(down, P_SIZE, d)))
        chain = joined(er[0, 0, which, EX - 1 : EX], own, er[1, 0, which, 0:1])
        return jnp.minimum(best, jnp.minimum(chain[:EX], chain[2:]))

    rho_bound = bound(rho_min, 0)
    p_bound = bound(p_min, 1)

    speed_max = spread_end(0, lambda rows: jnp.max(rows, axis=0, keepdims=True))
    ratio = (COURANT / speed_max)[0:1, 0:1].reshape(1, 1, 1)

    for c in range(COMPS):
        lows[c] = cons[c] - ratio * lows[c]
        deltas[c] = -(ratio * deltas[c])
    low_density, low_safe, _, _, low_pressure = primitives([lows[c] for c in range(COMPS)])
    low_sigma = entropy(low_density, low_safe, low_pressure)
    d_rho = sum([deltas[c] for c in range(1, SPECIES)], deltas[0])
    rho_scale = 1.0 / jnp.maximum(-d_rho, SLOPE_FLOOR)
    count = X * Y * Z * sizes[0] * sizes[1] * sizes[2]
    stat_lane = lax.broadcasted_iota(jnp.int32, (1, ROW), 1)

    def combine_stats(rows):
        return jnp.where(
            stat_lane < 2,
            jnp.min(rows, axis=0, keepdims=True),
            jnp.sum(rows, axis=0, keepdims=True),
        )

    def next_blend(got, packed):
        t_density, rho_scale, t_p, p_scale, rho_bound, p_bound, mean_square, base = packed
        lowest_rho = got[0:1, 0:1].reshape(1, 1, 1)
        lowest_p = got[0:1, 1:2].reshape(1, 1, 1)
        spread = got[0:1, 2:3].reshape(1, 1, 1) * (1.0 / count) + SPREAD
        rho_target = rho_bound - RELAX * jnp.maximum(rho_bound - lowest_rho, 0.0)
        p_target = p_bound - RELAX * jnp.maximum(p_bound - lowest_p, 0.0)
        step_rho = jnp.minimum(t_density - nodes(rho_target), 0.0) * rho_scale
        step_p = jnp.minimum(t_p - nodes(p_target), 0.0) * p_scale
        lowered = element(jnp.minimum(step_rho, step_p), jnp.minimum)
        cap = spread / (spread + mean_square)
        return jnp.maximum(jnp.minimum(cap, base + lowered), 0.0)

    per_edge = Z // (2 * P_SIZE)
    blend = None
    for newton in range(ITERS):
        blend_nodes = None if blend is None else nodes(blend)
        trial = [
            lows[c] + (deltas[c] if blend is None else blend_nodes * deltas[c])
            for c in range(COMPS)
        ]
        t_density, t_safe, _, t_vel, t_p = primitives(trial)
        residual = entropy(t_density, t_safe, t_p) - low_sigma
        square = residual * residual
        stats = jnp.where(
            stat_lane == 0,
            total(t_density, jnp.minimum),
            jnp.where(stat_lane == 1, total(t_p, jnp.minimum), total(square, jnp.add)),
        )
        spread_start(newton + 1, 0, stats)
        cross = sum([t_vel[k] * deltas[SPECIES + k] for k in range(1, 3)], t_vel[0] * deltas[SPECIES])
        speed2 = t_vel[0] * t_vel[0] + t_vel[1] * t_vel[1] + t_vel[2] * t_vel[2]
        slope = (GAMMA - 1.0) * (deltas[SPECIES + 3] - cross + 0.5 * speed2 * d_rho)
        p_scale = 1.0 / jnp.maximum(-slope, SLOPE_FLOOR)
        mean_square = element(square, jnp.add) * (1.0 / (P_SIZE**3))
        base = jnp.ones((EX, Y, Z), jnp.float32) if blend is None else blend
        if newton == ITERS - 1:
            fields = (t_density, rho_scale, t_p, p_scale)
            for i, value in enumerate(fields):
                pk[i * X : (i + 1) * X] = value
            for i, value in enumerate((rho_bound, p_bound, mean_square, base)):
                pk[4 * X + i * EX : 4 * X + (i + 1) * EX] = value
            items = [value[x : x + 1] for value in fields for x in range(X)]
            for value in (rho_bound, p_bound, mean_square, base):
                items += [value[e : e + 1] for e in range(EX)]
            for v in range(pz.shape[0]):
                packed = jnp.zeros((1, Y, Z), jnp.float32)
                for j, item in enumerate(items[v * per_edge : (v + 1) * per_edge]):
                    at = 2 * P_SIZE * j
                    moved = roll(item, at + P_SIZE, 2)
                    inside = (lane_index >= at) & (lane_index < at + 2 * P_SIZE)
                    packed = jnp.where(inside, moved, packed)
                pz[v] = packed[0]
            for side, k in ((0, 1), (1, -1)):
                arrivals["b", 2, side] = [send(pz, qz.at[side], 20 + side, step(2, k))]
            for d in (0, 1):
                for side, k in ((0, 1), (1, -1)):
                    if side == 0 or sizes[d] > 2:
                        copy = send(pk, pn.at[side, d], 16 + 2 * d + side, step(d, k))
                        arrivals["b", d, side] = [copy]
                    else:
                        arrivals["b", d, side] = []
        got = spread_end(newton + 1, combine_stats)
        blend = next_blend(
            got, (t_density, rho_scale, t_p, p_scale, rho_bound, p_bound, mean_square, base)
        )

    beside = {}
    arrive("b", 2, 0)
    arrive("b", 2, 1)
    near = (lane_index & (2 * P_SIZE - 1)) < P_SIZE
    edges = [jnp.where(near, qz[0, v][None], qz[1, v][None]) for v in range(qz.shape[1])]
    items = [
        roll(edges[j // per_edge], -(2 * P_SIZE * (j % per_edge) + P_SIZE), 2)
        for j in range(4 * X + 4 * EX)
    ]
    packed = [jnp.concatenate(items[i * X : (i + 1) * X], axis=0) for i in range(4)]
    packed += [
        jnp.concatenate(items[4 * X + i * EX : 4 * X + (i + 1) * EX], axis=0) for i in range(4)
    ]
    beside[2, 0] = beside[2, 1] = next_blend(got, packed)
    for d in (0, 1):
        for side in (0, 1):
            arrive("b", d, side)
            if side == 1 and sizes[d] == 2:
                beside[d, side] = beside[d, 0]
                continue
            packed = [pn[side, d, i * X : (i + 1) * X] for i in range(4)]
            packed += [pn[side, d, 4 * X + i * EX : 4 * X + (i + 1) * EX] for i in range(4)]
            beside[d, side] = next_blend(got, packed)

    pick_lanes = (
        lax.broadcasted_iota(jnp.int32, (Z, EZ), 1) * P_SIZE
        == lax.broadcasted_iota(jnp.int32, (Z, EZ), 0)
    ).astype(jnp.float32)
    for e in range(EX):
        few = jnp.dot(
            blend[e], pick_lanes, preferred_element_type=jnp.float32, precision=lax.Precision.HIGHEST
        )
        bl[e] = jnp.concatenate([few[j * P_SIZE : j * P_SIZE + 1] for j in range(EY)], axis=0)

    theta = []
    for d in (2, 1):
        above = roll(jnp.where(index[d] == 0, beside[d, 1], blend), -1, d)
        below = roll(jnp.where(index[d] == extent[d] - 1, beside[d, 0], blend), 1, d)
        theta.append((nodes(jnp.minimum(blend, above)), nodes(jnp.minimum(blend, below))))
    x_blend = joined(beside[0, 0][EX - 1 : EX], nodes(blend), beside[0, 1][0:1])
    x_theta = jnp.minimum(x_blend[:-1], x_blend[1:])
    for c in range(COMPS):
        faces = x_theta * dx[c]
        change = faces[1:] - faces[:-1]
        for number in range(2):
            upper, lower = theta[number]
            change += upper * du[number, c] - lower * dw[number, c]
        out[c] = lows[c] - ratio * change

    for copy in started:
        copy.wait_send()
    for turn in range(ITERS + 1):
        spread_sent(turn)


def solution(mesh):
    sizes = tuple(mesh.shape[name] for name in AXES)

    def local(species, velocity_in, pressure_in, wall_types):
        X, Y, Z = pressure_in.shape
        EX, EY, EZ = wall_types.shape[1:]
        packs = -(-COMPS // (Z // (4 * X)))
        edge_packs = -(-(4 * X + 4 * EX) // (Z // (2 * P_SIZE)))
        vmem = lambda *shape: pltpu.VMEM(shape, jnp.float32)
        reduce_scratch = []
        for _ in range(ITERS + 1):
            for group in reduce_groups(sizes):
                n = len(group_offsets(sizes, group))
                reduce_scratch += [
                    vmem(1, ROW),
                    vmem(n, ROW),
                    pltpu.SemaphoreType.DMA(()),
                    pltpu.SemaphoreType.DMA(()),
                ]
        return tuple(
            pl.pallas_call(
                functools.partial(kernel, sizes),
                out_shape=[
                    pltpu.VMEM((COMPS, X, Y, Z), jnp.float32),
                    pltpu.VMEM((EX, EY, EZ), jnp.float32),
                ],
                in_specs=[pl.BlockSpec(memory_space=pltpu.HBM)] * 4,
                out_specs=[pl.BlockSpec(memory_space=pltpu.VMEM)] * 2,
                scratch_shapes=[
                    vmem(SPECIES, X, Y, Z),
                    vmem(3, X, Y, Z),
                    vmem(X, Y, Z),
                    pltpu.VMEM((3, EX, EY, EZ), jnp.int32),
                    pltpu.SemaphoreType.DMA((4,)),
                    vmem(2, SPECIES, 2, Y, Z),
                    vmem(2, 3, 2, Y, Z),
                    vmem(2, 2, Y, Z),
                    vmem(2, COMPS, 2 * X, Z),
                    vmem(2, COMPS, 2 * X, Z),
                    vmem(COMPS, X, Y, Z),
                    vmem(packs, Y, Z),
                    vmem(2, packs, Y, Z),
                    vmem(3, 3, EX, Y, Z),
                    vmem(2, 3, 3, EX, Y, Z),
                    vmem(4 * X + 4 * EX, Y, Z),
                    vmem(2, 2, 4 * X + 4 * EX, Y, Z),
                    vmem(edge_packs, Y, Z),
                    vmem(2, edge_packs, Y, Z),
                    vmem(COMPS, X + 1, Y, Z),
                    vmem(2, COMPS, X, Y, Z),
                    vmem(2, COMPS, X, Y, Z),
                    vmem(COMPS, X, Y, Z),
                    vmem(COMPS, X, Y, Z),
                    pltpu.SemaphoreType.DMA((22,)),
                    pltpu.SemaphoreType.DMA((22,)),
                    pltpu.SemaphoreType.REGULAR((len(halo_links(sizes)),)),
                    pltpu.SemaphoreType.REGULAR,
                ]
                + reduce_scratch,
                compiler_params=pltpu.CompilerParams(collective_id=0, has_side_effects=True),
            )(species, velocity_in, pressure_in, wall_types)
        )

    in_specs = (
        P(None, "gx", "gy", "gz"),
        P(None, "gx", "gy", "gz"),
        P("gx", "gy", "gz"),
        P(None, "gx", "gy", "gz"),
    )
    out_specs = (P(None, "gx", "gy", "gz"), P("gx", "gy", "gz"))
    return jax.shard_map(local, mesh=mesh, in_specs=in_specs, out_specs=out_specs, check_vma=False)
```

```python
import functools
import itertools

import jax
import jax.numpy as jnp
from jax import lax
from jax.experimental import pallas as pl
from jax.experimental.pallas import tpu as pltpu
from jax.sharding import PartitionSpec as P

SPECIES = 5
P_SIZE = 4
ITERS = 2
GAMMA = 1.4
COURANT = 0.4
FLOOR = 0.1
SLOPE_FLOOR = 0.01
SPREAD = 0.002
RELAX = 0.1

COMPS = SPECIES + 4
AXES = ("gx", "gy", "gz")
ROW = 128
DIRECT = 64
MESH = pl.DeviceIdType.MESH


def reduce_groups(sizes):
    if sizes[0] * sizes[1] * sizes[2] <= DIRECT:
        return [(0, 1, 2)]
    return [(2,), (1,), (0,)]


def group_offsets(sizes, group):
    spans = [range(sizes[d]) if d in group else (0,) for d in range(3)]
    far = lambda off: sum(min(off[d], sizes[d] - off[d]) for d in range(3))
    return sorted(itertools.product(*spans), key=far)


def halo_links(sizes):
    return [(d, k) for d in range(3) for k in ((1,) if sizes[d] == 2 else (1, -1))]


def conserved_of(inputs):
    species, velocity, pressure = inputs[:SPECIES], inputs[SPECIES : SPECIES + 3], inputs[-1]
    density = sum(species[1:], species[0])
    square = velocity[0] * velocity[0] + velocity[1] * velocity[1] + velocity[2] * velocity[2]
    energy = pressure * (1.0 / (GAMMA - 1.0)) + 0.5 * density * square
    return list(species) + [density * v for v in velocity] + [energy]


def primitives(cons):
    density = sum(cons[1:SPECIES], cons[0])
    safe = jnp.maximum(density, FLOOR)
    inverse = 1.0 / safe
    momentum = cons[SPECIES : SPECIES + 3]
    velocity = [m * inverse for m in momentum]
    kinetic = momentum[0] * velocity[0] + momentum[1] * velocity[1] + momentum[2] * velocity[2]
    pressure = (GAMMA - 1.0) * (cons[SPECIES + 3] - 0.5 * kinetic)
    return density, safe, inverse, velocity, pressure


def sound_of(inverse, pressure):
    return jnp.sqrt(GAMMA * jnp.maximum(pressure, FLOOR) * inverse)


def entropy(density, safe, pressure):
    return density * (jnp.log(jnp.maximum(pressure, FLOOR)) - GAMMA * jnp.log(safe))


def flux_term(cons, velocity, pressure, comp, d):
    term = cons[comp] * velocity[d]
    if comp == SPECIES + d:
        term = term + pressure
    if comp == SPECIES + 3:
        term = term + pressure * velocity[d]
    return term


def face_pair(mm, left, right, pp, jump, rate, wall, wall_value):
    both = left + right
    high = (7.0 * both - (mm + pp)) * (1.0 / 12.0)
    low = 0.5 * both - rate * jump
    keep = 0.0 if wall_value is None else wall_value
    diff = jnp.where(wall, 0.0, high - low)
    return jnp.where(wall, keep, low), diff


def kernel(
    sizes, sp_hbm, ve_hbm, pr_hbm, wa_hbm, out, bl, sp, ve, pr, wa, load_sem,
    xsp, xve, xpr, ys, yr, hy, zs, zr, es, er, pk, pn, pz, qz,
    dx, du, dw, lows, deltas, halo_send, halo_recv, near_sem, all_sem, *reduce_scratch
):
    X, Y, Z = pr.shape
    EX, EY, EZ = wa.shape[1:]
    loads = [
        pltpu.make_async_copy(source, target, load_sem.at[i])
        for i, (source, target) in enumerate(
            ((sp_hbm, sp), (ve_hbm, ve), (pr_hbm, pr), (wa_hbm, wa))
        )
    ]
    for copy in loads:
        copy.start()
    me = [lax.axis_index(name) for name in AXES]
    groups = reduce_groups(sizes)

    place = [[me[d]] + [lax.rem(me[d] + k, sizes[d]) for k in range(1, sizes[d])] for d in range(3)]

    def device(off):
        return tuple(place[d][off[d]] for d in range(3))

    def step(d, k):
        return tuple(k % sizes[d] if a == d else 0 for a in range(3))

    def traced(flag):
        return jnp.where(flag, 1, 0).astype(jnp.int32)

    links = halo_links(sizes)
    near = {link: near_sem.at[i] for i, link in enumerate(links)}

    def later(d, k):
        return me[d] != sizes[d] - 1 if k == 1 else me[d] == 0

    def neighbour(d, k):
        return device(step(d, k))

    corner = tuple(n - 1 for n in sizes)
    is_corner = (me[0] == corner[0]) & (me[1] == corner[1]) & (me[2] == corner[2])
    devices = sizes[0] * sizes[1] * sizes[2]
    barrier = pltpu.get_barrier_semaphore()

    @pl.when(jnp.logical_not(is_corner))
    def _():
        pl.semaphore_signal(barrier, inc=1, device_id=corner, device_id_type=MESH)

    expected = jnp.where(is_corner, devices - 1, 0).astype(jnp.int32)
    for d, k in links:

        @pl.when(later(d, k))
        def _(d=d, k=k):
            pl.semaphore_signal(barrier, inc=1, device_id=neighbour(d, k), device_id_type=MESH)

        expected = expected + 1 - traced(later(d, k))

    @pl.when(expected > 0)
    def _():
        pl.semaphore_wait(barrier, expected)

    for d, k in links:
        back = (d, k if sizes[d] == 2 else -k)

        @pl.when(jnp.logical_not(later(d, k)))
        def _(d=d, k=k, back=back):
            pl.semaphore_signal(
                near[back], inc=1, device_id=neighbour(d, k), device_id_type=MESH
            )

    @pl.when(is_corner)
    def _():
        def tell(i, carry):
            z = lax.rem(i, sizes[2])
            y = lax.rem(lax.div(i, sizes[2]), sizes[1])
            x = lax.div(i, sizes[2] * sizes[1])
            pl.semaphore_signal(all_sem, inc=1, device_id=(x, y, z), device_id_type=MESH)
            return carry

        if devices <= DIRECT:
            for at in itertools.product(*[range(n) for n in sizes]):
                if at != corner:
                    pl.semaphore_signal(all_sem, inc=1, device_id=at, device_id_type=MESH)
        else:
            lax.fori_loop(0, devices - 1, tell, 0)

    def await_near(d, k):
        @pl.when(later(d, k))
        def _():
            pl.semaphore_wait(near[d, k], 1)

    def await_all():
        @pl.when(jnp.logical_not(is_corner))
        def _():
            pl.semaphore_wait(all_sem, 1)

    for copy in loads:
        copy.wait()

    started = []

    def send(src, dst, slot, off):
        copy = pltpu.make_async_remote_copy(
            src_ref=src,
            dst_ref=dst,
            send_sem=halo_send.at[slot],
            recv_sem=halo_recv.at[slot],
            device_id=device(off),
            device_id_type=MESH,
        )
        copy.start()
        started.append(copy)
        return copy

    def spread_copy(turn, stage, i):
        base = 4 * (turn * len(groups) + stage)
        mine, buf, ssem, rsem = reduce_scratch[base : base + 4]
        group = groups[stage]
        off = group_offsets(sizes, group)[i]
        there = tuple(
            lax.rem(sizes[d] - 1 - me[d] + off[d], sizes[d]) if d in group else me[d]
            for d in range(3)
        )
        can_be_me = all((off[d] + 1 - sizes[d]) % 2 == 0 or sizes[d] % 2 for d in group)
        copy = pltpu.make_async_remote_copy(
            src_ref=mine,
            dst_ref=buf.at[pl.ds(i, 1)],
            send_sem=ssem,
            recv_sem=rsem,
            device_id=there,
            device_id_type=MESH,
        )
        return copy, can_be_me, functools.reduce(lambda a, b: a & b, [t == m for t, m in zip(there, me)])

    def spread_start(turn, stage, row):
        base = 4 * (turn * len(groups) + stage)
        mine, buf = reduce_scratch[base : base + 2]
        mine[...] = row
        for i in range(buf.shape[0]):
            copy, can_be_me, is_me = spread_copy(turn, stage, i)
            if not can_be_me:
                copy.start()
                continue

            @pl.when(jnp.logical_not(is_me))
            def _(copy=copy):
                copy.start()

            @pl.when(is_me)
            def _(i=i):
                buf[i : i + 1] = row

    def spread_whole(turn, stage):
        base = 4 * (turn * len(groups) + stage)
        _, buf, ssem, rsem = reduce_scratch[base : base + 4]
        rows = buf.at[pl.ds(0, buf.shape[0] - 1)]
        return pltpu.make_async_remote_copy(
            src_ref=rows,
            dst_ref=rows,
            send_sem=ssem,
            recv_sem=rsem,
            device_id=device((1, 1, 1)),
            device_id_type=MESH,
        )

    def spread_end(turn, combine):
        for stage in range(len(groups)):
            if stage > 0:
                spread_start(turn, stage, row)
            spread_whole(turn, stage).wait_recv()
            row = combine(reduce_scratch[4 * (turn * len(groups) + stage) + 1][...])
        return row

    def spread_sent(turn):
        for stage in range(len(groups)):
            spread_whole(turn, stage).wait_send()

    row_index = lax.broadcasted_iota(jnp.int32, (1, Y, Z), 1)
    lane_index = lax.broadcasted_iota(jnp.int32, (1, Y, Z), 2)
    index = {1: row_index, 2: lane_index}
    extent = {1: Y, 2: Z}

    def roll(value, shift, axis):
        return pltpu.roll(value, shift % value.shape[axis], axis)

    def mesh_group(value, axis, op):
        for s in (1, 2):
            low = (index[axis] & s) == 0
            value = op(value, jnp.where(low, roll(value, -s, axis), roll(value, s, axis)))
        return value

    def element(value, op):
        parts = value.reshape(EX, P_SIZE, Y, Z)
        value = op(op(parts[:, 0], parts[:, 1]), op(parts[:, 2], parts[:, 3]))
        return mesh_group(mesh_group(value, 1, op), 2, op)

    def nodes(value):
        return jnp.broadcast_to(value[:, None], (EX, P_SIZE, Y, Z)).reshape(X, Y, Z)

    def total(value, op):
        value = functools.reduce(op, [value[x] for x in range(X)])
        value = {jnp.minimum: jnp.min, jnp.maximum: jnp.max, jnp.add: jnp.sum}[op](
            value, axis=0, keepdims=True
        )
        return {jnp.minimum: jnp.min, jnp.maximum: jnp.max, jnp.add: jnp.sum}[op](
            value, axis=1, keepdims=True
        )

    def block(comp):
        if comp < SPECIES:
            return sp[comp]
        if comp < SPECIES + 3:
            return ve[comp - SPECIES]
        return pr[...]

    own_inputs = [block(c) for c in range(COMPS)]

    cons = conserved_of(own_inputs)
    density, _, inverse, velocity, pressure = primitives(cons)
    sound = sound_of(inverse, pressure)
    speed = jnp.abs(velocity[0]) + jnp.abs(velocity[1]) + jnp.abs(velocity[2]) + 3.0 * sound
    speed_row = jnp.broadcast_to(total(speed, jnp.maximum), (1, ROW))
    late = me[2] == corner[2]
    last_chip = (me[0] == corner[0]) & (me[1] >= corner[1] - 1) & late

    @pl.when(last_chip)
    def _():
        await_all()
        spread_start(0, 0, speed_row)


    for c in range(COMPS):
        for x in range(X):
            ys[0, c, 2 * x : 2 * x + 2, :] = own_inputs[c][x, Y - 2 : Y, :]
            ys[1, c, 2 * x : 2 * x + 2, :] = own_inputs[c][x, 0:2, :]
    packs = zs.shape[0]
    per_pack = Z // (4 * X)
    for v in range(packs):
        packed = jnp.zeros((1, Y, Z), jnp.float32)
        for c in range(v * per_pack, min((v + 1) * per_pack, COMPS)):
            for x in range(X):
                at = ((c - v * per_pack) * X + x) * 4
                moved = roll(own_inputs[c][x : x + 1], at + 2, 2)
                packed = jnp.where((lane_index >= at) & (lane_index < at + 4), moved, packed)
        zs[v] = packed[0]

    rho_min = element(density, jnp.minimum)
    p_min = element(pressure, jnp.minimum)
    widen = (
        lax.broadcasted_iota(jnp.int32, (EZ, Z), 1) // P_SIZE
        == lax.broadcasted_iota(jnp.int32, (EZ, Z), 0)
    ).astype(jnp.float32)
    heighten = (
        lax.broadcasted_iota(jnp.int32, (Y, EY), 0) // P_SIZE
        == lax.broadcasted_iota(jnp.int32, (Y, EY), 1)
    ).astype(jnp.float32)
    walls = []
    for d in range(3):
        layers = []
        for e in range(EX):
            flags = wa[d, e].astype(jnp.float32)
            flags = jnp.dot(flags, widen, preferred_element_type=jnp.float32)
            layers.append(jnp.dot(heighten, flags, preferred_element_type=jnp.float32)[None])
        walls.append(jnp.concatenate(layers, axis=0))
        es[d, 0] = rho_min
        es[d, 1] = p_min
        es[d, 2] = walls[d]

    arrivals = {}

    def halo(key, src, dst, slot, off):
        copy = pltpu.make_async_remote_copy(
            src_ref=src,
            dst_ref=dst,
            send_sem=halo_send.at[slot],
            recv_sem=halo_recv.at[slot],
            device_id=device(off),
            device_id_type=MESH,
        )
        arrivals.setdefault(key, []).append(copy)
        started.append(copy)

    for side, k in ((0, 1), (1, -1)):
        at = X - 2 if side == 0 else 0
        halo(("x", side), sp.at[:, at : at + 2], xsp.at[side], 3 * side, step(0, k))
        halo(("x", side), ve.at[:, at : at + 2], xve.at[side], 3 * side + 1, step(0, k))
        halo(("x", side), pr.at[at : at + 2], xpr.at[side], 3 * side + 2, step(0, k))
        halo(("y", side), ys.at[side], yr.at[side], 6 + side, step(1, k))
        halo(("z", side), zs, zr.at[side], 8 + side, step(2, k))
        for d in range(3):
            halo(("e", d, side), es.at[d], er.at[side, d], 10 + 2 * d + side, step(d, k))

    def send_halo(d):
        for side, k in ((0, 1), (1, -1)):
            if (d, k) in links:
                await_near(d, k)
            for key in ((AXES[d][1], side), ("e", d, side)):
                for copy in arrivals[key]:
                    copy.start()

    @pl.when(jnp.logical_not(late))
    def _():
        send_halo(0)
        send_halo(1)

    send_halo(2)

    @pl.when(late)
    def _():
        send_halo(1)

    @pl.when(jnp.logical_not(last_chip))
    def _():
        await_all()
        spread_start(0, 0, speed_row)

    @pl.when(late)
    def _():
        send_halo(0)

    def arrive(*key):
        for copy in arrivals[key]:
            copy.wait_recv()

    def cyclic_fluxes(d, halo_inputs, number, first):
        n = extent[d]
        ix = index[d]
        halo = conserved_of(halo_inputs)
        _, _, h_inv, h_vel, h_p = primitives(halo)
        h_rate = jnp.abs(h_vel[d]) + sound_of(h_inv, h_p)
        rate = jnp.abs(velocity[d]) + sound
        at_first, last = ix == 0, ix == n - 1
        two_first, two_last = ix < 2, ix >= n - 2

        def right_of(value, beyond):
            return roll(jnp.where(at_first, beyond, value), -1, d)

        arrive("e", d, 0)
        arrive("e", d, 1)
        flag = right_of(walls[d], er[1, d, 2])
        flag_low = roll(walls[d], -1, d)
        ends = (ix & (P_SIZE - 1)) == P_SIZE - 1
        wall = nodes(jnp.where(ends, flag, 0.0)) > 0.5
        wall_low = nodes(jnp.where(ends, flag_low, 0.0)) > 0.5
        half_rate = 0.5 * jnp.maximum(rate, right_of(rate, h_rate))
        half_low = 0.5 * jnp.maximum(h_rate, roll(rate, -1, d))
        wall_p = 0.5 * (pressure + right_of(pressure, h_p))
        wall_p_low = 0.5 * (h_p + roll(pressure, -1, d))
        for c in range(COMPS):
            f = flux_term(cons, velocity, pressure, c, d)
            h = flux_term(halo, h_vel, h_p, c, d)
            is_normal = c == SPECIES + d
            low, diff = face_pair(
                roll(jnp.where(last, h, f), 1, d),
                f,
                right_of(f, h),
                roll(jnp.where(two_first, h, f), -2, d),
                right_of(cons[c], halo[c]) - cons[c],
                half_rate,
                wall,
                wall_p if is_normal else None,
            )
            edge_low, edge_diff = face_pair(
                roll(h, 1, d),
                h,
                roll(f, -1, d),
                roll(f, -2, d),
                roll(cons[c], -1, d) - halo[c],
                half_low,
                wall_low,
                wall_p_low if is_normal else None,
            )
            before_low = roll(jnp.where(last, edge_low, low), 1, d)
            before_diff = roll(jnp.where(last, edge_diff, diff), 1, d)
            du[number, c] = diff
            dw[number, c] = before_diff
            if first:
                lows[c] = low - before_low
                deltas[c] = diff - before_diff
            else:
                lows[c] += low - before_low
                deltas[c] += diff - before_diff

    arrive("y", 0)
    arrive("y", 1)
    for c in range(COMPS):
        hy[c] = own_inputs[c]
        for x in range(X):
            hy[c, x, Y - 2 : Y, :] = yr[0, c, 2 * x : 2 * x + 2, :]
            hy[c, x, 0:2, :] = yr[1, c, 2 * x : 2 * x + 2, :]
    cyclic_fluxes(1, [hy[c] for c in range(COMPS)], 1, True)

    arrive("z", 0)
    arrive("z", 1)
    merged = [
        jnp.where((lane_index & 3) < 2, zr[0, v][None], zr[1, v][None]) for v in range(packs)
    ]
    z_halo = []
    for c in range(COMPS):
        layers = []
        for x in range(X):
            at = ((c % per_pack) * X + x) * 4
            layers.append(roll(merged[c // per_pack], -(at + 2), 2))
        z_halo.append(jnp.concatenate(layers, axis=0))
    cyclic_fluxes(2, z_halo, 0, False)

    for side in (0, 1):
        arrive("x", side)
        arrive("e", 0, side)
    sides = []
    for side in (0, 1):
        inputs = [xsp[side, c] for c in range(SPECIES)]
        inputs += [xve[side, c] for c in range(3)]
        inputs.append(xpr[side])
        halo = conserved_of(inputs)
        _, _, h_inv, h_vel, h_p = primitives(halo)
        sides.append((halo, h_vel, h_p, jnp.abs(h_vel[0]) + sound_of(h_inv, h_p)))

    def joined(below, own, above):
        return jnp.concatenate([below, own, above], axis=0)

    rate = joined(sides[0][3], jnp.abs(velocity[0]) + sound, sides[1][3])
    p_ext = joined(sides[0][2], pressure, sides[1][2])
    half_rate = 0.5 * jnp.maximum(rate[1 : X + 2], rate[2 : X + 3])
    wall_p = 0.5 * (p_ext[1 : X + 2] + p_ext[2 : X + 3])
    planes = []
    for x in range(-1, X):
        if (x + 1) % P_SIZE:
            planes.append(jnp.zeros((1, Y, Z), jnp.float32))
        elif x == X - 1:
            planes.append(er[1, 0, 2, 0:1])
        else:
            e = (x + 1) // P_SIZE
            planes.append(walls[0][e : e + 1])
    wall = jnp.concatenate(planes, axis=0) > 0.5
    for c in range(COMPS):
        f = joined(
            flux_term(sides[0][0], sides[0][1], sides[0][2], c, 0),
            flux_term(cons, velocity, pressure, c, 0),
            flux_term(sides[1][0], sides[1][1], sides[1][2], c, 0),
        )
        u = joined(sides[0][0][c], cons[c], sides[1][0][c])
        low, diff = face_pair(
            f[0 : X + 1],
            f[1 : X + 2],
            f[2 : X + 3],
            f[3 : X + 4],
            u[2 : X + 3] - u[1 : X + 2],
            half_rate,
            wall,
            wall_p if c == SPECIES else None,
        )
        dx[c] = diff
        lows[c] += low[1:] - low[:-1]
        deltas[c] += diff[1:] - diff[:-1]

    def bound(own, which):
        best = own
        for d in (1, 2):
            n = extent[d]
            up = jnp.where(index[d] < P_SIZE, er[1, d, which], own)
            down = jnp.where(index[d] >= n - P_SIZE, er[0, d, which], own)
            best = jnp.minimum(best, jnp.minimum(roll(up, -P_SIZE, d), roll(down, P_SIZE, d)))
        chain = joined(er[0, 0, which, EX - 1 : EX], own, er[1, 0, which, 0:1])
        return jnp.minimum(best, jnp.minimum(chain[:EX], chain[2:]))

    rho_bound = bound(rho_min, 0)
    p_bound = bound(p_min, 1)

    speed_max = spread_end(0, lambda rows: jnp.max(rows, axis=0, keepdims=True))
    ratio = (COURANT / speed_max)[0:1, 0:1].reshape(1, 1, 1)

    for c in range(COMPS):
        lows[c] = cons[c] - ratio * lows[c]
        deltas[c] = -(ratio * deltas[c])
    low_density, low_safe, _, _, low_pressure = primitives([lows[c] for c in range(COMPS)])
    low_sigma = entropy(low_density, low_safe, low_pressure)
    d_rho = sum([deltas[c] for c in range(1, SPECIES)], deltas[0])
    rho_scale = 1.0 / jnp.maximum(-d_rho, SLOPE_FLOOR)
    count = X * Y * Z * sizes[0] * sizes[1] * sizes[2]
    stat_lane = lax.broadcasted_iota(jnp.int32, (1, ROW), 1)

    def combine_stats(rows):
        return jnp.where(
            stat_lane < 2,
            jnp.min(rows, axis=0, keepdims=True),
            jnp.sum(rows, axis=0, keepdims=True),
        )

    def next_blend(got, packed):
        t_density, rho_scale, t_p, p_scale, rho_bound, p_bound, mean_square, base = packed
        lowest_rho = got[0:1, 0:1].reshape(1, 1, 1)
        lowest_p = got[0:1, 1:2].reshape(1, 1, 1)
        spread = got[0:1, 2:3].reshape(1, 1, 1) * (1.0 / count) + SPREAD
        rho_target = rho_bound - RELAX * jnp.maximum(rho_bound - lowest_rho, 0.0)
        p_target = p_bound - RELAX * jnp.maximum(p_bound - lowest_p, 0.0)
        step_rho = jnp.minimum(t_density - nodes(rho_target), 0.0) * rho_scale
        step_p = jnp.minimum(t_p - nodes(p_target), 0.0) * p_scale
        lowered = element(jnp.minimum(step_rho, step_p), jnp.minimum)
        cap = spread / (spread + mean_square)
        return jnp.maximum(jnp.minimum(cap, base + lowered), 0.0)

    per_edge = Z // (2 * P_SIZE)
    blend = None
    for newton in range(ITERS):
        blend_nodes = None if blend is None else nodes(blend)
        trial = [
            lows[c] + (deltas[c] if blend is None else blend_nodes * deltas[c])
            for c in range(COMPS)
        ]
        t_density, t_safe, _, t_vel, t_p = primitives(trial)
        residual = entropy(t_density, t_safe, t_p) - low_sigma
        square = residual * residual
        stats = jnp.where(
            stat_lane == 0,
            total(t_density, jnp.minimum),
            jnp.where(stat_lane == 1, total(t_p, jnp.minimum), total(square, jnp.add)),
        )
        spread_start(newton + 1, 0, stats)
        cross = sum([t_vel[k] * deltas[SPECIES + k] for k in range(1, 3)], t_vel[0] * deltas[SPECIES])
        speed2 = t_vel[0] * t_vel[0] + t_vel[1] * t_vel[1] + t_vel[2] * t_vel[2]
        slope = (GAMMA - 1.0) * (deltas[SPECIES + 3] - cross + 0.5 * speed2 * d_rho)
        p_scale = 1.0 / jnp.maximum(-slope, SLOPE_FLOOR)
        mean_square = element(square, jnp.add) * (1.0 / (P_SIZE**3))
        base = jnp.ones((EX, Y, Z), jnp.float32) if blend is None else blend
        if newton == ITERS - 1:
            fields = (t_density, rho_scale, t_p, p_scale)
            for i, value in enumerate(fields):
                pk[i * X : (i + 1) * X] = value
            for i, value in enumerate((rho_bound, p_bound, mean_square, base)):
                pk[4 * X + i * EX : 4 * X + (i + 1) * EX] = value
            items = [value[x : x + 1] for value in fields for x in range(X)]
            for value in (rho_bound, p_bound, mean_square, base):
                items += [value[e : e + 1] for e in range(EX)]
            for v in range(pz.shape[0]):
                packed = jnp.zeros((1, Y, Z), jnp.float32)
                for j, item in enumerate(items[v * per_edge : (v + 1) * per_edge]):
                    at = 2 * P_SIZE * j
                    moved = roll(item, at + P_SIZE, 2)
                    inside = (lane_index >= at) & (lane_index < at + 2 * P_SIZE)
                    packed = jnp.where(inside, moved, packed)
                pz[v] = packed[0]
            for side, k in ((0, 1), (1, -1)):
                arrivals["b", 2, side] = [send(pz, qz.at[side], 20 + side, step(2, k))]
            for d in (0, 1):
                for side, k in ((0, 1), (1, -1)):
                    if side == 0 or sizes[d] > 2:
                        copy = send(pk, pn.at[side, d], 16 + 2 * d + side, step(d, k))
                        arrivals["b", d, side] = [copy]
                    else:
                        arrivals["b", d, side] = []
        got = spread_end(newton + 1, combine_stats)
        blend = next_blend(
            got, (t_density, rho_scale, t_p, p_scale, rho_bound, p_bound, mean_square, base)
        )

    beside = {}
    arrive("b", 2, 0)
    arrive("b", 2, 1)
    near = (lane_index & (2 * P_SIZE - 1)) < P_SIZE
    edges = [jnp.where(near, qz[0, v][None], qz[1, v][None]) for v in range(qz.shape[1])]
    items = [
        roll(edges[j // per_edge], -(2 * P_SIZE * (j % per_edge) + P_SIZE), 2)
        for j in range(4 * X + 4 * EX)
    ]
    packed = [jnp.concatenate(items[i * X : (i + 1) * X], axis=0) for i in range(4)]
    packed += [
        jnp.concatenate(items[4 * X + i * EX : 4 * X + (i + 1) * EX], axis=0) for i in range(4)
    ]
    beside[2, 0] = beside[2, 1] = next_blend(got, packed)
    for d in (0, 1):
        for side in (0, 1):
            arrive("b", d, side)
            if side == 1 and sizes[d] == 2:
                beside[d, side] = beside[d, 0]
                continue
            packed = [pn[side, d, i * X : (i + 1) * X] for i in range(4)]
            packed += [pn[side, d, 4 * X + i * EX : 4 * X + (i + 1) * EX] for i in range(4)]
            beside[d, side] = next_blend(got, packed)

    pick_lanes = (
        lax.broadcasted_iota(jnp.int32, (Z, EZ), 1) * P_SIZE
        == lax.broadcasted_iota(jnp.int32, (Z, EZ), 0)
    ).astype(jnp.float32)
    for e in range(EX):
        few = jnp.dot(
            blend[e], pick_lanes, preferred_element_type=jnp.float32, precision=lax.Precision.HIGHEST
        )
        bl[e] = jnp.concatenate([few[j * P_SIZE : j * P_SIZE + 1] for j in range(EY)], axis=0)

    theta = []
    for d in (2, 1):
        above = roll(jnp.where(index[d] == 0, beside[d, 1], blend), -1, d)
        below = roll(jnp.where(index[d] == extent[d] - 1, beside[d, 0], blend), 1, d)
        theta.append((nodes(jnp.minimum(blend, above)), nodes(jnp.minimum(blend, below))))
    x_blend = joined(beside[0, 0][EX - 1 : EX], nodes(blend), beside[0, 1][0:1])
    x_theta = jnp.minimum(x_blend[:-1], x_blend[1:])
    for c in range(COMPS):
        faces = x_theta * dx[c]
        change = faces[1:] - faces[:-1]
        for number in range(2):
            upper, lower = theta[number]
            change += upper * du[number, c] - lower * dw[number, c]
        out[c] = lows[c] - ratio * change

    for copy in started:
        copy.wait_send()
    for turn in range(ITERS + 1):
        spread_sent(turn)


def store(state, weights, state_hbm, weights_hbm, sem):
    copies = [
        pltpu.make_async_copy(state, state_hbm, sem.at[0]),
        pltpu.make_async_copy(weights, weights_hbm, sem.at[1]),
    ]
    for copy in copies:
        copy.start()
    for copy in copies:
        copy.wait()


def solution(mesh):
    sizes = tuple(mesh.shape[name] for name in AXES)

    def local(species, velocity_in, pressure_in, wall_types):
        X, Y, Z = pressure_in.shape
        EX, EY, EZ = wall_types.shape[1:]
        packs = -(-COMPS // (Z // (4 * X)))
        edge_packs = -(-(4 * X + 4 * EX) // (Z // (2 * P_SIZE)))
        vmem = lambda *shape: pltpu.VMEM(shape, jnp.float32)
        reduce_scratch = []
        for _ in range(ITERS + 1):
            for group in reduce_groups(sizes):
                n = len(group_offsets(sizes, group))
                reduce_scratch += [
                    vmem(1, ROW),
                    vmem(n, ROW),
                    pltpu.SemaphoreType.DMA(()),
                    pltpu.SemaphoreType.DMA(()),
                ]
        state, weights = (
            pl.pallas_call(
                functools.partial(kernel, sizes),
                out_shape=[
                    pltpu.VMEM((COMPS, X, Y, Z), jnp.float32),
                    pltpu.VMEM((EX, EY, EZ), jnp.float32),
                ],
                in_specs=[pl.BlockSpec(memory_space=pltpu.HBM)] * 4,
                out_specs=[pl.BlockSpec(memory_space=pltpu.VMEM)] * 2,
                scratch_shapes=[
                    vmem(SPECIES, X, Y, Z),
                    vmem(3, X, Y, Z),
                    vmem(X, Y, Z),
                    pltpu.VMEM((3, EX, EY, EZ), jnp.int32),
                    pltpu.SemaphoreType.DMA((4,)),
                    vmem(2, SPECIES, 2, Y, Z),
                    vmem(2, 3, 2, Y, Z),
                    vmem(2, 2, Y, Z),
                    vmem(2, COMPS, 2 * X, Z),
                    vmem(2, COMPS, 2 * X, Z),
                    vmem(COMPS, X, Y, Z),
                    vmem(packs, Y, Z),
                    vmem(2, packs, Y, Z),
                    vmem(3, 3, EX, Y, Z),
                    vmem(2, 3, 3, EX, Y, Z),
                    vmem(4 * X + 4 * EX, Y, Z),
                    vmem(2, 2, 4 * X + 4 * EX, Y, Z),
                    vmem(edge_packs, Y, Z),
                    vmem(2, edge_packs, Y, Z),
                    vmem(COMPS, X + 1, Y, Z),
                    vmem(2, COMPS, X, Y, Z),
                    vmem(2, COMPS, X, Y, Z),
                    vmem(COMPS, X, Y, Z),
                    vmem(COMPS, X, Y, Z),
                    pltpu.SemaphoreType.DMA((22,)),
                    pltpu.SemaphoreType.DMA((22,)),
                    pltpu.SemaphoreType.REGULAR((len(halo_links(sizes)),)),
                    pltpu.SemaphoreType.REGULAR,
                ]
                + reduce_scratch,
                compiler_params=pltpu.CompilerParams(collective_id=0, has_side_effects=True),
            )(species, velocity_in, pressure_in, wall_types)
        )
        return tuple(
            pl.pallas_call(
                store,
                out_shape=[
                    jax.ShapeDtypeStruct((COMPS, X, Y, Z), jnp.float32),
                    jax.ShapeDtypeStruct((EX, EY, EZ), jnp.float32),
                ],
                in_specs=[pl.BlockSpec(memory_space=pltpu.VMEM)] * 2,
                out_specs=[pl.BlockSpec(memory_space=pltpu.HBM)] * 2,
                scratch_shapes=[pltpu.SemaphoreType.DMA((2,))],
            )(*[pltpu.with_memory_space_constraint(v, pltpu.VMEM) for v in (state, weights)])
        )

    in_specs = (
        P(None, "gx", "gy", "gz"),
        P(None, "gx", "gy", "gz"),
        P("gx", "gy", "gz"),
        P(None, "gx", "gy", "gz"),
    )
    out_specs = (P(None, "gx", "gy", "gz"), P("gx", "gy", "gz"))
    return jax.shard_map(local, mesh=mesh, in_specs=in_specs, out_specs=out_specs, check_vma=False)
```

```python
import functools
import itertools

import jax
import jax.numpy as jnp
from jax import lax
from jax.experimental import pallas as pl
from jax.experimental.pallas import tpu as pltpu
from jax.sharding import PartitionSpec as P

SPECIES = 5
P_SIZE = 4
ITERS = 2
GAMMA = 1.4
COURANT = 0.4
FLOOR = 0.1
SLOPE_FLOOR = 0.01
SPREAD = 0.002
RELAX = 0.1

COMPS = SPECIES + 4
AXES = ("gx", "gy", "gz")
ROW = 128
DIRECT = 64
MESH = pl.DeviceIdType.MESH


def reduce_groups(sizes):
    if sizes[0] * sizes[1] * sizes[2] <= DIRECT:
        return [(0, 1, 2)]
    return [(2,), (1,), (0,)]


def group_offsets(sizes, group):
    spans = [range(sizes[d]) if d in group else (0,) for d in range(3)]
    far = lambda off: sum(min(off[d], sizes[d] - off[d]) for d in range(3))
    return sorted(itertools.product(*spans), key=far)


def halo_links(sizes):
    return [(d, k) for d in range(3) for k in ((1,) if sizes[d] == 2 else (1, -1))]


def conserved_of(inputs):
    species, velocity, pressure = inputs[:SPECIES], inputs[SPECIES : SPECIES + 3], inputs[-1]
    density = sum(species[1:], species[0])
    square = velocity[0] * velocity[0] + velocity[1] * velocity[1] + velocity[2] * velocity[2]
    energy = pressure * (1.0 / (GAMMA - 1.0)) + 0.5 * density * square
    return list(species) + [density * v for v in velocity] + [energy]


def primitives(cons):
    density = sum(cons[1:SPECIES], cons[0])
    safe = jnp.maximum(density, FLOOR)
    inverse = 1.0 / safe
    momentum = cons[SPECIES : SPECIES + 3]
    velocity = [m * inverse for m in momentum]
    kinetic = momentum[0] * velocity[0] + momentum[1] * velocity[1] + momentum[2] * velocity[2]
    pressure = (GAMMA - 1.0) * (cons[SPECIES + 3] - 0.5 * kinetic)
    return density, safe, inverse, velocity, pressure


def state_of(density, momentum, energy):
    safe = jnp.maximum(density, FLOOR)
    inverse = 1.0 / safe
    velocity = [m * inverse for m in momentum]
    kinetic = momentum[0] * velocity[0] + momentum[1] * velocity[1] + momentum[2] * velocity[2]
    pressure = (GAMMA - 1.0) * (energy - 0.5 * kinetic)
    return safe, velocity, pressure


def sound_of(inverse, pressure):
    return jnp.sqrt(GAMMA * jnp.maximum(pressure, FLOOR) * inverse)


def entropy(density, safe, pressure):
    return density * (jnp.log(jnp.maximum(pressure, FLOOR)) - GAMMA * jnp.log(safe))


def flux_term(cons, velocity, pressure, comp, d):
    term = cons[comp] * velocity[d]
    if comp == SPECIES + d:
        term = term + pressure
    if comp == SPECIES + 3:
        term = term + pressure * velocity[d]
    return term


def face_pair(mm, left, right, pp, jump, rate, wall, wall_value):
    both = left + right
    high = (7.0 * both - (mm + pp)) * (1.0 / 12.0)
    low = 0.5 * both - rate * jump
    keep = 0.0 if wall_value is None else wall_value
    diff = jnp.where(wall, 0.0, high - low)
    return jnp.where(wall, keep, low), diff


def kernel(
    sizes, sp_hbm, ve_hbm, pr_hbm, wa_hbm, out, bl, sp, ve, pr, wa, load_sem,
    xsp, xve, xpr, ys, yr, hy, zs, zr, es, er, pk, pnx, pny, pz, qz,
    dx, du, dw, lows, deltas, halo_send, halo_recv, near_sem, all_sem, relay, relay_send, relay_recv, *reduce_scratch
):
    X, Y, Z = pr.shape
    EX, EY, EZ = wa.shape[1:]
    loads = [
        pltpu.make_async_copy(source, target, load_sem.at[i])
        for i, (source, target) in enumerate(
            ((sp_hbm, sp), (ve_hbm, ve), (pr_hbm, pr), (wa_hbm, wa))
        )
    ]
    for copy in loads:
        copy.start()
    me = [lax.axis_index(name) for name in AXES]
    groups = reduce_groups(sizes)

    place = [[me[d]] + [lax.rem(me[d] + k, sizes[d]) for k in range(1, sizes[d])] for d in range(3)]

    def device(off):
        return tuple(place[d][off[d]] for d in range(3))

    def step(d, k):
        return tuple(k % sizes[d] if a == d else 0 for a in range(3))

    relayed = len(groups) == 1
    if relayed:
        reduce_scratch[1][...] = jnp.zeros_like(reduce_scratch[1])

    def traced(flag):
        return jnp.where(flag, 1, 0).astype(jnp.int32)

    links = halo_links(sizes)
    near = {link: near_sem.at[i] for i, link in enumerate(links)}

    def later(d, k):
        return me[d] != sizes[d] - 1 if k == 1 else me[d] == 0

    def neighbour(d, k):
        return device(step(d, k))

    corner = tuple(n - 1 for n in sizes)
    is_corner = (me[0] == corner[0]) & (me[1] == corner[1]) & (me[2] == corner[2])
    devices = sizes[0] * sizes[1] * sizes[2]
    barrier = pltpu.get_barrier_semaphore()

    @pl.when(jnp.logical_not(is_corner))
    def _():
        pl.semaphore_signal(barrier, inc=1, device_id=corner, device_id_type=MESH)

    expected = jnp.where(is_corner, devices - 1, 0).astype(jnp.int32)
    for d, k in links:

        @pl.when(later(d, k))
        def _(d=d, k=k):
            pl.semaphore_signal(barrier, inc=1, device_id=neighbour(d, k), device_id_type=MESH)

        expected = expected + 1 - traced(later(d, k))

    @pl.when(expected > 0)
    def _():
        pl.semaphore_wait(barrier, expected)

    for d, k in links:
        back = (d, k if sizes[d] == 2 else -k)

        @pl.when(jnp.logical_not(later(d, k)))
        def _(d=d, k=k, back=back):
            pl.semaphore_signal(
                near[back], inc=1, device_id=neighbour(d, k), device_id_type=MESH
            )

    @pl.when(is_corner)
    def _():
        def tell(i, carry):
            z = lax.rem(i, sizes[2])
            y = lax.rem(lax.div(i, sizes[2]), sizes[1])
            x = lax.div(i, sizes[2] * sizes[1])
            pl.semaphore_signal(all_sem, inc=1, device_id=(x, y, z), device_id_type=MESH)
            return carry

        if devices <= DIRECT:
            for at in itertools.product(*[range(n) for n in sizes]):
                if at != corner:
                    pl.semaphore_signal(all_sem, inc=1, device_id=at, device_id_type=MESH)
        else:
            lax.fori_loop(0, devices - 1, tell, 0)

    def await_near(d, k):
        @pl.when(later(d, k))
        def _():
            pl.semaphore_wait(near[d, k], 1)

    def await_all():
        @pl.when(jnp.logical_not(is_corner))
        def _():
            pl.semaphore_wait(all_sem, 1)

    for copy in loads:
        copy.wait()

    def send(src, dst, slot, off):
        copy = pltpu.make_async_remote_copy(
            src_ref=src,
            dst_ref=dst,
            send_sem=halo_send.at[slot],
            recv_sem=halo_recv.at[slot],
            device_id=device(off),
            device_id_type=MESH,
        )
        copy.start()
        started.append(copy)
        return copy

    origin = (me[0] == 0) & (me[1] <= 1)
    next_up = origin & (me[2] == 1)
    origin = origin & (me[2] == 0)
    plane_rows = ((origin, devices - 2), (jnp.logical_not(origin), devices - 3))
    relay_copy = pltpu.make_async_remote_copy(
        src_ref=reduce_scratch[0],
        dst_ref=relay,
        send_sem=relay_send,
        recv_sem=relay_recv,
        device_id=neighbour(2, 1),
        device_id_type=MESH,
    )

    def speed_out():
        await_all()
        if not relayed:
            spread_start(0, 0, speed_row)
            return

        @pl.when(next_up)
        def _():
            relay_copy.wait_recv()
            spread_start(0, 0, jnp.maximum(speed_row, relay[...]))

        @pl.when(jnp.logical_not(origin | next_up))
        def _():
            spread_start(0, 0, speed_row)

    def spread_copy(turn, stage, i):
        base = 4 * (turn * len(groups) + stage)
        mine, buf, ssem, rsem = reduce_scratch[base : base + 4]
        group = groups[stage]
        off = group_offsets(sizes, group)[i]
        there = tuple(
            lax.rem(sizes[d] - 1 - me[d] + off[d], sizes[d]) if d in group else me[d]
            for d in range(3)
        )
        can_be_me = all((off[d] + 1 - sizes[d]) % 2 == 0 or sizes[d] % 2 for d in group)
        copy = pltpu.make_async_remote_copy(
            src_ref=mine,
            dst_ref=buf.at[pl.ds(i, 1)],
            send_sem=ssem,
            recv_sem=rsem,
            device_id=there,
            device_id_type=MESH,
        )
        return copy, can_be_me, functools.reduce(lambda a, b: a & b, [t == m for t, m in zip(there, me)])

    def spread_start(turn, stage, row):
        base = 4 * (turn * len(groups) + stage)
        mine, buf = reduce_scratch[base : base + 2]
        mine[...] = row
        for i in range(buf.shape[0]):
            copy, can_be_me, is_me = spread_copy(turn, stage, i)
            if not can_be_me:
                copy.start()
                continue

            @pl.when(jnp.logical_not(is_me))
            def _(copy=copy):
                copy.start()

            @pl.when(is_me)
            def _(i=i):
                buf[i : i + 1] = row

    def spread_whole(turn, stage, rows=None):
        base = 4 * (turn * len(groups) + stage)
        _, buf, ssem, rsem = reduce_scratch[base : base + 4]
        rows = buf.at[pl.ds(0, rows or buf.shape[0] - 1)]
        return pltpu.make_async_remote_copy(
            src_ref=rows,
            dst_ref=rows,
            send_sem=ssem,
            recv_sem=rsem,
            device_id=device((1, 1, 1)),
            device_id_type=MESH,
        )

    def spread_end(turn, combine):
        for stage in range(len(groups)):
            if stage > 0:
                spread_start(turn, stage, row)
            if turn == 0 and relayed:
                for flag, rows in plane_rows:

                    @pl.when(flag)
                    def _(rows=rows):
                        spread_whole(turn, stage, rows).wait_recv()
            else:
                spread_whole(turn, stage).wait_recv()
            row = combine(reduce_scratch[4 * (turn * len(groups) + stage) + 1][...])
        return row

    def spread_sent(turn):
        for stage in range(len(groups)):
            if turn == 0 and relayed:

                @pl.when(jnp.logical_not(origin))
                def _():
                    spread_whole(turn, stage).wait_send()

            else:
                spread_whole(turn, stage).wait_send()

    row_index = lax.broadcasted_iota(jnp.int32, (1, Y, Z), 1)
    lane_index = lax.broadcasted_iota(jnp.int32, (1, Y, Z), 2)
    index = {1: row_index, 2: lane_index}
    extent = {1: Y, 2: Z}

    def roll(value, shift, axis):
        return pltpu.roll(value, shift % value.shape[axis], axis)

    def mesh_group(value, axis, op):
        for s in (1, 2):
            low = (index[axis] & s) == 0
            value = op(value, jnp.where(low, roll(value, -s, axis), roll(value, s, axis)))
        return value

    def lane_group(value, op):
        place = lane_index & (P_SIZE - 1)
        for s in range(1, P_SIZE):
            ahead = roll(value, -s, 2)
            behind = roll(value, P_SIZE - s, 2)
            turned = jnp.where(place < P_SIZE - s, ahead, behind)
            whole = turned if s == 1 else op(whole, turned)
        return op(value, whole)

    def element(value, op):
        parts = value.reshape(EX, P_SIZE, Y, Z)
        value = op(op(parts[:, 0], parts[:, 1]), op(parts[:, 2], parts[:, 3]))
        return lane_group(mesh_group(value, 1, op), op)

    def nodes(value):
        return jnp.broadcast_to(value[:, None], (EX, P_SIZE, Y, Z)).reshape(X, Y, Z)

    def total(value, op):
        value = functools.reduce(op, [value[x] for x in range(X)])
        value = {jnp.minimum: jnp.min, jnp.maximum: jnp.max, jnp.add: jnp.sum}[op](
            value, axis=0, keepdims=True
        )
        return {jnp.minimum: jnp.min, jnp.maximum: jnp.max, jnp.add: jnp.sum}[op](
            value, axis=1, keepdims=True
        )

    def block(comp):
        if comp < SPECIES:
            return sp[comp]
        if comp < SPECIES + 3:
            return ve[comp - SPECIES]
        return pr[...]

    late = me[2] == corner[2]
    ahead = late & (me[1] < corner[1] - 1)
    last_x = me[0] == corner[0]
    started = []
    arrivals = {}

    def halo(key, src, dst, slot, off):
        copy = pltpu.make_async_remote_copy(
            src_ref=src,
            dst_ref=dst,
            send_sem=halo_send.at[slot],
            recv_sem=halo_recv.at[slot],
            device_id=device(off),
            device_id_type=MESH,
        )
        arrivals.setdefault(key, []).append(copy)
        started.append(copy)

    for side, k in ((0, 1), (1, -1)):
        at = X - 2 if side == 0 else 0
        halo(("x", side), sp.at[:, at : at + 2], xsp.at[side], 3 * side, step(0, k))
        halo(("x", side), ve.at[:, at : at + 2], xve.at[side], 3 * side + 1, step(0, k))
        halo(("x", side), pr.at[at : at + 2], xpr.at[side], 3 * side + 2, step(0, k))

    @pl.when(ahead & last_x)
    def _():
        arrivals["x", 0][0].start()

    own_inputs = [block(c) for c in range(COMPS)]

    cons = conserved_of(own_inputs)
    density, _, inverse, velocity, pressure = primitives(cons)
    sound = sound_of(inverse, pressure)
    speed = jnp.abs(velocity[0]) + jnp.abs(velocity[1]) + jnp.abs(velocity[2]) + 3.0 * sound
    speed_row = jnp.broadcast_to(total(speed, jnp.maximum), (1, ROW))
    last_chip = (me[0] == corner[0]) & (me[1] >= corner[1] - 1) & late

    @pl.when(last_chip)
    def _():
        speed_out()


    for c in range(COMPS):
        for x in range(X):
            ys[0, c, 2 * x : 2 * x + 2, :] = own_inputs[c][x, Y - 2 : Y, :]
            ys[1, c, 2 * x : 2 * x + 2, :] = own_inputs[c][x, 0:2, :]
    packs = zs.shape[0]
    per_pack = Z // (4 * X)
    for v in range(packs):
        packed = jnp.zeros((1, Y, Z), jnp.float32)
        for c in range(v * per_pack, min((v + 1) * per_pack, COMPS)):
            for x in range(X):
                at = ((c - v * per_pack) * X + x) * 4
                moved = roll(own_inputs[c][x : x + 1], at + 2, 2)
                packed = jnp.where((lane_index >= at) & (lane_index < at + 4), moved, packed)
        zs[v] = packed[0]

    rho_min = element(density, jnp.minimum)
    p_min = element(pressure, jnp.minimum)
    widen = (
        lax.broadcasted_iota(jnp.int32, (EZ, Z), 1) // P_SIZE
        == lax.broadcasted_iota(jnp.int32, (EZ, Z), 0)
    ).astype(jnp.float32)
    heighten = (
        lax.broadcasted_iota(jnp.int32, (Y, EY), 0) // P_SIZE
        == lax.broadcasted_iota(jnp.int32, (Y, EY), 1)
    ).astype(jnp.float32)
    walls = []
    for d in range(3):
        layers = []
        for e in range(EX):
            flags = wa[d, e].astype(jnp.float32)
            flags = jnp.dot(flags, widen, preferred_element_type=jnp.float32)
            layers.append(jnp.dot(heighten, flags, preferred_element_type=jnp.float32)[None])
        walls.append(jnp.concatenate(layers, axis=0))
        turn_row = row_index & (P_SIZE - 1)
        es[d] = jnp.where(turn_row == 0, rho_min, jnp.where(turn_row == 1, p_min, walls[d]))

    def spread_rows(value, which):
        value = jnp.where((row_index & (P_SIZE - 1)) == which, value, jnp.inf)
        return mesh_group(value, 1, jnp.minimum)

    def edge(side, d, which):
        side = 0 if sizes[d] == 2 and d == 0 else side
        return spread_rows(er[side, d], which)

    for side, k in ((0, 1), (1, -1)):
        halo(("y", side), ys.at[side], yr.at[side], 6 + side, step(1, k))
        halo(("z", side), zs, zr.at[side], 8 + side, step(2, k))
        for d in range(3):
            if d == 0 and sizes[0] == 2 and side == 1:
                arrivals["e", d, side] = []
                continue
            halo(("e", d, side), es.at[d], er.at[side, d], 10 + 2 * d + side, step(d, k))

    def send_halo(d, skip=0):
        for side, k in ((0, 1), (1, -1)):
            if (d, k) in links and not skip:
                await_near(d, k)
            for key in ((AXES[d][1], side), ("e", d, side)):
                for copy in arrivals[key][skip if side == 0 and key[0] != "e" else 0 :]:
                    copy.start()
            if d == 2 and side == 0 and relayed:

                @pl.when(origin)
                def _():
                    reduce_scratch[0][...] = speed_row
                    relay_copy.start()


    @pl.when(jnp.logical_not(late))
    def _():
        send_halo(0)
        send_halo(1)

    send_halo(2)

    @pl.when(ahead & jnp.logical_not(last_x))
    def _():
        for k in (1, -1):
            if (0, k) in links:
                await_near(0, k)
        arrivals["x", 0][0].start()

    @pl.when(late)
    def _():
        send_halo(1)

    @pl.when(jnp.logical_not(last_chip))
    def _():
        speed_out()

    @pl.when(ahead)
    def _():
        send_halo(0, 1)

    @pl.when(late & jnp.logical_not(ahead))
    def _():
        send_halo(0)

    def arrive(*key):
        for copy in arrivals[key]:
            copy.wait_recv()

    def cyclic_fluxes(d, halo_inputs, number, first):
        n = extent[d]
        ix = index[d]
        halo = conserved_of(halo_inputs)
        _, _, h_inv, h_vel, h_p = primitives(halo)
        h_rate = jnp.abs(h_vel[d]) + sound_of(h_inv, h_p)
        rate = jnp.abs(velocity[d]) + sound

        def beside(value, beyond, k):
            edge_of = ix < k if k > 0 else ix >= n + k
            return roll(jnp.where(edge_of, beyond, value), -k, d)

        shifts = (-2, -1, 1, 2)
        along = {k: {d: beside(velocity[d], h_vel[d], k)} for k in shifts}
        p_at = {k: beside(pressure, h_p, k) for k in shifts}
        arrive("e", d, 0)
        arrive("e", d, 1)
        flag = roll(jnp.where(ix == 0, edge(1, d, 2), walls[d]), -1, d)
        ends = ix & (P_SIZE - 1)
        wall = nodes(jnp.where(ends == P_SIZE - 1, flag, 0.0)) > 0.5
        wall_low = nodes(jnp.where(ends == 0, walls[d], 0.0)) > 0.5
        half_rate = 0.5 * jnp.maximum(rate, beside(rate, h_rate, 1))
        half_low = 0.5 * jnp.maximum(beside(rate, h_rate, -1), rate)
        wall_p = 0.5 * (pressure + p_at[1])
        wall_p_low = 0.5 * (p_at[-1] + pressure)
        for c in range(COMPS):
            u_at = {k: beside(cons[c], halo[c], k) for k in shifts}
            f_at = {k: flux_term({c: u_at[k]}, along[k], p_at[k], c, d) for k in shifts}
            f = flux_term(cons, velocity, pressure, c, d)
            is_normal = c == SPECIES + d
            low, diff = face_pair(
                f_at[-1],
                f,
                f_at[1],
                f_at[2],
                u_at[1] - cons[c],
                half_rate,
                wall,
                wall_p if is_normal else None,
            )
            before_low, before_diff = face_pair(
                f_at[-2],
                f_at[-1],
                f,
                f_at[1],
                cons[c] - u_at[-1],
                half_low,
                wall_low,
                wall_p_low if is_normal else None,
            )
            du[number, c] = diff
            dw[number, c] = before_diff
            slot = max(c - SPECIES + 1, 0)
            if first:
                lows[c] = low - before_low
            else:
                lows[c] += low - before_low
            if first and c in (0, *range(SPECIES, COMPS)):
                deltas[slot] = diff - before_diff
            else:
                deltas[slot] += diff - before_diff

    arrive("y", 0)
    arrive("y", 1)
    for c in range(COMPS):
        hy[c] = own_inputs[c]
        for x in range(X):
            hy[c, x, Y - 2 : Y, :] = yr[0, c, 2 * x : 2 * x + 2, :]
            hy[c, x, 0:2, :] = yr[1, c, 2 * x : 2 * x + 2, :]
    cyclic_fluxes(1, [hy[c] for c in range(COMPS)], 1, True)

    arrive("z", 0)
    arrive("z", 1)
    merged = [
        jnp.where((lane_index & 3) < 2, zr[0, v][None], zr[1, v][None]) for v in range(packs)
    ]
    z_halo = []
    for c in range(COMPS):
        layers = []
        for x in range(X):
            at = ((c % per_pack) * X + x) * 4
            layers.append(roll(merged[c // per_pack], -(at + 2), 2))
        z_halo.append(jnp.concatenate(layers, axis=0))
    cyclic_fluxes(2, z_halo, 0, False)

    for side in (0, 1):
        arrive("x", side)
        arrive("e", 0, side)
    sides = []
    for side in (0, 1):
        inputs = [xsp[side, c] for c in range(SPECIES)]
        inputs += [xve[side, c] for c in range(3)]
        inputs.append(xpr[side])
        halo = conserved_of(inputs)
        _, _, h_inv, h_vel, h_p = primitives(halo)
        sides.append((halo, h_vel, h_p, jnp.abs(h_vel[0]) + sound_of(h_inv, h_p)))

    def joined(below, own, above):
        return jnp.concatenate([below, own, above], axis=0)

    rate = joined(sides[0][3], jnp.abs(velocity[0]) + sound, sides[1][3])
    p_ext = joined(sides[0][2], pressure, sides[1][2])
    half_rate = 0.5 * jnp.maximum(rate[1 : X + 2], rate[2 : X + 3])
    wall_p = 0.5 * (p_ext[1 : X + 2] + p_ext[2 : X + 3])
    planes = []
    for x in range(-1, X):
        if (x + 1) % P_SIZE:
            planes.append(jnp.zeros((1, Y, Z), jnp.float32))
        elif x == X - 1:
            planes.append(edge(1, 0, 2)[0:1])
        else:
            e = (x + 1) // P_SIZE
            planes.append(walls[0][e : e + 1])
    wall = jnp.concatenate(planes, axis=0) > 0.5
    for c in range(COMPS):
        f = joined(
            flux_term(sides[0][0], sides[0][1], sides[0][2], c, 0),
            flux_term(cons, velocity, pressure, c, 0),
            flux_term(sides[1][0], sides[1][1], sides[1][2], c, 0),
        )
        u = joined(sides[0][0][c], cons[c], sides[1][0][c])
        low, diff = face_pair(
            f[0 : X + 1],
            f[1 : X + 2],
            f[2 : X + 3],
            f[3 : X + 4],
            u[2 : X + 3] - u[1 : X + 2],
            half_rate,
            wall,
            wall_p if c == SPECIES else None,
        )
        dx[c] = diff
        lows[c] += low[1:] - low[:-1]
        deltas[max(c - SPECIES + 1, 0)] += diff[1:] - diff[:-1]

    def bound(own, which):
        best = own
        for d in (1, 2):
            n = extent[d]
            up = jnp.where(index[d] < P_SIZE, edge(1, d, which), own)
            down = jnp.where(index[d] >= n - P_SIZE, edge(0, d, which), own)
            best = jnp.minimum(best, jnp.minimum(roll(up, -P_SIZE, d), roll(down, P_SIZE, d)))
        chain = joined(edge(0, 0, which)[EX - 1 : EX], own, edge(1, 0, which)[0:1])
        return jnp.minimum(best, jnp.minimum(chain[:EX], chain[2:]))

    rho_bound = bound(rho_min, 0)
    p_bound = bound(p_min, 1)

    fluxes = [sum([lows[c] for c in range(1, SPECIES)], lows[0])]
    fluxes += [lows[c] for c in range(SPECIES, COMPS)]
    jumps = [deltas[i] for i in range(COMPS - SPECIES + 1)]

    speed_max = spread_end(0, lambda rows: jnp.max(rows, axis=0, keepdims=True))
    ratio = (COURANT / speed_max).reshape(1, 1, ROW)

    def five(values):
        return [sum([values[c] for c in range(1, SPECIES)], values[0])] + [
            values[c] for c in range(SPECIES, COMPS)
        ]

    low_five = [u - ratio * f for u, f in zip(five(cons), fluxes)]
    d_five = [-(ratio * d) for d in jumps]
    low_safe, _, low_pressure = state_of(low_five[0], low_five[1:4], low_five[4])
    low_sigma = entropy(low_five[0], low_safe, low_pressure)
    d_rho = d_five[0]
    rho_scale = 1.0 / jnp.maximum(-d_rho, SLOPE_FLOOR)
    count = X * Y * Z * sizes[0] * sizes[1] * sizes[2]
    stat_lane = lax.broadcasted_iota(jnp.int32, (1, ROW), 1)

    def combine_stats(rows):
        return jnp.where(
            stat_lane < 2,
            jnp.min(rows, axis=0, keepdims=True),
            jnp.sum(rows, axis=0, keepdims=True),
        )

    def broadcast_stats(got):
        lowest_rho = got[0:1, 0:1].reshape(1, 1, 1)
        lowest_p = got[0:1, 1:2].reshape(1, 1, 1)
        spread = got[0:1, 2:3].reshape(1, 1, 1) * (1.0 / count) + SPREAD
        return lowest_rho, lowest_p, spread

    def next_blend(got, packed):
        t_density, rho_scale, t_p, p_scale, rho_bound, p_bound, mean_square, base = packed
        lowest_rho, lowest_p, spread = got
        rho_target = rho_bound - RELAX * jnp.maximum(rho_bound - lowest_rho, 0.0)
        p_target = p_bound - RELAX * jnp.maximum(p_bound - lowest_p, 0.0)
        step_rho = jnp.minimum(t_density - nodes(rho_target), 0.0) * rho_scale
        step_p = jnp.minimum(t_p - nodes(p_target), 0.0) * p_scale
        lowered = element(jnp.minimum(step_rho, step_p), jnp.minimum)
        cap = spread / (spread + mean_square)
        return jnp.maximum(jnp.minimum(cap, base + lowered), 0.0)

    per_edge = Z // (2 * P_SIZE)
    depth = 2 * X + 2 * EX

    def share(phase, fields):
        at = 0
        for value in fields:
            pk[phase, at : at + value.shape[0]] = value
            at += value.shape[0]
        slot = 16 + 6 * phase
        for side, k in ((0, 1), (1, -1)):
            if side == 0 or sizes[0] > 2:
                arrivals["b", phase, 0, side] = [
                    send(pk.at[phase], pnx.at[side, phase], slot + side, step(0, k))
                ]
            else:
                arrivals["b", phase, 0, side] = []
        for side, k in ((0, 1), (1, -1)):
            rows = pl.ds(Y - P_SIZE, P_SIZE) if side == 0 else pl.ds(0, P_SIZE)
            arrivals["b", phase, 1, side] = [
                send(pk.at[phase, :, rows], pny.at[phase, :, rows], slot + 2 + side, step(1, k))
            ]
        items = [value[x : x + 1] for value in fields for x in range(value.shape[0])]
        for v in range(pz.shape[1]):
            packed = jnp.zeros((1, Y, Z), jnp.float32)
            for j, item in enumerate(items[v * per_edge : (v + 1) * per_edge]):
                at = 2 * P_SIZE * j
                moved = roll(item, at + P_SIZE, 2)
                inside = (lane_index >= at) & (lane_index < at + 2 * P_SIZE)
                packed = jnp.where(inside, moved, packed)
            pz[phase, v] = packed[0]
        for side, k in ((0, 1), (1, -1)):
            arrivals["b", phase, 2, side] = [
                send(pz.at[phase], qz.at[side, phase], slot + 4 + side, step(2, k))
            ]

    def unpack(early, late):
        low_density, d_density, rho_bound, p_bound = early
        t_p, p_scale, mean_square, base = late
        t_density = low_density + nodes(base) * d_density
        scale = 1.0 / jnp.maximum(-d_density, SLOPE_FLOOR)
        return t_density, scale, t_p, p_scale, rho_bound, p_bound, mean_square, base

    def cut_fields(layer):
        ends = (0, X, 2 * X, 2 * X + EX, depth)
        return [layer(a, b) for a, b in zip(ends[:-1], ends[1:])]

    blend = None
    for newton in range(ITERS):
        blend_nodes = None if blend is None else nodes(blend)
        trial = [
            low + (d if blend is None else blend_nodes * d) for low, d in zip(low_five, d_five)
        ]
        t_density = trial[0]
        t_safe, t_vel, t_p = state_of(t_density, trial[1:4], trial[4])
        residual = entropy(t_density, t_safe, t_p) - low_sigma
        square = residual * residual
        stats = jnp.where(
            stat_lane == 0,
            total(t_density, jnp.minimum),
            jnp.where(stat_lane == 1, total(t_p, jnp.minimum), total(square, jnp.add)),
        )
        spread_start(newton + 1, 0, stats)
        if newton == ITERS - 2:
            share(0, (low_five[0], d_rho, rho_bound, p_bound))
        cross = t_vel[0] * d_five[1] + t_vel[1] * d_five[2] + t_vel[2] * d_five[3]
        speed2 = t_vel[0] * t_vel[0] + t_vel[1] * t_vel[1] + t_vel[2] * t_vel[2]
        slope = (GAMMA - 1.0) * (d_five[4] - cross + 0.5 * speed2 * d_rho)
        p_scale = 1.0 / jnp.maximum(-slope, SLOPE_FLOOR)
        mean_square = element(square, jnp.add) * (1.0 / (P_SIZE**3))
        base = jnp.ones((EX, Y, Z), jnp.float32) if blend is None else blend
        beside = {}
        if newton == ITERS - 1:
            share(1, (t_p, p_scale, mean_square, base))
            for copy in started:
                copy.wait_send()
            for turn in range(ITERS):
                spread_sent(turn)
            if relayed:

                @pl.when(origin)
                def _():
                    relay_copy.wait_send()

            def arrive_both(d):
                for phase in (0, 1):
                    for side in (0, 1):
                        arrive("b", phase, d, side)

            arrive_both(1)
            arrive_both(2)
            beside[1] = unpack(
                *[cut_fields(lambda a, b: pny[phase, a:b]) for phase in (0, 1)]
            )
            near = (lane_index & (2 * P_SIZE - 1)) < P_SIZE
            halves = []
            for phase in (0, 1):
                edges = [
                    jnp.where(near, qz[0, phase, v][None], qz[1, phase, v][None])
                    for v in range(pz.shape[1])
                ]
                items = [
                    roll(edges[j // per_edge], -(2 * P_SIZE * (j % per_edge) + P_SIZE), 2)
                    for j in range(depth)
                ]
                halves.append(cut_fields(lambda a, b: jnp.concatenate(items[a:b], axis=0)))
            beside[2] = unpack(*halves)
            arrive_both(0)
            for side in (0, 1):
                if side == 0 or sizes[0] > 2:
                    beside[0, side] = unpack(
                        *[cut_fields(lambda a, b: pnx[side, phase, a:b]) for phase in (0, 1)]
                    )
        got = broadcast_stats(spread_end(newton + 1, combine_stats))
        blend = next_blend(
            got, (t_density, rho_scale, t_p, p_scale, rho_bound, p_bound, mean_square, base)
        )

    beside = {key: next_blend(got, packed) for key, packed in beside.items()}
    beside.setdefault((0, 1), beside[0, 0])

    theta = []
    for d in (2, 1):
        above = roll(jnp.where(index[d] == 0, beside[d], blend), -1, d)
        below = roll(jnp.where(index[d] == extent[d] - 1, beside[d], blend), 1, d)
        theta.append((nodes(jnp.minimum(blend, above)), nodes(jnp.minimum(blend, below))))
    x_blend = joined(beside[0, 0][EX - 1 : EX], nodes(blend), beside[0, 1][0:1])
    x_theta = jnp.minimum(x_blend[:-1], x_blend[1:])
    for c in range(COMPS):
        faces = x_theta * dx[c]
        change = lows[c] + (faces[1:] - faces[:-1])
        for number in range(2):
            upper, lower = theta[number]
            change += upper * du[number, c] - lower * dw[number, c]
        out[c] = cons[c] - ratio * change

    pick_lanes = (
        lax.broadcasted_iota(jnp.int32, (Z, EZ), 1) * P_SIZE
        == lax.broadcasted_iota(jnp.int32, (Z, EZ), 0)
    ).astype(jnp.float32)
    for e in range(EX):
        few = jnp.dot(
            blend[e], pick_lanes, preferred_element_type=jnp.float32, precision=lax.Precision.HIGHEST
        )
        bl[e] = jnp.concatenate([few[j * P_SIZE : j * P_SIZE + 1] for j in range(EY)], axis=0)

    spread_sent(ITERS)


def store(state, weights, state_hbm, weights_hbm, sem):
    copies = [
        pltpu.make_async_copy(state, state_hbm, sem.at[0]),
        pltpu.make_async_copy(weights, weights_hbm, sem.at[1]),
    ]
    for copy in copies:
        copy.start()
    for copy in copies:
        copy.wait()


def solution(mesh):
    sizes = tuple(mesh.shape[name] for name in AXES)

    def local(species, velocity_in, pressure_in, wall_types):
        X, Y, Z = pressure_in.shape
        EX, EY, EZ = wall_types.shape[1:]
        packs = -(-COMPS // (Z // (4 * X)))
        depth = 2 * X + 2 * EX
        edge_packs = -(-depth // (Z // (2 * P_SIZE)))
        vmem = lambda *shape: pltpu.VMEM(shape, jnp.float32)
        reduce_scratch = []
        for _ in range(ITERS + 1):
            for group in reduce_groups(sizes):
                n = len(group_offsets(sizes, group))
                reduce_scratch += [
                    vmem(1, ROW),
                    vmem(n, ROW),
                    pltpu.SemaphoreType.DMA(()),
                    pltpu.SemaphoreType.DMA(()),
                ]
        state, weights = (
            pl.pallas_call(
                functools.partial(kernel, sizes),
                out_shape=[
                    pltpu.VMEM((COMPS, X, Y, Z), jnp.float32),
                    pltpu.VMEM((EX, EY, EZ), jnp.float32),
                ],
                in_specs=[pl.BlockSpec(memory_space=pltpu.HBM)] * 4,
                out_specs=[pl.BlockSpec(memory_space=pltpu.VMEM)] * 2,
                scratch_shapes=[
                    vmem(SPECIES, X, Y, Z),
                    vmem(3, X, Y, Z),
                    vmem(X, Y, Z),
                    pltpu.VMEM((3, EX, EY, EZ), jnp.int32),
                    pltpu.SemaphoreType.DMA((4,)),
                    vmem(2, SPECIES, 2, Y, Z),
                    vmem(2, 3, 2, Y, Z),
                    vmem(2, 2, Y, Z),
                    vmem(2, COMPS, 2 * X, Z),
                    vmem(2, COMPS, 2 * X, Z),
                    vmem(COMPS, X, Y, Z),
                    vmem(packs, Y, Z),
                    vmem(2, packs, Y, Z),
                    vmem(3, EX, Y, Z),
                    vmem(2, 3, EX, Y, Z),
                    vmem(2, depth, Y, Z),
                    vmem(2, 2, depth, Y, Z),
                    vmem(2, depth, Y, Z),
                    vmem(2, edge_packs, Y, Z),
                    vmem(2, 2, edge_packs, Y, Z),
                    vmem(COMPS, X + 1, Y, Z),
                    vmem(2, COMPS, X, Y, Z),
                    vmem(2, COMPS, X, Y, Z),
                    vmem(COMPS, X, Y, Z),
                    vmem(COMPS - SPECIES + 1, X, Y, Z),
                    pltpu.SemaphoreType.DMA((28,)),
                    pltpu.SemaphoreType.DMA((28,)),
                    pltpu.SemaphoreType.REGULAR((len(halo_links(sizes)),)),
                    pltpu.SemaphoreType.REGULAR,
                    vmem(1, ROW),
                    pltpu.SemaphoreType.DMA(()),
                    pltpu.SemaphoreType.DMA(()),
                ]
                + reduce_scratch,
                compiler_params=pltpu.CompilerParams(collective_id=0, has_side_effects=True),
            )(species, velocity_in, pressure_in, wall_types)
        )
        return tuple(
            pl.pallas_call(
                store,
                out_shape=[
                    jax.ShapeDtypeStruct((COMPS, X, Y, Z), jnp.float32),
                    jax.ShapeDtypeStruct((EX, EY, EZ), jnp.float32),
                ],
                in_specs=[pl.BlockSpec(memory_space=pltpu.VMEM)] * 2,
                out_specs=[pl.BlockSpec(memory_space=pltpu.HBM)] * 2,
                scratch_shapes=[pltpu.SemaphoreType.DMA((2,))],
            )(*[pltpu.with_memory_space_constraint(v, pltpu.VMEM) for v in (state, weights)])
        )

    in_specs = (
        P(None, "gx", "gy", "gz"),
        P(None, "gx", "gy", "gz"),
        P("gx", "gy", "gz"),
        P(None, "gx", "gy", "gz"),
    )
    out_specs = (P(None, "gx", "gy", "gz"), P("gx", "gy", "gz"))
    return jax.shard_map(local, mesh=mesh, in_specs=in_specs, out_specs=out_specs, check_vma=False)
```

```python
import functools
import itertools

import jax
import jax.numpy as jnp
from jax import lax
from jax.experimental import pallas as pl
from jax.experimental.pallas import tpu as pltpu
from jax.sharding import PartitionSpec as P

SPECIES = 5
P_SIZE = 4
ITERS = 2
GAMMA = 1.4
COURANT = 0.4
FLOOR = 0.1
SLOPE_FLOOR = 0.01
SPREAD = 0.002
RELAX = 0.1

COMPS = SPECIES + 4
AXES = ("gx", "gy", "gz")
ROW = 128
DIRECT = 64
MESH = pl.DeviceIdType.MESH


def reduce_groups(sizes):
    if sizes[0] * sizes[1] * sizes[2] <= DIRECT:
        return [(0, 1, 2)]
    return [(2,), (1,), (0,)]


def group_offsets(sizes, group):
    spans = [range(sizes[d]) if d in group else (0,) for d in range(3)]
    far = lambda off: sum(min(off[d], sizes[d] - off[d]) for d in range(3))
    return sorted(itertools.product(*spans), key=far)


def halo_links(sizes):
    return [(d, k) for d in range(3) for k in ((1,) if sizes[d] == 2 else (1, -1))]


def conserved_of(inputs):
    species, velocity, pressure = inputs[:SPECIES], inputs[SPECIES : SPECIES + 3], inputs[-1]
    density = sum(species[1:], species[0])
    square = velocity[0] * velocity[0] + velocity[1] * velocity[1] + velocity[2] * velocity[2]
    energy = pressure * (1.0 / (GAMMA - 1.0)) + 0.5 * density * square
    return list(species) + [density * v for v in velocity] + [energy]


def primitives(cons):
    density = sum(cons[1:SPECIES], cons[0])
    safe = jnp.maximum(density, FLOOR)
    inverse = 1.0 / safe
    momentum = cons[SPECIES : SPECIES + 3]
    velocity = [m * inverse for m in momentum]
    kinetic = momentum[0] * velocity[0] + momentum[1] * velocity[1] + momentum[2] * velocity[2]
    pressure = (GAMMA - 1.0) * (cons[SPECIES + 3] - 0.5 * kinetic)
    return density, safe, inverse, velocity, pressure


def state_of(density, momentum, energy):
    safe = jnp.maximum(density, FLOOR)
    inverse = 1.0 / safe
    velocity = [m * inverse for m in momentum]
    kinetic = momentum[0] * velocity[0] + momentum[1] * velocity[1] + momentum[2] * velocity[2]
    pressure = (GAMMA - 1.0) * (energy - 0.5 * kinetic)
    return safe, velocity, pressure


def sound_of(inverse, pressure):
    return jnp.sqrt(GAMMA * jnp.maximum(pressure, FLOOR) * inverse)


def entropy(density, safe, pressure):
    return density * (jnp.log(jnp.maximum(pressure, FLOOR)) - GAMMA * jnp.log(safe))


def flux_term(cons, velocity, pressure, comp, d):
    term = cons[comp] * velocity[d]
    if comp == SPECIES + d:
        term = term + pressure
    if comp == SPECIES + 3:
        term = term + pressure * velocity[d]
    return term


def face_pair(mm, left, right, pp, jump, rate, wall, wall_value):
    both = left + right
    high = (7.0 * both - (mm + pp)) * (1.0 / 12.0)
    low = 0.5 * both - rate * jump
    keep = 0.0 if wall_value is None else wall_value
    diff = jnp.where(wall, 0.0, high - low)
    return jnp.where(wall, keep, low), diff


def kernel(
    sizes, sp_hbm, ve_hbm, pr_hbm, wa_hbm, out, bl, inp, wa, load_sem,
    xh, ys, yr, hy, zs, zr, es, er, pk, pnx, pny, pz, qz, dx, du, dw, lows, deltas,
    sent_sem, came_sem, near_sem, all_sem, relay, relay_sem, row_sent, row_came, *rows_scratch
):
    X, Y, Z = inp.shape[1:]
    EX, EY, EZ = wa.shape[1:]
    loads = [
        pltpu.make_async_copy(sp_hbm, inp.at[:SPECIES], load_sem.at[0]),
        pltpu.make_async_copy(ve_hbm, inp.at[SPECIES : SPECIES + 3], load_sem.at[0]),
        pltpu.make_async_copy(pr_hbm, inp.at[SPECIES + 3], load_sem.at[0]),
        pltpu.make_async_copy(wa_hbm, wa, load_sem.at[1]),
    ]
    for copy in loads:
        copy.start()
    me = [lax.axis_index(name) for name in AXES]
    groups = reduce_groups(sizes)

    place = [[me[d]] + [lax.rem(me[d] + k, sizes[d]) for k in range(1, sizes[d])] for d in range(3)]

    def device(off):
        return tuple(place[d][off[d]] for d in range(3))

    def step(d, k):
        return tuple(k % sizes[d] if a == d else 0 for a in range(3))

    relayed = len(groups) == 1
    if relayed:
        rows_scratch[1][...] = jnp.zeros_like(rows_scratch[1])

    def traced(flag):
        return jnp.where(flag, 1, 0).astype(jnp.int32)

    links = halo_links(sizes)
    near = {link: near_sem.at[i] for i, link in enumerate(links)}

    def later(d, k):
        return me[d] != sizes[d] - 1 if k == 1 else me[d] == 0

    def neighbour(d, k):
        return device(step(d, k))

    corner = tuple(n - 1 for n in sizes)
    is_corner = (me[0] == corner[0]) & (me[1] == corner[1]) & (me[2] == corner[2])
    devices = sizes[0] * sizes[1] * sizes[2]
    barrier = pltpu.get_barrier_semaphore()

    @pl.when(jnp.logical_not(is_corner))
    def _():
        pl.semaphore_signal(barrier, inc=1, device_id=corner, device_id_type=MESH)

    expected = jnp.where(is_corner, devices - 1, 0).astype(jnp.int32)
    for d, k in links:

        @pl.when(later(d, k))
        def _(d=d, k=k):
            pl.semaphore_signal(barrier, inc=1, device_id=neighbour(d, k), device_id_type=MESH)

        expected = expected + 1 - traced(later(d, k))

    @pl.when(expected > 0)
    def _():
        pl.semaphore_wait(barrier, expected)

    for d, k in links:
        back = (d, k if sizes[d] == 2 else -k)

        @pl.when(jnp.logical_not(later(d, k)))
        def _(d=d, k=k, back=back):
            pl.semaphore_signal(
                near[back], inc=1, device_id=neighbour(d, k), device_id_type=MESH
            )

    @pl.when(is_corner)
    def _():
        def tell(i, carry):
            z = lax.rem(i, sizes[2])
            y = lax.rem(lax.div(i, sizes[2]), sizes[1])
            x = lax.div(i, sizes[2] * sizes[1])
            pl.semaphore_signal(all_sem, inc=1, device_id=(x, y, z), device_id_type=MESH)
            return carry

        if devices <= DIRECT:
            for at in itertools.product(*[range(n) for n in sizes]):
                if at != corner:
                    pl.semaphore_signal(all_sem, inc=1, device_id=at, device_id_type=MESH)
        else:
            lax.fori_loop(0, devices - 1, tell, 0)

    def await_near(d, k):
        @pl.when(later(d, k))
        def _():
            pl.semaphore_wait(near[d, k], 1)

    def await_all():
        @pl.when(jnp.logical_not(is_corner))
        def _():
            pl.semaphore_wait(all_sem, 1)

    pltpu.make_async_copy(inp, inp, load_sem.at[0]).wait()

    origin = (me[0] == 0) & (me[1] <= 1)
    next_up = origin & (me[2] == 1)
    origin = origin & (me[2] == 0)
    plane_rows = ((origin, devices - 2), (jnp.logical_not(origin), devices - 3))
    if relayed:
        relay_copy = pltpu.make_async_remote_copy(
            src_ref=rows_scratch[0],
            dst_ref=relay,
            send_sem=row_sent,
            recv_sem=relay_sem,
            device_id=neighbour(2, 1),
            device_id_type=MESH,
        )

    def speed_out():
        await_all()
        if not relayed:
            spread_start(0, 0, speed_row)
            return

        @pl.when(next_up)
        def _():
            relay_copy.wait_recv()
            spread_start(0, 0, jnp.maximum(speed_row, relay[...]))

        @pl.when(jnp.logical_not(origin | next_up))
        def _():
            spread_start(0, 0, speed_row)

    def row_parts(turn, stage):
        base = 2 * (turn * len(groups) + stage)
        mine, buf = rows_scratch[base : base + 2]
        return mine, buf, row_came.at[turn % 2 * len(groups) + stage]

    def spread_copy(turn, stage, i):
        mine, buf, came = row_parts(turn, stage)
        group = groups[stage]
        off = group_offsets(sizes, group)[i]
        there = tuple(
            lax.rem(sizes[d] - 1 - me[d] + off[d], sizes[d]) if d in group else me[d]
            for d in range(3)
        )
        can_be_me = all((off[d] + 1 - sizes[d]) % 2 == 0 or sizes[d] % 2 for d in group)
        copy = pltpu.make_async_remote_copy(
            src_ref=mine,
            dst_ref=buf.at[pl.ds(i, 1)],
            send_sem=row_sent,
            recv_sem=came,
            device_id=there,
            device_id_type=MESH,
        )
        return copy, can_be_me, functools.reduce(lambda a, b: a & b, [t == m for t, m in zip(there, me)])

    def spread_start(turn, stage, row):
        if turn or stage:
            before = turn * len(groups) + stage - 1
            spread_sent(before // len(groups), before % len(groups))
        mine, buf, _ = row_parts(turn, stage)
        mine[...] = row
        for i in range(buf.shape[0]):
            copy, can_be_me, is_me = spread_copy(turn, stage, i)
            if not can_be_me:
                copy.start()
                continue

            @pl.when(jnp.logical_not(is_me))
            def _(copy=copy):
                copy.start()

            @pl.when(is_me)
            def _(i=i):
                buf[i : i + 1] = row

    def spread_whole(turn, stage, rows=None):
        _, buf, came = row_parts(turn, stage)
        rows = buf.at[pl.ds(0, rows or buf.shape[0] - 1)]
        return pltpu.make_async_remote_copy(
            src_ref=rows,
            dst_ref=rows,
            send_sem=row_sent,
            recv_sem=came,
            device_id=device((1, 1, 1)),
            device_id_type=MESH,
        )

    def spread_end(turn, combine):
        for stage in range(len(groups)):
            if stage > 0:
                spread_start(turn, stage, row)
            if turn == 0 and relayed:
                for flag, rows in plane_rows:

                    @pl.when(flag)
                    def _(rows=rows):
                        spread_whole(turn, stage, rows).wait_recv()
            else:
                spread_whole(turn, stage).wait_recv()
            row = combine(row_parts(turn, stage)[1][...])
        return row

    def spread_sent(turn, stage):
        if turn == 0 and relayed:

            @pl.when(jnp.logical_not(origin))
            def _():
                spread_whole(turn, stage).wait_send()

            @pl.when(origin)
            def _():
                relay_copy.wait_send()

        else:
            spread_whole(turn, stage).wait_send()

    row_index = lax.broadcasted_iota(jnp.int32, (1, Y, Z), 1)
    lane_index = lax.broadcasted_iota(jnp.int32, (1, Y, Z), 2)
    index = {1: row_index, 2: lane_index}
    extent = {1: Y, 2: Z}

    def roll(value, shift, axis):
        return pltpu.roll(value, shift % value.shape[axis], axis)

    def mesh_group(value, axis, op):
        for s in (1, 2):
            low = (index[axis] & s) == 0
            value = op(value, jnp.where(low, roll(value, -s, axis), roll(value, s, axis)))
        return value

    def lane_group(value, op):
        place = lane_index & (P_SIZE - 1)
        for s in range(1, P_SIZE):
            ahead = roll(value, -s, 2)
            behind = roll(value, P_SIZE - s, 2)
            turned = jnp.where(place < P_SIZE - s, ahead, behind)
            whole = turned if s == 1 else op(whole, turned)
        return op(value, whole)

    def element(value, op):
        parts = value.reshape(EX, P_SIZE, Y, Z)
        value = op(op(parts[:, 0], parts[:, 1]), op(parts[:, 2], parts[:, 3]))
        return lane_group(mesh_group(value, 1, op), op)

    def nodes(value):
        return jnp.broadcast_to(value[:, None], (EX, P_SIZE, Y, Z)).reshape(X, Y, Z)

    def total(value, op):
        value = functools.reduce(op, [value[x] for x in range(X)])
        value = {jnp.minimum: jnp.min, jnp.maximum: jnp.max, jnp.add: jnp.sum}[op](
            value, axis=0, keepdims=True
        )
        return {jnp.minimum: jnp.min, jnp.maximum: jnp.max, jnp.add: jnp.sum}[op](
            value, axis=1, keepdims=True
        )

    late = me[2] == corner[2]
    last_x = me[0] == corner[0]
    last_chip = last_x & (me[1] >= corner[1] - 1) & late
    first_sides = ((0, 1),) if sizes[0] == 2 else ((0, 1), (1, -1))
    packs = zs.shape[0] - EX
    body = COMPS * 2 * X

    def remote(src, dst, sent, came, off):
        return pltpu.make_async_remote_copy(
            src_ref=src,
            dst_ref=dst,
            send_sem=sent_sem.at[sent],
            recv_sem=came_sem.at[came],
            device_id=device(off),
            device_id_type=MESH,
        )

    landing = {
        "x": (xh, 0, 0),
        "y": (yr, 1, 1),
        "z": (zr, 2, 2),
        "e": (er, 3, 3),
        ("b", 0): (pnx, 0, 4),
        ("b", 1): (pny.at[:, :, pl.ds(0, 2 * P_SIZE)], 1, 5),
        ("b", 2): (qz, 2, 6),
    }

    def whole(key):
        ref, sent, came = landing[key]
        return remote(ref, ref, sent, came, step(2, 1))

    def arrive(key):
        whole(key).wait_recv()

    def sent_all(key):
        whole(key).wait_send()

    def send_x():
        for d, k in links:
            if d == 0:
                await_near(d, k)
        for side, k in ((0, 1), (1, -1)):
            at = X - 2 if side == 0 else 0
            remote(inp.at[:, at : at + 2], xh.at[side], 0, 0, step(0, k)).start()

    def send_e():
        for side, k in first_sides:
            remote(es, er.at[side], 3, 3, step(0, k)).start()

    def send_y():
        for side, k in ((0, 1), (1, -1)):
            if (1, k) in links:
                await_near(1, k)
            remote(ys.at[side], yr.at[side], 1, 1, step(1, k)).start()

    def send_z():
        for side, k in ((0, 1), (1, -1)):
            if (2, k) in links:
                await_near(2, k)
            remote(zs, zr.at[side], 2, 2, step(2, k)).start()
            if side == 0 and relayed:

                @pl.when(origin)
                def _():
                    rows_scratch[0][...] = speed_row
                    relay_copy.start()

    @pl.when(late & last_x & jnp.logical_not(last_chip))
    def _():
        send_x()

    own_inputs = [inp[c] for c in range(COMPS)]

    cons = conserved_of(own_inputs)
    density, _, inverse, velocity, pressure = primitives(cons)
    sound = sound_of(inverse, pressure)
    speed = jnp.abs(velocity[0]) + jnp.abs(velocity[1]) + jnp.abs(velocity[2]) + 3.0 * sound
    speed_row = jnp.broadcast_to(total(speed, jnp.maximum), (1, ROW))

    @pl.when(last_chip)
    def _():
        speed_out()
        send_x()

    for c in range(COMPS):
        for x in range(X):
            at = 2 * (c * X + x)
            ys[0, at : at + 2, :] = own_inputs[c][x, Y - 2 : Y, :]
            ys[1, at : at + 2, :] = own_inputs[c][x, 0:2, :]
    per_pack = Z // (4 * X)
    for v in range(packs):
        packed = jnp.zeros((1, Y, Z), jnp.float32)
        for c in range(v * per_pack, min((v + 1) * per_pack, COMPS)):
            for x in range(X):
                at = ((c - v * per_pack) * X + x) * 4
                moved = roll(own_inputs[c][x : x + 1], at + 2, 2)
                packed = jnp.where((lane_index >= at) & (lane_index < at + 4), moved, packed)
        zs[v] = packed[0]

    rho_min = element(density, jnp.minimum)
    p_min = element(pressure, jnp.minimum)
    widen = (
        lax.broadcasted_iota(jnp.int32, (EZ, Z), 1) // P_SIZE
        == lax.broadcasted_iota(jnp.int32, (EZ, Z), 0)
    ).astype(jnp.float32)
    heighten = (
        lax.broadcasted_iota(jnp.int32, (Y, EY), 0) // P_SIZE
        == lax.broadcasted_iota(jnp.int32, (Y, EY), 1)
    ).astype(jnp.float32)
    loads[3].wait()
    walls = []
    for d in range(3):
        layers = []
        for e in range(EX):
            flags = wa[d, e].astype(jnp.float32)
            flags = jnp.dot(flags, widen, preferred_element_type=jnp.float32)
            layers.append(jnp.dot(heighten, flags, preferred_element_type=jnp.float32)[None])
        walls.append(jnp.concatenate(layers, axis=0))
        turn_row = row_index & (P_SIZE - 1)
        fields = jnp.where(turn_row == 0, rho_min, jnp.where(turn_row == 1, p_min, walls[d]))
        if d == 0:
            es[...] = fields
        elif d == 1:
            for side in (0, 1):
                ys[side, body : body + EX * Y, :] = fields.reshape(EX * Y, Z)
        else:
            zs[packs : packs + EX] = fields

    def spread_rows(value, which):
        value = jnp.where((row_index & (P_SIZE - 1)) == which, value, jnp.inf)
        return mesh_group(value, 1, jnp.minimum)

    def edge(side, d, which):
        if d == 0:
            fields = er[0 if sizes[0] == 2 else side]
        elif d == 1:
            fields = yr[side, body : body + EX * Y, :].reshape(EX, Y, Z)
        else:
            fields = zr[side, packs : packs + EX]
        return spread_rows(fields, which)

    @pl.when(jnp.logical_not(late))
    def _():
        send_x()
        send_e()
        send_y()

    send_z()

    @pl.when(late & jnp.logical_not(last_x))
    def _():
        send_x()

    @pl.when(late)
    def _():
        send_e()
        send_y()

    @pl.when(jnp.logical_not(last_chip))
    def _():
        speed_out()

    def cyclic_fluxes(d, halo_inputs, number, first):
        n = extent[d]
        ix = index[d]
        halo = conserved_of(halo_inputs)
        _, _, h_inv, h_vel, h_p = primitives(halo)
        h_rate = jnp.abs(h_vel[d]) + sound_of(h_inv, h_p)
        rate = jnp.abs(velocity[d]) + sound

        def beside(value, beyond, k):
            edge_of = ix < k if k > 0 else ix >= n + k
            return roll(jnp.where(edge_of, beyond, value), -k, d)

        shifts = (-2, -1, 1, 2)
        along = {k: {d: beside(velocity[d], h_vel[d], k)} for k in shifts}
        p_at = {k: beside(pressure, h_p, k) for k in shifts}
        flag = roll(jnp.where(ix == 0, edge(1, d, 2), walls[d]), -1, d)
        ends = ix & (P_SIZE - 1)
        wall = nodes(jnp.where(ends == P_SIZE - 1, flag, 0.0)) > 0.5
        wall_low = nodes(jnp.where(ends == 0, walls[d], 0.0)) > 0.5
        half_rate = 0.5 * jnp.maximum(rate, beside(rate, h_rate, 1))
        half_low = 0.5 * jnp.maximum(beside(rate, h_rate, -1), rate)
        wall_p = 0.5 * (pressure + p_at[1])
        wall_p_low = 0.5 * (p_at[-1] + pressure)
        for c in range(COMPS):
            u_at = {k: beside(cons[c], halo[c], k) for k in shifts}
            f_at = {k: flux_term({c: u_at[k]}, along[k], p_at[k], c, d) for k in shifts}
            f = flux_term(cons, velocity, pressure, c, d)
            is_normal = c == SPECIES + d
            low, diff = face_pair(
                f_at[-1],
                f,
                f_at[1],
                f_at[2],
                u_at[1] - cons[c],
                half_rate,
                wall,
                wall_p if is_normal else None,
            )
            before_low, before_diff = face_pair(
                f_at[-2],
                f_at[-1],
                f,
                f_at[1],
                cons[c] - u_at[-1],
                half_low,
                wall_low,
                wall_p_low if is_normal else None,
            )
            du[number, c] = diff
            dw[number, c] = before_diff
            slot = max(c - SPECIES + 1, 0)
            if first:
                lows[c] = low - before_low
            else:
                lows[c] += low - before_low
            if first and c in (0, *range(SPECIES, COMPS)):
                deltas[slot] = diff - before_diff
            else:
                deltas[slot] += diff - before_diff

    arrive("y")
    for c in range(COMPS):
        hy[c] = own_inputs[c]
        for x in range(X):
            at = 2 * (c * X + x)
            hy[c, x, Y - 2 : Y, :] = yr[0, at : at + 2, :]
            hy[c, x, 0:2, :] = yr[1, at : at + 2, :]
    cyclic_fluxes(1, [hy[c] for c in range(COMPS)], 1, True)

    arrive("z")
    merged = [
        jnp.where((lane_index & 3) < 2, zr[0, v][None], zr[1, v][None]) for v in range(packs)
    ]
    z_halo = []
    for c in range(COMPS):
        layers = []
        for x in range(X):
            at = ((c % per_pack) * X + x) * 4
            layers.append(roll(merged[c // per_pack], -(at + 2), 2))
        z_halo.append(jnp.concatenate(layers, axis=0))
    cyclic_fluxes(2, z_halo, 0, False)

    arrive("x")
    arrive("e")
    sides = []
    for side in (0, 1):
        halo = conserved_of([xh[side, c] for c in range(COMPS)])
        _, _, h_inv, h_vel, h_p = primitives(halo)
        sides.append((halo, h_vel, h_p, jnp.abs(h_vel[0]) + sound_of(h_inv, h_p)))

    def joined(below, own, above):
        return jnp.concatenate([below, own, above], axis=0)

    rate = joined(sides[0][3], jnp.abs(velocity[0]) + sound, sides[1][3])
    p_ext = joined(sides[0][2], pressure, sides[1][2])
    half_rate = 0.5 * jnp.maximum(rate[1 : X + 2], rate[2 : X + 3])
    wall_p = 0.5 * (p_ext[1 : X + 2] + p_ext[2 : X + 3])
    planes = []
    for x in range(-1, X):
        if (x + 1) % P_SIZE:
            planes.append(jnp.zeros((1, Y, Z), jnp.float32))
        elif x == X - 1:
            planes.append(edge(1, 0, 2)[0:1])
        else:
            e = (x + 1) // P_SIZE
            planes.append(walls[0][e : e + 1])
    wall = jnp.concatenate(planes, axis=0) > 0.5
    for c in range(COMPS):
        f = joined(
            flux_term(sides[0][0], sides[0][1], sides[0][2], c, 0),
            flux_term(cons, velocity, pressure, c, 0),
            flux_term(sides[1][0], sides[1][1], sides[1][2], c, 0),
        )
        u = joined(sides[0][0][c], cons[c], sides[1][0][c])
        low, diff = face_pair(
            f[0 : X + 1],
            f[1 : X + 2],
            f[2 : X + 3],
            f[3 : X + 4],
            u[2 : X + 3] - u[1 : X + 2],
            half_rate,
            wall,
            wall_p if c == SPECIES else None,
        )
        dx[c] = diff
        lows[c] += low[1:] - low[:-1]
        deltas[max(c - SPECIES + 1, 0)] += diff[1:] - diff[:-1]

    def bound(own, which):
        best = own
        for d in (1, 2):
            n = extent[d]
            up = jnp.where(index[d] < P_SIZE, edge(1, d, which), own)
            down = jnp.where(index[d] >= n - P_SIZE, edge(0, d, which), own)
            best = jnp.minimum(best, jnp.minimum(roll(up, -P_SIZE, d), roll(down, P_SIZE, d)))
        chain = joined(edge(0, 0, which)[EX - 1 : EX], own, edge(1, 0, which)[0:1])
        return jnp.minimum(best, jnp.minimum(chain[:EX], chain[2:]))

    rho_bound = bound(rho_min, 0)
    p_bound = bound(p_min, 1)

    fluxes = [sum([lows[c] for c in range(1, SPECIES)], lows[0])]
    fluxes += [lows[c] for c in range(SPECIES, COMPS)]
    jumps = [deltas[i] for i in range(COMPS - SPECIES + 1)]

    speed_max = spread_end(0, lambda rows: jnp.max(rows, axis=0, keepdims=True))
    ratio = (COURANT / speed_max).reshape(1, 1, ROW)

    def five(values):
        return [sum([values[c] for c in range(1, SPECIES)], values[0])] + [
            values[c] for c in range(SPECIES, COMPS)
        ]

    low_five = [u - ratio * f for u, f in zip(five(cons), fluxes)]
    d_five = [-(ratio * d) for d in jumps]
    low_safe, _, low_pressure = state_of(low_five[0], low_five[1:4], low_five[4])
    low_sigma = entropy(low_five[0], low_safe, low_pressure)
    d_rho = d_five[0]
    rho_scale = 1.0 / jnp.maximum(-d_rho, SLOPE_FLOOR)
    count = X * Y * Z * sizes[0] * sizes[1] * sizes[2]
    stat_lane = lax.broadcasted_iota(jnp.int32, (1, ROW), 1)

    def combine_stats(rows):
        return jnp.where(
            stat_lane < 2,
            jnp.min(rows, axis=0, keepdims=True),
            jnp.sum(rows, axis=0, keepdims=True),
        )

    def broadcast_stats(got):
        lowest_rho = got[0:1, 0:1].reshape(1, 1, 1)
        lowest_p = got[0:1, 1:2].reshape(1, 1, 1)
        spread = got[0:1, 2:3].reshape(1, 1, 1) * (1.0 / count) + SPREAD
        return lowest_rho, lowest_p, spread

    def next_blend(got, packed):
        t_density, rho_scale, t_p, p_scale, rho_bound, p_bound, mean_square, base = packed
        lowest_rho, lowest_p, spread = got
        rho_target = rho_bound - RELAX * jnp.maximum(rho_bound - lowest_rho, 0.0)
        p_target = p_bound - RELAX * jnp.maximum(p_bound - lowest_p, 0.0)
        step_rho = jnp.minimum(t_density - nodes(rho_target), 0.0) * rho_scale
        step_p = jnp.minimum(t_p - nodes(p_target), 0.0) * p_scale
        lowered = element(jnp.minimum(step_rho, step_p), jnp.minimum)
        cap = spread / (spread + mean_square)
        return jnp.maximum(jnp.minimum(cap, base + lowered), 0.0)

    per_edge = Z // (2 * P_SIZE)
    depth = 2 * X + 2 * EX

    def share(phase, fields):
        at = 0
        for value in fields:
            pk[phase, at : at + value.shape[0]] = value
            at += value.shape[0]
        for side, k in first_sides:
            remote(pk.at[phase], pnx.at[side, phase], 0, 4, step(0, k)).start()
        for side, k in ((0, 1), (1, -1)):
            rows = pl.ds(Y - P_SIZE, P_SIZE) if side == 0 else pl.ds(0, P_SIZE)
            remote(pk.at[phase, :, rows], pny.at[phase, :, rows], 1, 5, step(1, k)).start()
        items = [value[x : x + 1] for value in fields for x in range(value.shape[0])]
        for v in range(pz.shape[1]):
            packed = jnp.zeros((1, Y, Z), jnp.float32)
            for j, item in enumerate(items[v * per_edge : (v + 1) * per_edge]):
                at = 2 * P_SIZE * j
                moved = roll(item, at + P_SIZE, 2)
                inside = (lane_index >= at) & (lane_index < at + 2 * P_SIZE)
                packed = jnp.where(inside, moved, packed)
            pz[phase, v] = packed[0]
        for side, k in ((0, 1), (1, -1)):
            remote(pz.at[phase], qz.at[side, phase], 2, 6, step(2, k)).start()

    def unpack(early, late):
        low_density, d_density, rho_bound, p_bound = early
        t_p, p_scale, mean_square, base = late
        t_density = low_density + nodes(base) * d_density
        scale = 1.0 / jnp.maximum(-d_density, SLOPE_FLOOR)
        return t_density, scale, t_p, p_scale, rho_bound, p_bound, mean_square, base

    def cut_fields(layer):
        ends = (0, X, 2 * X, 2 * X + EX, depth)
        return [layer(a, b) for a, b in zip(ends[:-1], ends[1:])]

    blend = None
    for newton in range(ITERS):
        blend_nodes = None if blend is None else nodes(blend)
        trial = [
            low + (d if blend is None else blend_nodes * d) for low, d in zip(low_five, d_five)
        ]
        t_density = trial[0]
        t_safe, t_vel, t_p = state_of(t_density, trial[1:4], trial[4])
        residual = entropy(t_density, t_safe, t_p) - low_sigma
        square = residual * residual
        stats = jnp.where(
            stat_lane == 0,
            total(t_density, jnp.minimum),
            jnp.where(stat_lane == 1, total(t_p, jnp.minimum), total(square, jnp.add)),
        )
        spread_start(newton + 1, 0, stats)
        if newton == ITERS - 2:
            for key in ("x", "y", "z", "e"):
                sent_all(key)
            share(0, (low_five[0], d_rho, rho_bound, p_bound))
        cross = t_vel[0] * d_five[1] + t_vel[1] * d_five[2] + t_vel[2] * d_five[3]
        speed2 = t_vel[0] * t_vel[0] + t_vel[1] * t_vel[1] + t_vel[2] * t_vel[2]
        slope = (GAMMA - 1.0) * (d_five[4] - cross + 0.5 * speed2 * d_rho)
        p_scale = 1.0 / jnp.maximum(-slope, SLOPE_FLOOR)
        mean_square = element(square, jnp.add) * (1.0 / (P_SIZE**3))
        base = jnp.ones((EX, Y, Z), jnp.float32) if blend is None else blend
        beside = {}
        if newton == ITERS - 1:
            share(1, (t_p, p_scale, mean_square, base))
            for d in range(3):
                sent_all(("b", d))

            arrive(("b", 1))
            arrive(("b", 2))
            beside[1] = unpack(
                *[cut_fields(lambda a, b: pny[phase, a:b]) for phase in (0, 1)]
            )
            near = (lane_index & (2 * P_SIZE - 1)) < P_SIZE
            halves = []
            for phase in (0, 1):
                edges = [
                    jnp.where(near, qz[0, phase, v][None], qz[1, phase, v][None])
                    for v in range(pz.shape[1])
                ]
                items = [
                    roll(edges[j // per_edge], -(2 * P_SIZE * (j % per_edge) + P_SIZE), 2)
                    for j in range(depth)
                ]
                halves.append(cut_fields(lambda a, b: jnp.concatenate(items[a:b], axis=0)))
            beside[2] = unpack(*halves)
            arrive(("b", 0))
            for side in (0, 1):
                if side == 0 or sizes[0] > 2:
                    beside[0, side] = unpack(
                        *[cut_fields(lambda a, b: pnx[side, phase, a:b]) for phase in (0, 1)]
                    )
        got = broadcast_stats(spread_end(newton + 1, combine_stats))
        blend = next_blend(
            got, (t_density, rho_scale, t_p, p_scale, rho_bound, p_bound, mean_square, base)
        )

    beside = {key: next_blend(got, packed) for key, packed in beside.items()}
    beside.setdefault((0, 1), beside[0, 0])

    theta = []
    for d in (2, 1):
        above = roll(jnp.where(index[d] == 0, beside[d], blend), -1, d)
        below = roll(jnp.where(index[d] == extent[d] - 1, beside[d], blend), 1, d)
        theta.append((nodes(jnp.minimum(blend, above)), nodes(jnp.minimum(blend, below))))
    x_blend = joined(beside[0, 0][EX - 1 : EX], nodes(blend), beside[0, 1][0:1])
    x_theta = jnp.minimum(x_blend[:-1], x_blend[1:])
    for c in range(COMPS):
        faces = x_theta * dx[c]
        change = lows[c] + (faces[1:] - faces[:-1])
        for number in range(2):
            upper, lower = theta[number]
            change += upper * du[number, c] - lower * dw[number, c]
        out[c] = cons[c] - ratio * change

    pick_lanes = (
        lax.broadcasted_iota(jnp.int32, (Z, EZ), 1) * P_SIZE
        == lax.broadcasted_iota(jnp.int32, (Z, EZ), 0)
    ).astype(jnp.float32)
    for e in range(EX):
        few = jnp.dot(
            blend[e], pick_lanes, preferred_element_type=jnp.float32, precision=lax.Precision.HIGHEST
        )
        bl[e] = jnp.concatenate([few[j * P_SIZE : j * P_SIZE + 1] for j in range(EY)], axis=0)

    spread_sent(ITERS, len(groups) - 1)


def store(state, weights, state_hbm, weights_hbm, sem):
    copies = [
        pltpu.make_async_copy(state, state_hbm, sem.at[0]),
        pltpu.make_async_copy(weights, weights_hbm, sem.at[1]),
    ]
    for copy in copies:
        copy.start()
    for copy in copies:
        copy.wait()


def solution(mesh):
    sizes = tuple(mesh.shape[name] for name in AXES)

    def local(species, velocity_in, pressure_in, wall_types):
        X, Y, Z = pressure_in.shape
        EX, EY, EZ = wall_types.shape[1:]
        packs = -(-COMPS // (Z // (4 * X)))
        depth = 2 * X + 2 * EX
        edge_packs = -(-depth // (Z // (2 * P_SIZE)))
        vmem = lambda *shape: pltpu.VMEM(shape, jnp.float32)
        groups = reduce_groups(sizes)
        dma = pltpu.SemaphoreType.DMA
        sides = 1 if sizes[0] == 2 else 2
        rows_scratch = []
        for _ in range(ITERS + 1):
            for group in groups:
                rows_scratch += [vmem(1, ROW), vmem(len(group_offsets(sizes, group)), ROW)]
        state, weights = (
            pl.pallas_call(
                functools.partial(kernel, sizes),
                out_shape=[
                    pltpu.VMEM((COMPS, X, Y, Z), jnp.float32),
                    pltpu.VMEM((EX, EY, EZ), jnp.float32),
                ],
                in_specs=[pl.BlockSpec(memory_space=pltpu.HBM)] * 4,
                out_specs=[pl.BlockSpec(memory_space=pltpu.VMEM)] * 2,
                scratch_shapes=[
                    vmem(COMPS, X, Y, Z),
                    pltpu.VMEM((3, EX, EY, EZ), jnp.int32),
                    dma((2,)),
                    vmem(2, COMPS, 2, Y, Z),
                    vmem(2, COMPS * 2 * X + EX * Y, Z),
                    vmem(2, COMPS * 2 * X + EX * Y, Z),
                    vmem(COMPS, X, Y, Z),
                    vmem(packs + EX, Y, Z),
                    vmem(2, packs + EX, Y, Z),
                    vmem(EX, Y, Z),
                    vmem(sides, EX, Y, Z),
                    vmem(2, depth, Y, Z),
                    vmem(sides, 2, depth, Y, Z),
                    vmem(2, depth, Y, Z),
                    vmem(2, edge_packs, Y, Z),
                    vmem(2, 2, edge_packs, Y, Z),
                    vmem(COMPS, X + 1, Y, Z),
                    vmem(2, COMPS, X, Y, Z),
                    vmem(2, COMPS, X, Y, Z),
                    vmem(COMPS, X, Y, Z),
                    vmem(COMPS - SPECIES + 1, X, Y, Z),
                    dma((4,)),
                    dma((7,)),
                    pltpu.SemaphoreType.REGULAR((len(halo_links(sizes)),)),
                    pltpu.SemaphoreType.REGULAR,
                    vmem(1, ROW),
                    dma(()),
                    dma(()),
                    dma((2 * len(groups),)),
                ]
                + rows_scratch,
                compiler_params=pltpu.CompilerParams(collective_id=0, has_side_effects=True),
            )(species, velocity_in, pressure_in, wall_types)
        )
        return tuple(
            pl.pallas_call(
                store,
                out_shape=[
                    jax.ShapeDtypeStruct((COMPS, X, Y, Z), jnp.float32),
                    jax.ShapeDtypeStruct((EX, EY, EZ), jnp.float32),
                ],
                in_specs=[pl.BlockSpec(memory_space=pltpu.VMEM)] * 2,
                out_specs=[pl.BlockSpec(memory_space=pltpu.HBM)] * 2,
                scratch_shapes=[pltpu.SemaphoreType.DMA((2,))],
            )(*[pltpu.with_memory_space_constraint(v, pltpu.VMEM) for v in (state, weights)])
        )

    in_specs = (
        P(None, "gx", "gy", "gz"),
        P(None, "gx", "gy", "gz"),
        P("gx", "gy", "gz"),
        P(None, "gx", "gy", "gz"),
    )
    out_specs = (P(None, "gx", "gy", "gz"), P("gx", "gy", "gz"))
    return jax.shard_map(local, mesh=mesh, in_specs=in_specs, out_specs=out_specs, check_vma=False)
```

```python
import functools
import itertools

import jax
import jax.numpy as jnp
from jax import lax
from jax.experimental import pallas as pl
from jax.experimental.pallas import tpu as pltpu
from jax.sharding import PartitionSpec as P

SPECIES = 5
P_SIZE = 4
ITERS = 2
GAMMA = 1.4
COURANT = 0.4
FLOOR = 0.1
SLOPE_FLOOR = 0.01
SPREAD = 0.002
RELAX = 0.1

COMPS = SPECIES + 4
AXES = ("gx", "gy", "gz")
ROW = 128
DIRECT = 64
MESH = pl.DeviceIdType.MESH


def reduce_groups(sizes):
    if sizes[0] * sizes[1] * sizes[2] <= DIRECT:
        return [(0, 1, 2)]
    return [(2,), (1,), (0,)]


def group_offsets(sizes, group):
    spans = [range(sizes[d]) if d in group else (0,) for d in range(3)]
    far = lambda off: sum(min(off[d], sizes[d] - off[d]) for d in range(3))
    return sorted(itertools.product(*spans), key=far)


def halo_links(sizes):
    return [(d, k) for d in range(3) for k in ((1,) if sizes[d] == 2 else (1, -1))]


def conserved_of(inputs):
    species, velocity, pressure = inputs[:SPECIES], inputs[SPECIES : SPECIES + 3], inputs[-1]
    density = sum(species[1:], species[0])
    square = velocity[0] * velocity[0] + velocity[1] * velocity[1] + velocity[2] * velocity[2]
    energy = pressure * (1.0 / (GAMMA - 1.0)) + 0.5 * density * square
    return list(species) + [density * v for v in velocity] + [energy]


def primitives(cons):
    density = sum(cons[1:SPECIES], cons[0])
    safe = jnp.maximum(density, FLOOR)
    inverse = 1.0 / safe
    momentum = cons[SPECIES : SPECIES + 3]
    velocity = [m * inverse for m in momentum]
    kinetic = momentum[0] * velocity[0] + momentum[1] * velocity[1] + momentum[2] * velocity[2]
    pressure = (GAMMA - 1.0) * (cons[SPECIES + 3] - 0.5 * kinetic)
    return density, safe, inverse, velocity, pressure


def state_of(density, momentum, energy):
    safe = jnp.maximum(density, FLOOR)
    inverse = 1.0 / safe
    velocity = [m * inverse for m in momentum]
    kinetic = momentum[0] * velocity[0] + momentum[1] * velocity[1] + momentum[2] * velocity[2]
    pressure = (GAMMA - 1.0) * (energy - 0.5 * kinetic)
    return safe, velocity, pressure


def sound_of(inverse, pressure):
    return jnp.sqrt(GAMMA * jnp.maximum(pressure, FLOOR) * inverse)


def entropy(density, safe, pressure):
    return density * (jnp.log(jnp.maximum(pressure, FLOOR)) - GAMMA * jnp.log(safe))


def flux_term(cons, velocity, pressure, comp, d):
    term = cons[comp] * velocity[d]
    if comp == SPECIES + d:
        term = term + pressure
    if comp == SPECIES + 3:
        term = term + pressure * velocity[d]
    return term


def face_pair(mm, left, right, pp, jump, rate, wall, wall_value):
    both = left + right
    high = (7.0 * both - (mm + pp)) * (1.0 / 12.0)
    low = 0.5 * both - rate * jump
    keep = 0.0 if wall_value is None else wall_value
    diff = jnp.where(wall, 0.0, high - low)
    return jnp.where(wall, keep, low), diff


def kernel(
    sizes, sp_hbm, ve_hbm, pr_hbm, wa_hbm, out, bl, inp, wa, load_sem,
    xh, ys, yr, hy, zs, zr, es, er, pk, pnx, pny, pz, qz, bs, bc, dx, du, dw, lows, deltas,
    sent_sem, came_sem, near_sem, all_sem, relay, relay_sem, row_sent, row_came, *rows_scratch
):
    X, Y, Z = inp.shape[1:]
    EX, EY, EZ = wa.shape[1:]
    loads = [
        pltpu.make_async_copy(sp_hbm, inp.at[:SPECIES], load_sem.at[0]),
        pltpu.make_async_copy(ve_hbm, inp.at[SPECIES : SPECIES + 3], load_sem.at[0]),
        pltpu.make_async_copy(pr_hbm, inp.at[SPECIES + 3], load_sem.at[0]),
        pltpu.make_async_copy(wa_hbm, wa, load_sem.at[1]),
    ]
    for copy in loads:
        copy.start()
    me = [lax.axis_index(name) for name in AXES]
    groups = reduce_groups(sizes)

    place = [[me[d]] + [lax.rem(me[d] + k, sizes[d]) for k in range(1, sizes[d])] for d in range(3)]

    def device(off):
        return tuple(place[d][off[d]] for d in range(3))

    def step(d, k):
        return tuple(k % sizes[d] if a == d else 0 for a in range(3))

    relayed = len(groups) == 1
    if relayed:
        rows_scratch[1][...] = jnp.zeros_like(rows_scratch[1])

    def traced(flag):
        return jnp.where(flag, 1, 0).astype(jnp.int32)

    links = halo_links(sizes)
    near = {link: near_sem.at[i] for i, link in enumerate(links)}

    def later(d, k):
        return me[d] != sizes[d] - 1 if k == 1 else me[d] == 0

    def neighbour(d, k):
        return device(step(d, k))

    corner = tuple(n - 1 for n in sizes)
    is_corner = (me[0] == corner[0]) & (me[1] == corner[1]) & (me[2] == corner[2])
    devices = sizes[0] * sizes[1] * sizes[2]
    barrier = pltpu.get_barrier_semaphore()

    @pl.when(jnp.logical_not(is_corner))
    def _():
        pl.semaphore_signal(barrier, inc=1, device_id=corner, device_id_type=MESH)

    expected = jnp.where(is_corner, devices - 1, 0).astype(jnp.int32)
    for d, k in links:

        @pl.when(later(d, k))
        def _(d=d, k=k):
            pl.semaphore_signal(barrier, inc=1, device_id=neighbour(d, k), device_id_type=MESH)

        expected = expected + 1 - traced(later(d, k))

    @pl.when(expected > 0)
    def _():
        pl.semaphore_wait(barrier, expected)

    for d, k in links:
        back = (d, k if sizes[d] == 2 else -k)

        @pl.when(jnp.logical_not(later(d, k)))
        def _(d=d, k=k, back=back):
            pl.semaphore_signal(
                near[back], inc=1, device_id=neighbour(d, k), device_id_type=MESH
            )

    @pl.when(is_corner)
    def _():
        def tell(i, carry):
            z = lax.rem(i, sizes[2])
            y = lax.rem(lax.div(i, sizes[2]), sizes[1])
            x = lax.div(i, sizes[2] * sizes[1])
            pl.semaphore_signal(all_sem, inc=1, device_id=(x, y, z), device_id_type=MESH)
            return carry

        if devices <= DIRECT:
            for at in itertools.product(*[range(n) for n in sizes]):
                if at != corner:
                    pl.semaphore_signal(all_sem, inc=1, device_id=at, device_id_type=MESH)
        else:
            lax.fori_loop(0, devices - 1, tell, 0)

    def await_near(d, k):
        @pl.when(later(d, k))
        def _():
            pl.semaphore_wait(near[d, k], 1)

    def await_all():
        @pl.when(jnp.logical_not(is_corner))
        def _():
            pl.semaphore_wait(all_sem, 1)

    pltpu.make_async_copy(inp, inp, load_sem.at[0]).wait()
    loads[3].wait()

    origin = (me[0] == 0) & (me[1] <= 1)
    next_up = origin & (me[2] == 1)
    origin = origin & (me[2] == 0)
    plane_rows = ((origin, devices - 2), (jnp.logical_not(origin), devices - 3))
    if relayed:
        relay_copy = pltpu.make_async_remote_copy(
            src_ref=rows_scratch[0],
            dst_ref=relay,
            send_sem=row_sent,
            recv_sem=relay_sem,
            device_id=neighbour(2, 1),
            device_id_type=MESH,
        )

    def speed_out():
        await_all()
        if not relayed:
            spread_start(0, 0, speed_row)
            return

        @pl.when(next_up)
        def _():
            relay_copy.wait_recv()
            spread_start(0, 0, jnp.maximum(speed_row, relay[...]))

        @pl.when(jnp.logical_not(origin | next_up))
        def _():
            spread_start(0, 0, speed_row)

    def row_parts(turn, stage):
        base = 2 * (turn * len(groups) + stage)
        mine, buf = rows_scratch[base : base + 2]
        return mine, buf, row_came.at[turn % 2 * len(groups) + stage]

    def spread_copy(turn, stage, i):
        mine, buf, came = row_parts(turn, stage)
        group = groups[stage]
        off = group_offsets(sizes, group)[i]
        there = tuple(
            lax.rem(sizes[d] - 1 - me[d] + off[d], sizes[d]) if d in group else me[d]
            for d in range(3)
        )
        can_be_me = all((off[d] + 1 - sizes[d]) % 2 == 0 or sizes[d] % 2 for d in group)
        copy = pltpu.make_async_remote_copy(
            src_ref=mine,
            dst_ref=buf.at[pl.ds(i, 1)],
            send_sem=row_sent,
            recv_sem=came,
            device_id=there,
            device_id_type=MESH,
        )
        return copy, can_be_me, functools.reduce(lambda a, b: a & b, [t == m for t, m in zip(there, me)])

    def spread_start(turn, stage, row):
        if turn or stage:
            before = turn * len(groups) + stage - 1
            spread_sent(before // len(groups), before % len(groups))
        mine, buf, _ = row_parts(turn, stage)
        mine[...] = row
        for i in range(buf.shape[0]):
            copy, can_be_me, is_me = spread_copy(turn, stage, i)
            if not can_be_me:
                copy.start()
                continue

            @pl.when(jnp.logical_not(is_me))
            def _(copy=copy):
                copy.start()

            @pl.when(is_me)
            def _(i=i):
                buf[i : i + 1] = row

    def spread_whole(turn, stage, rows=None):
        _, buf, came = row_parts(turn, stage)
        rows = buf.at[pl.ds(0, rows or buf.shape[0] - 1)]
        return pltpu.make_async_remote_copy(
            src_ref=rows,
            dst_ref=rows,
            send_sem=row_sent,
            recv_sem=came,
            device_id=device((1, 1, 1)),
            device_id_type=MESH,
        )

    def spread_end(turn, combine):
        for stage in range(len(groups)):
            if stage > 0:
                spread_start(turn, stage, row)
            if turn == 0 and relayed:
                for flag, rows in plane_rows:

                    @pl.when(flag)
                    def _(rows=rows):
                        spread_whole(turn, stage, rows).wait_recv()
            else:
                spread_whole(turn, stage).wait_recv()
            row = combine(row_parts(turn, stage)[1][...])
        return row

    def spread_sent(turn, stage):
        if turn == 0 and relayed:

            @pl.when(jnp.logical_not(origin))
            def _():
                spread_whole(turn, stage).wait_send()

            @pl.when(origin)
            def _():
                relay_copy.wait_send()

        else:
            spread_whole(turn, stage).wait_send()

    row_index = lax.broadcasted_iota(jnp.int32, (1, Y, Z), 1)
    lane_index = lax.broadcasted_iota(jnp.int32, (1, Y, Z), 2)
    index = {1: row_index, 2: lane_index}
    extent = {1: Y, 2: Z}

    def roll(value, shift, axis):
        return pltpu.roll(value, shift % value.shape[axis], axis)

    def mesh_group(value, axis, op):
        for s in (1, 2):
            low = (index[axis] & s) == 0
            value = op(value, jnp.where(low, roll(value, -s, axis), roll(value, s, axis)))
        return value

    def lane_group(value, op):
        place = lane_index & (P_SIZE - 1)
        for s in range(1, P_SIZE):
            ahead = roll(value, -s, 2)
            behind = roll(value, P_SIZE - s, 2)
            turned = jnp.where(place < P_SIZE - s, ahead, behind)
            whole = turned if s == 1 else op(whole, turned)
        return op(value, whole)

    def element(value, op):
        parts = value.reshape(EX, P_SIZE, Y, Z)
        value = op(op(parts[:, 0], parts[:, 1]), op(parts[:, 2], parts[:, 3]))
        return lane_group(mesh_group(value, 1, op), op)

    def nodes(value):
        return jnp.broadcast_to(value[:, None], (EX, P_SIZE, Y, Z)).reshape(X, Y, Z)

    def total(value, op):
        value = functools.reduce(op, [value[x] for x in range(X)])
        value = {jnp.minimum: jnp.min, jnp.maximum: jnp.max, jnp.add: jnp.sum}[op](
            value, axis=0, keepdims=True
        )
        return {jnp.minimum: jnp.min, jnp.maximum: jnp.max, jnp.add: jnp.sum}[op](
            value, axis=1, keepdims=True
        )

    late = me[2] == corner[2]
    last_x = me[0] == corner[0]
    last_chip = last_x & (me[1] >= corner[1] - 1) & late
    first_sides = ((0, 1),) if sizes[0] == 2 else ((0, 1), (1, -1))
    packs = zs.shape[0] - EX
    body = COMPS * 2 * X

    def remote(src, dst, sent, came, off):
        return pltpu.make_async_remote_copy(
            src_ref=src,
            dst_ref=dst,
            send_sem=sent_sem.at[sent],
            recv_sem=came_sem.at[came],
            device_id=device(off),
            device_id_type=MESH,
        )

    landing = {
        "x": (xh, 0, 0),
        "y": (yr, 1, 1),
        "z": (zr, 2, 2),
        "e": (er, 3, 3),
        ("b", 0): (pnx, 0, 4),
        ("b", 1): (pny, 1, 5),
        ("b", 2): (qz, 2, 6),
        "c": (bc, 3, 7),
    }

    def whole(key):
        ref, sent, came = landing[key]
        return remote(ref, ref, sent, came, step(2, 1))

    def arrive(key):
        whole(key).wait_recv()

    def sent_all(key):
        whole(key).wait_send()

    def send_x():
        for d, k in links:
            if d == 0:
                await_near(d, k)
        for side, k in ((0, 1), (1, -1)):
            at = X - 2 if side == 0 else 0
            remote(inp.at[:, at : at + 2], xh.at[side], 0, 0, step(0, k)).start()

    def send_e():
        for side, k in first_sides:
            remote(es, er.at[side], 3, 3, step(0, k)).start()

    def send_y():
        for side, k in ((0, 1), (1, -1)):
            if (1, k) in links:
                await_near(1, k)
            remote(ys.at[side], yr.at[side], 1, 1, step(1, k)).start()

    def send_z():
        for side, k in ((0, 1), (1, -1)):
            if (2, k) in links:
                await_near(2, k)
            remote(zs, zr.at[side], 2, 2, step(2, k)).start()
            if side == 0 and relayed:

                @pl.when(origin)
                def _():
                    rows_scratch[0][...] = speed_row
                    relay_copy.start()

    @pl.when(late & last_x & jnp.logical_not(last_chip))
    def _():
        send_x()

    own_inputs = [inp[c] for c in range(COMPS)]

    cons = conserved_of(own_inputs)
    density, _, inverse, velocity, pressure = primitives(cons)
    sound = sound_of(inverse, pressure)
    speed = jnp.abs(velocity[0]) + jnp.abs(velocity[1]) + jnp.abs(velocity[2]) + 3.0 * sound
    speed_row = jnp.broadcast_to(total(speed, jnp.maximum), (1, ROW))

    @pl.when(last_chip)
    def _():
        speed_out()
        send_x()

    for c in range(COMPS):
        for x in range(X):
            at = 2 * (c * X + x)
            ys[0, at : at + 2, :] = own_inputs[c][x, Y - 2 : Y, :]
            ys[1, at : at + 2, :] = own_inputs[c][x, 0:2, :]
    per_pack = Z // (4 * X)
    for v in range(packs):
        packed = jnp.zeros((1, Y, Z), jnp.float32)
        for c in range(v * per_pack, min((v + 1) * per_pack, COMPS)):
            for x in range(X):
                at = ((c - v * per_pack) * X + x) * 4
                moved = roll(own_inputs[c][x : x + 1], at + 2, 2)
                packed = jnp.where((lane_index >= at) & (lane_index < at + 4), moved, packed)
        zs[v] = packed[0]

    rho_min = element(density, jnp.minimum)
    p_min = element(pressure, jnp.minimum)
    widen = (
        lax.broadcasted_iota(jnp.int32, (EZ, Z), 1) // P_SIZE
        == lax.broadcasted_iota(jnp.int32, (EZ, Z), 0)
    ).astype(jnp.float32)
    heighten = (
        lax.broadcasted_iota(jnp.int32, (Y, EY), 0) // P_SIZE
        == lax.broadcasted_iota(jnp.int32, (Y, EY), 1)
    ).astype(jnp.float32)
    walls = []
    for d in range(3):
        layers = []
        for e in range(EX):
            flags = wa[d, e].astype(jnp.float32)
            flags = jnp.dot(flags, widen, preferred_element_type=jnp.float32)
            layers.append(jnp.dot(heighten, flags, preferred_element_type=jnp.float32)[None])
        walls.append(jnp.concatenate(layers, axis=0))
        turn_row = row_index & (P_SIZE - 1)
        fields = jnp.where(turn_row == 0, rho_min, jnp.where(turn_row == 1, p_min, walls[d]))
        if d == 0:
            es[...] = fields
        elif d == 1:
            for side in (0, 1):
                ys[side, body : body + EX * Y, :] = fields.reshape(EX * Y, Z)
        else:
            zs[packs : packs + EX] = fields

    def spread_rows(value, which):
        value = jnp.where((row_index & (P_SIZE - 1)) == which, value, jnp.inf)
        return mesh_group(value, 1, jnp.minimum)

    def edge(side, d, which):
        if d == 0:
            fields = er[0 if sizes[0] == 2 else side]
        elif d == 1:
            fields = yr[side, body : body + EX * Y, :].reshape(EX, Y, Z)
        else:
            fields = zr[side, packs : packs + EX]
        return spread_rows(fields, which)

    @pl.when(jnp.logical_not(late))
    def _():
        send_x()
        send_e()
        send_y()

    send_z()

    @pl.when(late & jnp.logical_not(last_x))
    def _():
        send_x()

    @pl.when(late)
    def _():
        send_e()
        send_y()

    @pl.when(jnp.logical_not(last_chip))
    def _():
        speed_out()

    def cyclic_fluxes(d, halo_inputs, number, first):
        n = extent[d]
        ix = index[d]
        halo = conserved_of(halo_inputs)
        _, _, h_inv, h_vel, h_p = primitives(halo)
        h_rate = jnp.abs(h_vel[d]) + sound_of(h_inv, h_p)
        rate = jnp.abs(velocity[d]) + sound

        def beside(value, beyond, k):
            edge_of = ix < k if k > 0 else ix >= n + k
            return roll(jnp.where(edge_of, beyond, value), -k, d)

        shifts = (-2, -1, 1, 2)
        along = {k: {d: beside(velocity[d], h_vel[d], k)} for k in shifts}
        p_at = {k: beside(pressure, h_p, k) for k in shifts}
        flag = roll(jnp.where(ix == 0, edge(1, d, 2), walls[d]), -1, d)
        ends = ix & (P_SIZE - 1)
        wall = nodes(jnp.where(ends == P_SIZE - 1, flag, 0.0)) > 0.5
        wall_low = nodes(jnp.where(ends == 0, walls[d], 0.0)) > 0.5
        half_rate = 0.5 * jnp.maximum(rate, beside(rate, h_rate, 1))
        half_low = 0.5 * jnp.maximum(beside(rate, h_rate, -1), rate)
        wall_p = 0.5 * (pressure + p_at[1])
        wall_p_low = 0.5 * (p_at[-1] + pressure)
        for c in range(COMPS):
            u_at = {k: beside(cons[c], halo[c], k) for k in shifts}
            f_at = {k: flux_term({c: u_at[k]}, along[k], p_at[k], c, d) for k in shifts}
            f = flux_term(cons, velocity, pressure, c, d)
            is_normal = c == SPECIES + d
            low, diff = face_pair(
                f_at[-1],
                f,
                f_at[1],
                f_at[2],
                u_at[1] - cons[c],
                half_rate,
                wall,
                wall_p if is_normal else None,
            )
            before_low, before_diff = face_pair(
                f_at[-2],
                f_at[-1],
                f,
                f_at[1],
                cons[c] - u_at[-1],
                half_low,
                wall_low,
                wall_p_low if is_normal else None,
            )
            du[number, c] = diff
            dw[number, c] = before_diff
            slot = max(c - SPECIES + 1, 0)
            if first:
                lows[c] = low - before_low
            else:
                lows[c] += low - before_low
            if first and c in (0, *range(SPECIES, COMPS)):
                deltas[slot] = diff - before_diff
            else:
                deltas[slot] += diff - before_diff

    arrive("y")
    for c in range(COMPS):
        hy[c] = own_inputs[c]
        for x in range(X):
            at = 2 * (c * X + x)
            hy[c, x, Y - 2 : Y, :] = yr[0, at : at + 2, :]
            hy[c, x, 0:2, :] = yr[1, at : at + 2, :]
    cyclic_fluxes(1, [hy[c] for c in range(COMPS)], 1, True)

    arrive("z")
    merged = [
        jnp.where((lane_index & 3) < 2, zr[0, v][None], zr[1, v][None]) for v in range(packs)
    ]
    z_halo = []
    for c in range(COMPS):
        layers = []
        for x in range(X):
            at = ((c % per_pack) * X + x) * 4
            layers.append(roll(merged[c // per_pack], -(at + 2), 2))
        z_halo.append(jnp.concatenate(layers, axis=0))
    cyclic_fluxes(2, z_halo, 0, False)

    arrive("x")
    arrive("e")
    sides = []
    for side in (0, 1):
        halo = conserved_of([xh[side, c] for c in range(COMPS)])
        _, _, h_inv, h_vel, h_p = primitives(halo)
        sides.append((halo, h_vel, h_p, jnp.abs(h_vel[0]) + sound_of(h_inv, h_p)))

    def joined(below, own, above):
        return jnp.concatenate([below, own, above], axis=0)

    rate = joined(sides[0][3], jnp.abs(velocity[0]) + sound, sides[1][3])
    p_ext = joined(sides[0][2], pressure, sides[1][2])
    half_rate = 0.5 * jnp.maximum(rate[1 : X + 2], rate[2 : X + 3])
    wall_p = 0.5 * (p_ext[1 : X + 2] + p_ext[2 : X + 3])
    planes = []
    for x in range(-1, X):
        if (x + 1) % P_SIZE:
            planes.append(jnp.zeros((1, Y, Z), jnp.float32))
        elif x == X - 1:
            planes.append(edge(1, 0, 2)[0:1])
        else:
            e = (x + 1) // P_SIZE
            planes.append(walls[0][e : e + 1])
    wall = jnp.concatenate(planes, axis=0) > 0.5
    for c in range(COMPS):
        f = joined(
            flux_term(sides[0][0], sides[0][1], sides[0][2], c, 0),
            flux_term(cons, velocity, pressure, c, 0),
            flux_term(sides[1][0], sides[1][1], sides[1][2], c, 0),
        )
        u = joined(sides[0][0][c], cons[c], sides[1][0][c])
        low, diff = face_pair(
            f[0 : X + 1],
            f[1 : X + 2],
            f[2 : X + 3],
            f[3 : X + 4],
            u[2 : X + 3] - u[1 : X + 2],
            half_rate,
            wall,
            wall_p if c == SPECIES else None,
        )
        dx[c] = diff
        lows[c] += low[1:] - low[:-1]
        deltas[max(c - SPECIES + 1, 0)] += diff[1:] - diff[:-1]

    def bound(own, which):
        best = own
        for d in (1, 2):
            n = extent[d]
            up = jnp.where(index[d] < P_SIZE, edge(1, d, which), own)
            down = jnp.where(index[d] >= n - P_SIZE, edge(0, d, which), own)
            best = jnp.minimum(best, jnp.minimum(roll(up, -P_SIZE, d), roll(down, P_SIZE, d)))
        chain = joined(edge(0, 0, which)[EX - 1 : EX], own, edge(1, 0, which)[0:1])
        return jnp.minimum(best, jnp.minimum(chain[:EX], chain[2:]))

    rho_bound = bound(rho_min, 0)
    p_bound = bound(p_min, 1)

    fluxes = [sum([lows[c] for c in range(1, SPECIES)], lows[0])]
    fluxes += [lows[c] for c in range(SPECIES, COMPS)]
    jumps = [deltas[i] for i in range(COMPS - SPECIES + 1)]

    speed_max = spread_end(0, lambda rows: jnp.max(rows, axis=0, keepdims=True))
    ratio = (COURANT / speed_max).reshape(1, 1, ROW)

    def five(values):
        return [sum([values[c] for c in range(1, SPECIES)], values[0])] + [
            values[c] for c in range(SPECIES, COMPS)
        ]

    low_five = [u - ratio * f for u, f in zip(five(cons), fluxes)]
    d_five = [-(ratio * d) for d in jumps]
    d_rho = d_five[0]
    rho_scale = 1.0 / jnp.maximum(-d_rho, SLOPE_FLOOR)
    count = X * Y * Z * sizes[0] * sizes[1] * sizes[2]
    stat_lane = lax.broadcasted_iota(jnp.int32, (1, ROW), 1)

    def combine_stats(rows):
        return jnp.where(
            stat_lane < 2,
            jnp.min(rows, axis=0, keepdims=True),
            jnp.sum(rows, axis=0, keepdims=True),
        )

    def broadcast_stats(got):
        lowest_rho = got[0:1, 0:1].reshape(1, 1, 1)
        lowest_p = got[0:1, 1:2].reshape(1, 1, 1)
        spread = got[0:1, 2:3].reshape(1, 1, 1) * (1.0 / count) + SPREAD
        return lowest_rho, lowest_p, spread

    def next_blend(got, packed):
        t_density, rho_scale, t_p, p_scale, rho_bound, p_bound, mean_square, base = packed
        lowest_rho, lowest_p, spread = got
        rho_target = rho_bound - RELAX * jnp.maximum(rho_bound - lowest_rho, 0.0)
        p_target = p_bound - RELAX * jnp.maximum(p_bound - lowest_p, 0.0)
        step_rho = jnp.minimum(t_density - nodes(rho_target), 0.0) * rho_scale
        step_p = jnp.minimum(t_p - nodes(p_target), 0.0) * p_scale
        lowered = element(jnp.minimum(step_rho, step_p), jnp.minimum)
        cap = spread / (spread + mean_square)
        return jnp.maximum(jnp.minimum(cap, base + lowered), 0.0)

    per_edge = Z // (2 * P_SIZE)
    depth = 10 * X + 2 * EX

    def share(fields):
        at = 0
        for value in fields:
            pk[at : at + value.shape[0]] = value
            at += value.shape[0]
        for side, k in first_sides:
            remote(pk, pnx.at[side], 0, 4, step(0, k)).start()
        for side, k in ((0, 1), (1, -1)):
            rows = pl.ds(Y - P_SIZE, P_SIZE) if side == 0 else pl.ds(0, P_SIZE)
            remote(pk.at[:, rows], pny.at[:, rows], 1, 5, step(1, k)).start()
        items = [value[x : x + 1] for value in fields for x in range(value.shape[0])]
        for v in range(pz.shape[0]):
            packed = jnp.zeros((1, Y, Z), jnp.float32)
            for j, item in enumerate(items[v * per_edge : (v + 1) * per_edge]):
                at = 2 * P_SIZE * j
                moved = roll(item, at + P_SIZE, 2)
                inside = (lane_index >= at) & (lane_index < at + 2 * P_SIZE)
                packed = jnp.where(inside, moved, packed)
            pz[v] = packed[0]
        for side, k in ((0, 1), (1, -1)):
            remote(pz, qz.at[side], 2, 6, step(2, k)).start()

    sides_x = len(first_sides)

    def share_blend():
        bs[...] = blend
        for side, k in first_sides:
            there = bc.at[pl.ds(side * EX, EX)]
            remote(bs, there, 3, 7, step(0, k)).start()
        for side, k in ((0, 1), (1, -1)):
            there = bc.at[pl.ds((sides_x + 1 + side) * EX, EX)]
            remote(bs, there, 3, 7, step(2, k)).start()
            rows = pl.ds(Y - P_SIZE, P_SIZE) if side == 0 else pl.ds(0, P_SIZE)
            there = bc.at[pl.ds(sides_x * EX, EX), rows]
            remote(bs.at[:, rows], there, 3, 7, step(1, k)).start()

    def trial_of(low, d, low_sigma, blend):
        weight = None if blend is None else nodes(blend)
        trial = [a + (b if weight is None else weight * b) for a, b in zip(low, d)]
        safe, speeds, p = state_of(trial[0], trial[1:4], trial[4])
        residual = entropy(trial[0], safe, p) - low_sigma
        return trial[0], speeds, p, residual * residual

    def scales_of(d, speeds, square):
        cross = speeds[0] * d[1] + speeds[1] * d[2] + speeds[2] * d[3]
        speed2 = speeds[0] * speeds[0] + speeds[1] * speeds[1] + speeds[2] * speeds[2]
        slope = (GAMMA - 1.0) * (d[4] - cross + 0.5 * speed2 * d[0])
        mean_square = element(square, jnp.add) * (1.0 / (P_SIZE**3))
        return 1.0 / jnp.maximum(-slope, SLOPE_FLOOR), mean_square

    def sigma_of(low):
        safe, _, p = state_of(low[0], low[1:4], low[4])
        return entropy(low[0], safe, p)

    def neighbour_low(layer):
        low = [layer(i * X, (i + 1) * X) for i in range(5)]
        d = [layer(i * X, (i + 1) * X) for i in range(5, 10)]
        bounds = [layer(10 * X + i * EX, 10 * X + (i + 1) * EX) for i in range(2)]
        scale = 1.0 / jnp.maximum(-d[0], SLOPE_FLOOR)
        return low, d, sigma_of(low), scale, bounds

    def neighbour_fields(known, blend):
        low, d, sigma, scale, bounds = known
        density, speeds, p, square = trial_of(low, d, sigma, blend)
        p_scale, mean_square = scales_of(d, speeds, square)
        return density, scale, p, p_scale, bounds[0], bounds[1], mean_square, blend

    low_sigma = sigma_of(low_five)
    blend = None
    for newton in range(ITERS):
        t_density, t_vel, t_p, square = trial_of(low_five, d_five, low_sigma, blend)
        stats = jnp.where(
            stat_lane == 0,
            total(t_density, jnp.minimum),
            jnp.where(stat_lane == 1, total(t_p, jnp.minimum), total(square, jnp.add)),
        )
        spread_start(newton + 1, 0, stats)
        if newton == ITERS - 2:
            for key in ("x", "y", "z", "e"):
                sent_all(key)
            share((*low_five, *d_five, rho_bound, p_bound))
        p_scale, mean_square = scales_of(d_five, t_vel, square)
        base = jnp.ones((EX, Y, Z), jnp.float32) if blend is None else blend
        beside = {}
        if newton == ITERS - 1:
            for d in (1, 2, 0):
                arrive(("b", d))
            known = {1: neighbour_low(lambda a, b: pny[a:b])}
            near = (lane_index & (2 * P_SIZE - 1)) < P_SIZE
            edges = [
                jnp.where(near, qz[0, v][None], qz[1, v][None]) for v in range(pz.shape[0])
            ]
            items = [
                roll(edges[j // per_edge], -(2 * P_SIZE * (j % per_edge) + P_SIZE), 2)
                for j in range(depth)
            ]
            known[2] = neighbour_low(lambda a, b: jnp.concatenate(items[a:b], axis=0))
            for side in range(sides_x):
                known[0, side] = neighbour_low(lambda a, b: pnx[side, a:b])
            for d in range(3):
                sent_all(("b", d))
            sent_all("c")
            arrive("c")
            at = sides_x * EX
            weights = {(0, side): bc[side * EX : (side + 1) * EX] for side in range(sides_x)}
            weights[1] = bc[at : at + EX]
            weights[2] = jnp.where(
                lane_index < P_SIZE, bc[at + 2 * EX : at + 3 * EX], bc[at + EX : at + 2 * EX]
            )
            beside = {key: neighbour_fields(known[key], weights[key]) for key in known}
        got = broadcast_stats(spread_end(newton + 1, combine_stats))
        blend = next_blend(
            got, (t_density, rho_scale, t_p, p_scale, rho_bound, p_bound, mean_square, base)
        )
        if newton == ITERS - 2:
            share_blend()

    beside = {key: next_blend(got, packed) for key, packed in beside.items()}
    beside.setdefault((0, 1), beside[0, 0])

    theta = []
    for d in (2, 1):
        above = roll(jnp.where(index[d] == 0, beside[d], blend), -1, d)
        below = roll(jnp.where(index[d] == extent[d] - 1, beside[d], blend), 1, d)
        theta.append((nodes(jnp.minimum(blend, above)), nodes(jnp.minimum(blend, below))))
    x_blend = joined(beside[0, 0][EX - 1 : EX], nodes(blend), beside[0, 1][0:1])
    x_theta = jnp.minimum(x_blend[:-1], x_blend[1:])
    for c in range(COMPS):
        faces = x_theta * dx[c]
        change = lows[c] + (faces[1:] - faces[:-1])
        for number in range(2):
            upper, lower = theta[number]
            change += upper * du[number, c] - lower * dw[number, c]
        out[c] = cons[c] - ratio * change

    pick_lanes = (
        lax.broadcasted_iota(jnp.int32, (Z, EZ), 1) * P_SIZE
        == lax.broadcasted_iota(jnp.int32, (Z, EZ), 0)
    ).astype(jnp.float32)
    for e in range(EX):
        few = jnp.dot(
            blend[e], pick_lanes, preferred_element_type=jnp.float32, precision=lax.Precision.HIGHEST
        )
        bl[e] = jnp.concatenate([few[j * P_SIZE : j * P_SIZE + 1] for j in range(EY)], axis=0)

    spread_sent(ITERS, len(groups) - 1)


def store(state, weights, state_hbm, weights_hbm, sem):
    copies = [
        pltpu.make_async_copy(state, state_hbm, sem.at[0]),
        pltpu.make_async_copy(weights, weights_hbm, sem.at[1]),
    ]
    for copy in copies:
        copy.start()
    for copy in copies:
        copy.wait()


def solution(mesh):
    sizes = tuple(mesh.shape[name] for name in AXES)

    def local(species, velocity_in, pressure_in, wall_types):
        X, Y, Z = pressure_in.shape
        EX, EY, EZ = wall_types.shape[1:]
        packs = -(-COMPS // (Z // (4 * X)))
        depth = 10 * X + 2 * EX
        edge_packs = -(-depth // (Z // (2 * P_SIZE)))
        vmem = lambda *shape: pltpu.VMEM(shape, jnp.float32)
        groups = reduce_groups(sizes)
        dma = pltpu.SemaphoreType.DMA
        sides = 1 if sizes[0] == 2 else 2
        rows_scratch = []
        for _ in range(ITERS + 1):
            for group in groups:
                rows_scratch += [vmem(1, ROW), vmem(len(group_offsets(sizes, group)), ROW)]
        state, weights = (
            pl.pallas_call(
                functools.partial(kernel, sizes),
                out_shape=[
                    pltpu.VMEM((COMPS, X, Y, Z), jnp.float32),
                    pltpu.VMEM((EX, EY, EZ), jnp.float32),
                ],
                in_specs=[pl.BlockSpec(memory_space=pltpu.HBM)] * 4,
                out_specs=[pl.BlockSpec(memory_space=pltpu.VMEM)] * 2,
                scratch_shapes=[
                    vmem(COMPS, X, Y, Z),
                    pltpu.VMEM((3, EX, EY, EZ), jnp.int32),
                    dma((2,)),
                    vmem(2, COMPS, 2, Y, Z),
                    vmem(2, COMPS * 2 * X + EX * Y, Z),
                    vmem(2, COMPS * 2 * X + EX * Y, Z),
                    vmem(COMPS, X, Y, Z),
                    vmem(packs + EX, Y, Z),
                    vmem(2, packs + EX, Y, Z),
                    vmem(EX, Y, Z),
                    vmem(sides, EX, Y, Z),
                    vmem(depth, Y, Z),
                    vmem(sides, depth, Y, Z),
                    vmem(depth, Y, Z),
                    vmem(edge_packs, Y, Z),
                    vmem(2, edge_packs, Y, Z),
                    vmem(EX, Y, Z),
                    vmem((sides + 3) * EX, Y, Z),
                    vmem(COMPS, X + 1, Y, Z),
                    vmem(2, COMPS, X, Y, Z),
                    vmem(2, COMPS, X, Y, Z),
                    vmem(COMPS, X, Y, Z),
                    vmem(COMPS - SPECIES + 1, X, Y, Z),
                    dma((4,)),
                    dma((8,)),
                    pltpu.SemaphoreType.REGULAR((len(halo_links(sizes)),)),
                    pltpu.SemaphoreType.REGULAR,
                    vmem(1, ROW),
                    dma(()),
                    dma(()),
                    dma((2 * len(groups),)),
                ]
                + rows_scratch,
                compiler_params=pltpu.CompilerParams(collective_id=0, has_side_effects=True),
            )(species, velocity_in, pressure_in, wall_types)
        )
        return tuple(
            pl.pallas_call(
                store,
                out_shape=[
                    jax.ShapeDtypeStruct((COMPS, X, Y, Z), jnp.float32),
                    jax.ShapeDtypeStruct((EX, EY, EZ), jnp.float32),
                ],
                in_specs=[pl.BlockSpec(memory_space=pltpu.VMEM)] * 2,
                out_specs=[pl.BlockSpec(memory_space=pltpu.HBM)] * 2,
                scratch_shapes=[pltpu.SemaphoreType.DMA((2,))],
            )(*[pltpu.with_memory_space_constraint(v, pltpu.VMEM) for v in (state, weights)])
        )

    in_specs = (
        P(None, "gx", "gy", "gz"),
        P(None, "gx", "gy", "gz"),
        P("gx", "gy", "gz"),
        P(None, "gx", "gy", "gz"),
    )
    out_specs = (P(None, "gx", "gy", "gz"), P("gx", "gy", "gz"))
    return jax.shard_map(local, mesh=mesh, in_specs=in_specs, out_specs=out_specs, check_vma=False)
```

```python
import functools
import itertools

import jax
import jax.numpy as jnp
from jax import lax
from jax.experimental import pallas as pl
from jax.experimental.pallas import tpu as pltpu
from jax.sharding import PartitionSpec as P

SPECIES = 5
P_SIZE = 4
ITERS = 2
GAMMA = 1.4
COURANT = 0.4
FLOOR = 0.1
SLOPE_FLOOR = 0.01
SPREAD = 0.002
RELAX = 0.1

COMPS = SPECIES + 4
AXES = ("gx", "gy", "gz")
ROW = 128
DIRECT = 64
MESH = pl.DeviceIdType.MESH


def reduce_groups(sizes):
    if sizes[0] * sizes[1] * sizes[2] <= DIRECT:
        return [(0, 1, 2)]
    return [(2,), (1,), (0,)]


def group_offsets(sizes, group):
    spans = [range(sizes[d]) if d in group else (0,) for d in range(3)]
    far = lambda off: sum(min(off[d], sizes[d] - off[d]) for d in range(3))
    return sorted(itertools.product(*spans), key=far)


def halo_links(sizes):
    return [(d, k) for d in range(3) for k in ((1,) if sizes[d] == 2 else (1, -1))]


def conserved_of(inputs):
    species, velocity, pressure = inputs[:SPECIES], inputs[SPECIES : SPECIES + 3], inputs[-1]
    density = sum(species[1:], species[0])
    square = velocity[0] * velocity[0] + velocity[1] * velocity[1] + velocity[2] * velocity[2]
    energy = pressure * (1.0 / (GAMMA - 1.0)) + 0.5 * density * square
    return list(species) + [density * v for v in velocity] + [energy]


def primitives(cons):
    density = sum(cons[1:SPECIES], cons[0])
    safe = jnp.maximum(density, FLOOR)
    inverse = 1.0 / safe
    momentum = cons[SPECIES : SPECIES + 3]
    velocity = [m * inverse for m in momentum]
    kinetic = momentum[0] * velocity[0] + momentum[1] * velocity[1] + momentum[2] * velocity[2]
    pressure = (GAMMA - 1.0) * (cons[SPECIES + 3] - 0.5 * kinetic)
    return density, safe, inverse, velocity, pressure


def state_of(density, momentum, energy):
    safe = jnp.maximum(density, FLOOR)
    inverse = 1.0 / safe
    velocity = [m * inverse for m in momentum]
    kinetic = momentum[0] * velocity[0] + momentum[1] * velocity[1] + momentum[2] * velocity[2]
    pressure = (GAMMA - 1.0) * (energy - 0.5 * kinetic)
    return safe, velocity, pressure


def sound_of(inverse, pressure):
    return jnp.sqrt(GAMMA * jnp.maximum(pressure, FLOOR) * inverse)


def entropy(density, safe, pressure):
    return density * (jnp.log(jnp.maximum(pressure, FLOOR)) - GAMMA * jnp.log(safe))


def flux_term(cons, velocity, pressure, comp, d):
    term = cons[comp] * velocity[d]
    if comp == SPECIES + d:
        term = term + pressure
    if comp == SPECIES + 3:
        term = term + pressure * velocity[d]
    return term


def face_pair(mm, left, right, pp, jump, rate, wall, wall_value):
    both = left + right
    high = (7.0 * both - (mm + pp)) * (1.0 / 12.0)
    low = 0.5 * both - rate * jump
    keep = 0.0 if wall_value is None else wall_value
    diff = jnp.where(wall, 0.0, high - low)
    return jnp.where(wall, keep, low), diff


def kernel(
    sizes, sp_hbm, ve_hbm, pr_hbm, wa_hbm, out, bl, inp, wa, load_sem,
    xh, ys, yr, hy, zs, zr, es, er, pk, pnx, pny, pz, qz, bs, bc, dx, du, dw, lows, deltas,
    sent_sem, came_sem, near_sem, all_sem, relay, relay_sem, row_sent, row_came, *rows_scratch
):
    X, Y, Z = inp.shape[1:]
    EX, EY, EZ = wa.shape[1:]
    loads = [
        pltpu.make_async_copy(sp_hbm, inp.at[:SPECIES], load_sem.at[0]),
        pltpu.make_async_copy(ve_hbm, inp.at[SPECIES : SPECIES + 3], load_sem.at[0]),
        pltpu.make_async_copy(pr_hbm, inp.at[SPECIES + 3], load_sem.at[0]),
        pltpu.make_async_copy(wa_hbm, wa, load_sem.at[1]),
    ]
    for copy in loads:
        copy.start()
    me = [lax.axis_index(name) for name in AXES]
    groups = reduce_groups(sizes)

    place = [[me[d]] + [lax.rem(me[d] + k, sizes[d]) for k in range(1, sizes[d])] for d in range(3)]

    def device(off):
        return tuple(place[d][off[d]] for d in range(3))

    def step(d, k):
        return tuple(k % sizes[d] if a == d else 0 for a in range(3))

    relayed = len(groups) == 1
    if relayed:
        rows_scratch[1][...] = jnp.zeros_like(rows_scratch[1])

    def traced(flag):
        return jnp.where(flag, 1, 0).astype(jnp.int32)

    links = halo_links(sizes)
    near = {link: near_sem.at[i] for i, link in enumerate(links)}

    def later(d, k):
        return me[d] != sizes[d] - 1 if k == 1 else me[d] == 0

    def neighbour(d, k):
        return device(step(d, k))

    corner = tuple(n - 1 for n in sizes)
    is_corner = (me[0] == corner[0]) & (me[1] == corner[1]) & (me[2] == corner[2])
    devices = sizes[0] * sizes[1] * sizes[2]
    barrier = pltpu.get_barrier_semaphore()

    @pl.when(jnp.logical_not(is_corner))
    def _():
        pl.semaphore_signal(barrier, inc=1, device_id=corner, device_id_type=MESH)

    expected = jnp.where(is_corner, devices - 1, 0).astype(jnp.int32)
    for d, k in links:

        @pl.when(later(d, k))
        def _(d=d, k=k):
            pl.semaphore_signal(barrier, inc=1, device_id=neighbour(d, k), device_id_type=MESH)

        expected = expected + 1 - traced(later(d, k))

    @pl.when(expected > 0)
    def _():
        pl.semaphore_wait(barrier, expected)

    for d, k in links:
        back = (d, k if sizes[d] == 2 else -k)

        @pl.when(jnp.logical_not(later(d, k)))
        def _(d=d, k=k, back=back):
            pl.semaphore_signal(
                near[back], inc=1, device_id=neighbour(d, k), device_id_type=MESH
            )

    @pl.when(is_corner)
    def _():
        def tell(i, carry):
            z = lax.rem(i, sizes[2])
            y = lax.rem(lax.div(i, sizes[2]), sizes[1])
            x = lax.div(i, sizes[2] * sizes[1])
            pl.semaphore_signal(all_sem, inc=1, device_id=(x, y, z), device_id_type=MESH)
            return carry

        if devices <= DIRECT:
            for at in itertools.product(*[range(n) for n in sizes]):
                if at != corner:
                    pl.semaphore_signal(all_sem, inc=1, device_id=at, device_id_type=MESH)
        else:
            lax.fori_loop(0, devices - 1, tell, 0)

    def await_near(d, k):
        @pl.when(later(d, k))
        def _():
            pl.semaphore_wait(near[d, k], 1)

    def await_all():
        @pl.when(jnp.logical_not(is_corner))
        def _():
            pl.semaphore_wait(all_sem, 1)

    pltpu.make_async_copy(inp, inp, load_sem.at[0]).wait()
    loads[3].wait()

    origin = (me[0] == 0) & (me[1] <= 1)
    next_up = origin & (me[2] == 1)
    origin = origin & (me[2] == 0)
    plane_rows = ((origin, devices - 2), (jnp.logical_not(origin), devices - 3))
    if relayed:
        relay_copy = pltpu.make_async_remote_copy(
            src_ref=rows_scratch[0],
            dst_ref=relay,
            send_sem=row_sent,
            recv_sem=relay_sem,
            device_id=neighbour(2, 1),
            device_id_type=MESH,
        )

    def speed_out():
        await_all()
        if not relayed:
            spread_start(0, 0, speed_row)
            return

        @pl.when(next_up)
        def _():
            relay_copy.wait_recv()
            spread_start(0, 0, jnp.maximum(speed_row, relay[...]))

        @pl.when(jnp.logical_not(origin | next_up))
        def _():
            spread_start(0, 0, speed_row)

    def row_parts(turn, stage):
        base = 2 * (turn * len(groups) + stage)
        mine, buf = rows_scratch[base : base + 2]
        return mine, buf, row_came.at[turn % 2 * len(groups) + stage]

    def spread_copy(turn, stage, i):
        mine, buf, came = row_parts(turn, stage)
        group = groups[stage]
        off = group_offsets(sizes, group)[i]
        there = tuple(
            lax.rem(sizes[d] - 1 - me[d] + off[d], sizes[d]) if d in group else me[d]
            for d in range(3)
        )
        can_be_me = all((off[d] + 1 - sizes[d]) % 2 == 0 or sizes[d] % 2 for d in group)
        copy = pltpu.make_async_remote_copy(
            src_ref=mine,
            dst_ref=buf.at[pl.ds(i, 1)],
            send_sem=row_sent,
            recv_sem=came,
            device_id=there,
            device_id_type=MESH,
        )
        return copy, can_be_me, functools.reduce(lambda a, b: a & b, [t == m for t, m in zip(there, me)])

    def spread_start(turn, stage, row):
        if turn or stage:
            before = turn * len(groups) + stage - 1
            spread_sent(before // len(groups), before % len(groups))
        mine, buf, _ = row_parts(turn, stage)
        mine[...] = row
        for i in range(buf.shape[0]):
            copy, can_be_me, is_me = spread_copy(turn, stage, i)
            if not can_be_me:
                copy.start()
                continue

            @pl.when(jnp.logical_not(is_me))
            def _(copy=copy):
                copy.start()

            @pl.when(is_me)
            def _(i=i):
                buf[i : i + 1] = row

    def spread_whole(turn, stage, rows=None):
        _, buf, came = row_parts(turn, stage)
        rows = buf.at[pl.ds(0, rows or buf.shape[0] - 1)]
        return pltpu.make_async_remote_copy(
            src_ref=rows,
            dst_ref=rows,
            send_sem=row_sent,
            recv_sem=came,
            device_id=device((1, 1, 1)),
            device_id_type=MESH,
        )

    def spread_end(turn, combine):
        for stage in range(len(groups)):
            if stage > 0:
                spread_start(turn, stage, row)
            if turn == 0 and relayed:
                for flag, rows in plane_rows:

                    @pl.when(flag)
                    def _(rows=rows):
                        spread_whole(turn, stage, rows).wait_recv()
            else:
                spread_whole(turn, stage).wait_recv()
            row = combine(row_parts(turn, stage)[1][...])
        return row

    def spread_sent(turn, stage):
        if turn == 0 and relayed:

            @pl.when(jnp.logical_not(origin))
            def _():
                spread_whole(turn, stage).wait_send()

            @pl.when(origin)
            def _():
                relay_copy.wait_send()

        else:
            spread_whole(turn, stage).wait_send()

    row_index = lax.broadcasted_iota(jnp.int32, (1, Y, Z), 1)
    lane_index = lax.broadcasted_iota(jnp.int32, (1, Y, Z), 2)
    index = {1: row_index, 2: lane_index}
    extent = {1: Y, 2: Z}

    def roll(value, shift, axis):
        return pltpu.roll(value, shift % value.shape[axis], axis)

    def mesh_group(value, axis, op):
        for s in (1, 2):
            low = (index[axis] & s) == 0
            value = op(value, jnp.where(low, roll(value, -s, axis), roll(value, s, axis)))
        return value

    def lane_group(value, op):
        place = lane_index & (P_SIZE - 1)
        for s in range(1, P_SIZE):
            ahead = roll(value, -s, 2)
            behind = roll(value, P_SIZE - s, 2)
            turned = jnp.where(place < P_SIZE - s, ahead, behind)
            whole = turned if s == 1 else op(whole, turned)
        return op(value, whole)

    def element(value, op):
        parts = value.reshape(EX, P_SIZE, Y, Z)
        value = op(op(parts[:, 0], parts[:, 1]), op(parts[:, 2], parts[:, 3]))
        return lane_group(mesh_group(value, 1, op), op)

    def nodes(value):
        return jnp.broadcast_to(value[:, None], (EX, P_SIZE, Y, Z)).reshape(X, Y, Z)

    def total(value, op):
        value = functools.reduce(op, [value[x] for x in range(X)])
        value = {jnp.minimum: jnp.min, jnp.maximum: jnp.max, jnp.add: jnp.sum}[op](
            value, axis=0, keepdims=True
        )
        return {jnp.minimum: jnp.min, jnp.maximum: jnp.max, jnp.add: jnp.sum}[op](
            value, axis=1, keepdims=True
        )

    late = me[2] == corner[2]
    last_x = me[0] == corner[0]
    last_chip = last_x & (me[1] >= corner[1] - 1) & late
    first_sides = ((0, 1),) if sizes[0] == 2 else ((0, 1), (1, -1))
    packs = zs.shape[0] - EX
    body = COMPS * 2 * X

    def remote(src, dst, sent, came, off):
        return pltpu.make_async_remote_copy(
            src_ref=src,
            dst_ref=dst,
            send_sem=sent_sem.at[sent],
            recv_sem=came_sem.at[came],
            device_id=device(off),
            device_id_type=MESH,
        )

    landing = {
        "x": (xh, 0, 0),
        "y": (yr, 1, 1),
        "z": (zr, 2, 2),
        "e": (er, 3, 3),
        ("b", 0): (pnx, 0, 4),
        ("b", 1): (pny, 1, 5),
        ("b", 2): (qz, 2, 6),
        "c": (bc, 3, 7),
    }

    def whole(key):
        ref, sent, came = landing[key]
        return remote(ref, ref, sent, came, step(2, 1))

    def arrive(key):
        whole(key).wait_recv()

    def sent_all(key):
        whole(key).wait_send()

    def send_x():
        for d, k in links:
            if d == 0:
                await_near(d, k)
        for side, k in ((0, 1), (1, -1)):
            at = X - 2 if side == 0 else 0
            remote(inp.at[:, at : at + 2], xh.at[side], 0, 0, step(0, k)).start()

    def send_e():
        for side, k in first_sides:
            remote(es, er.at[side], 3, 3, step(0, k)).start()

    def send_y():
        for side, k in ((0, 1), (1, -1)):
            if (1, k) in links:
                await_near(1, k)
            remote(ys.at[side], yr.at[side], 1, 1, step(1, k)).start()

    def send_z():
        for side, k in ((0, 1), (1, -1)):
            if (2, k) in links:
                await_near(2, k)
            remote(zs, zr.at[side], 2, 2, step(2, k)).start()
            if side == 0 and relayed:

                @pl.when(origin)
                def _():
                    rows_scratch[0][...] = speed_row
                    relay_copy.start()

    @pl.when(last_x & jnp.logical_not(last_chip))
    def _():
        send_x()

    own_inputs = [inp[c] for c in range(COMPS)]

    cons = conserved_of(own_inputs)
    density, _, inverse, velocity, pressure = primitives(cons)
    sound = sound_of(inverse, pressure)
    speed = jnp.abs(velocity[0]) + jnp.abs(velocity[1]) + jnp.abs(velocity[2]) + 3.0 * sound
    speed_row = jnp.broadcast_to(total(speed, jnp.maximum), (1, ROW))

    @pl.when(last_chip)
    def _():
        speed_out()
        send_x()

    for c in range(COMPS):
        for x in range(X):
            at = 2 * (c * X + x)
            ys[0, at : at + 2, :] = own_inputs[c][x, Y - 2 : Y, :]
            ys[1, at : at + 2, :] = own_inputs[c][x, 0:2, :]
    per_pack = Z // (4 * X)
    for v in range(packs):
        packed = jnp.zeros((1, Y, Z), jnp.float32)
        for c in range(v * per_pack, min((v + 1) * per_pack, COMPS)):
            for x in range(X):
                at = ((c - v * per_pack) * X + x) * 4
                moved = roll(own_inputs[c][x : x + 1], at + 2, 2)
                packed = jnp.where((lane_index >= at) & (lane_index < at + 4), moved, packed)
        zs[v] = packed[0]

    rho_min = element(density, jnp.minimum)
    p_min = element(pressure, jnp.minimum)
    widen = (
        lax.broadcasted_iota(jnp.int32, (EZ, Z), 1) // P_SIZE
        == lax.broadcasted_iota(jnp.int32, (EZ, Z), 0)
    ).astype(jnp.float32)
    heighten = (
        lax.broadcasted_iota(jnp.int32, (Y, EY), 0) // P_SIZE
        == lax.broadcasted_iota(jnp.int32, (Y, EY), 1)
    ).astype(jnp.float32)
    walls = []
    for d in range(3):
        layers = []
        for e in range(EX):
            flags = wa[d, e].astype(jnp.float32)
            flags = jnp.dot(flags, widen, preferred_element_type=jnp.float32)
            layers.append(jnp.dot(heighten, flags, preferred_element_type=jnp.float32)[None])
        walls.append(jnp.concatenate(layers, axis=0))
        turn_row = row_index & (P_SIZE - 1)
        fields = jnp.where(turn_row == 0, rho_min, jnp.where(turn_row == 1, p_min, walls[d]))
        if d == 0:
            es[...] = fields
        elif d == 1:
            for side in (0, 1):
                ys[side, body : body + EX * Y, :] = fields.reshape(EX * Y, Z)
        else:
            zs[packs : packs + EX] = fields

    def spread_rows(value, which):
        value = jnp.where((row_index & (P_SIZE - 1)) == which, value, jnp.inf)
        return mesh_group(value, 1, jnp.minimum)

    def edge(side, d, which):
        if d == 0:
            fields = er[0 if sizes[0] == 2 else side]
        elif d == 1:
            fields = yr[side, body : body + EX * Y, :].reshape(EX, Y, Z)
        else:
            fields = zr[side, packs : packs + EX]
        return spread_rows(fields, which)

    @pl.when(jnp.logical_not(late | last_x))
    def _():
        send_x()

    @pl.when(jnp.logical_not(late))
    def _():
        send_e()
        send_y()

    send_z()

    @pl.when(late & jnp.logical_not(last_x))
    def _():
        send_x()

    @pl.when(late)
    def _():
        send_e()
        send_y()

    @pl.when(jnp.logical_not(last_chip))
    def _():
        speed_out()

    def cyclic_fluxes(d, halo_inputs, number, first):
        n = extent[d]
        ix = index[d]
        halo = conserved_of(halo_inputs)
        _, _, h_inv, h_vel, h_p = primitives(halo)
        h_rate = jnp.abs(h_vel[d]) + sound_of(h_inv, h_p)
        rate = jnp.abs(velocity[d]) + sound

        def beside(value, beyond, k):
            edge_of = ix < k if k > 0 else ix >= n + k
            return roll(jnp.where(edge_of, beyond, value), -k, d)

        shifts = (-2, -1, 1, 2)
        along = {k: {d: beside(velocity[d], h_vel[d], k)} for k in shifts}
        p_at = {k: beside(pressure, h_p, k) for k in shifts}
        flag = roll(jnp.where(ix == 0, edge(1, d, 2), walls[d]), -1, d)
        ends = ix & (P_SIZE - 1)
        wall = nodes(jnp.where(ends == P_SIZE - 1, flag, 0.0)) > 0.5
        wall_low = nodes(jnp.where(ends == 0, walls[d], 0.0)) > 0.5
        half_rate = 0.5 * jnp.maximum(rate, beside(rate, h_rate, 1))
        half_low = 0.5 * jnp.maximum(beside(rate, h_rate, -1), rate)
        wall_p = 0.5 * (pressure + p_at[1])
        wall_p_low = 0.5 * (p_at[-1] + pressure)
        for c in range(COMPS):
            u_at = {k: beside(cons[c], halo[c], k) for k in shifts}
            f_at = {k: flux_term({c: u_at[k]}, along[k], p_at[k], c, d) for k in shifts}
            f = flux_term(cons, velocity, pressure, c, d)
            is_normal = c == SPECIES + d
            low, diff = face_pair(
                f_at[-1],
                f,
                f_at[1],
                f_at[2],
                u_at[1] - cons[c],
                half_rate,
                wall,
                wall_p if is_normal else None,
            )
            before_low, before_diff = face_pair(
                f_at[-2],
                f_at[-1],
                f,
                f_at[1],
                cons[c] - u_at[-1],
                half_low,
                wall_low,
                wall_p_low if is_normal else None,
            )
            du[number, c] = diff
            dw[number, c] = before_diff
            slot = max(c - SPECIES + 1, 0)
            if first:
                lows[c] = low - before_low
            else:
                lows[c] += low - before_low
            if first and c in (0, *range(SPECIES, COMPS)):
                deltas[slot] = diff - before_diff
            else:
                deltas[slot] += diff - before_diff

    arrive("y")
    for c in range(COMPS):
        hy[c] = own_inputs[c]
        for x in range(X):
            at = 2 * (c * X + x)
            hy[c, x, Y - 2 : Y, :] = yr[0, at : at + 2, :]
            hy[c, x, 0:2, :] = yr[1, at : at + 2, :]
    cyclic_fluxes(1, [hy[c] for c in range(COMPS)], 1, True)

    arrive("z")
    merged = [
        jnp.where((lane_index & 3) < 2, zr[0, v][None], zr[1, v][None]) for v in range(packs)
    ]
    z_halo = []
    for c in range(COMPS):
        layers = []
        for x in range(X):
            at = ((c % per_pack) * X + x) * 4
            layers.append(roll(merged[c // per_pack], -(at + 2), 2))
        z_halo.append(jnp.concatenate(layers, axis=0))
    cyclic_fluxes(2, z_halo, 0, False)

    arrive("x")
    arrive("e")
    sides = []
    for side in (0, 1):
        halo = conserved_of([xh[side, c] for c in range(COMPS)])
        _, _, h_inv, h_vel, h_p = primitives(halo)
        sides.append((halo, h_vel, h_p, jnp.abs(h_vel[0]) + sound_of(h_inv, h_p)))

    def joined(below, own, above):
        return jnp.concatenate([below, own, above], axis=0)

    rate = joined(sides[0][3], jnp.abs(velocity[0]) + sound, sides[1][3])
    p_ext = joined(sides[0][2], pressure, sides[1][2])
    half_rate = 0.5 * jnp.maximum(rate[1 : X + 2], rate[2 : X + 3])
    wall_p = 0.5 * (p_ext[1 : X + 2] + p_ext[2 : X + 3])
    planes = []
    for x in range(-1, X):
        if (x + 1) % P_SIZE:
            planes.append(jnp.zeros((1, Y, Z), jnp.float32))
        elif x == X - 1:
            planes.append(edge(1, 0, 2)[0:1])
        else:
            e = (x + 1) // P_SIZE
            planes.append(walls[0][e : e + 1])
    wall = jnp.concatenate(planes, axis=0) > 0.5
    for c in range(COMPS):
        f = joined(
            flux_term(sides[0][0], sides[0][1], sides[0][2], c, 0),
            flux_term(cons, velocity, pressure, c, 0),
            flux_term(sides[1][0], sides[1][1], sides[1][2], c, 0),
        )
        u = joined(sides[0][0][c], cons[c], sides[1][0][c])
        low, diff = face_pair(
            f[0 : X + 1],
            f[1 : X + 2],
            f[2 : X + 3],
            f[3 : X + 4],
            u[2 : X + 3] - u[1 : X + 2],
            half_rate,
            wall,
            wall_p if c == SPECIES else None,
        )
        dx[c] = diff
        lows[c] += low[1:] - low[:-1]
        deltas[max(c - SPECIES + 1, 0)] += diff[1:] - diff[:-1]

    def bound(own, which):
        best = own
        for d in (1, 2):
            n = extent[d]
            up = jnp.where(index[d] < P_SIZE, edge(1, d, which), own)
            down = jnp.where(index[d] >= n - P_SIZE, edge(0, d, which), own)
            best = jnp.minimum(best, jnp.minimum(roll(up, -P_SIZE, d), roll(down, P_SIZE, d)))
        chain = joined(edge(0, 0, which)[EX - 1 : EX], own, edge(1, 0, which)[0:1])
        return jnp.minimum(best, jnp.minimum(chain[:EX], chain[2:]))

    rho_bound = bound(rho_min, 0)
    p_bound = bound(p_min, 1)

    fluxes = [sum([lows[c] for c in range(1, SPECIES)], lows[0])]
    fluxes += [lows[c] for c in range(SPECIES, COMPS)]
    jumps = [deltas[i] for i in range(COMPS - SPECIES + 1)]

    speed_max = spread_end(0, lambda rows: jnp.max(rows, axis=0, keepdims=True))
    ratio = (COURANT / speed_max).reshape(1, 1, ROW)

    def five(values):
        return [sum([values[c] for c in range(1, SPECIES)], values[0])] + [
            values[c] for c in range(SPECIES, COMPS)
        ]

    low_five = [u - ratio * f for u, f in zip(five(cons), fluxes)]
    d_five = [-(ratio * d) for d in jumps]
    d_rho = d_five[0]
    rho_scale = 1.0 / jnp.maximum(-d_rho, SLOPE_FLOOR)
    count = X * Y * Z * sizes[0] * sizes[1] * sizes[2]
    stat_lane = lax.broadcasted_iota(jnp.int32, (1, ROW), 1)

    def combine_stats(rows):
        return jnp.where(
            stat_lane < 2,
            jnp.min(rows, axis=0, keepdims=True),
            jnp.sum(rows, axis=0, keepdims=True),
        )

    def broadcast_stats(got):
        lowest_rho = got[0:1, 0:1].reshape(1, 1, 1)
        lowest_p = got[0:1, 1:2].reshape(1, 1, 1)
        spread = got[0:1, 2:3].reshape(1, 1, 1) * (1.0 / count) + SPREAD
        return lowest_rho, lowest_p, spread

    def next_blend(got, packed):
        t_density, rho_scale, t_p, p_scale, rho_bound, p_bound, mean_square, base = packed
        lowest_rho, lowest_p, spread = got
        rho_target = rho_bound - RELAX * jnp.maximum(rho_bound - lowest_rho, 0.0)
        p_target = p_bound - RELAX * jnp.maximum(p_bound - lowest_p, 0.0)
        step_rho = jnp.minimum(t_density - nodes(rho_target), 0.0) * rho_scale
        step_p = jnp.minimum(t_p - nodes(p_target), 0.0) * p_scale
        lowered = element(jnp.minimum(step_rho, step_p), jnp.minimum)
        cap = spread / (spread + mean_square)
        return jnp.maximum(jnp.minimum(cap, base + lowered), 0.0)

    per_edge = Z // (2 * P_SIZE)
    depth = 10 * X + 2 * EX

    def share(fields):
        at = 0
        for value in fields:
            pk[at : at + value.shape[0]] = value
            at += value.shape[0]
        for side, k in first_sides:
            remote(pk, pnx.at[side], 0, 4, step(0, k)).start()
        for side, k in ((0, 1), (1, -1)):
            rows = pl.ds(Y - P_SIZE, P_SIZE) if side == 0 else pl.ds(0, P_SIZE)
            remote(pk.at[:, rows], pny.at[:, rows], 1, 5, step(1, k)).start()
        items = [value[x : x + 1] for value in fields for x in range(value.shape[0])]
        for v in range(pz.shape[0]):
            packed = jnp.zeros((1, Y, Z), jnp.float32)
            for j, item in enumerate(items[v * per_edge : (v + 1) * per_edge]):
                at = 2 * P_SIZE * j
                moved = roll(item, at + P_SIZE, 2)
                inside = (lane_index >= at) & (lane_index < at + 2 * P_SIZE)
                packed = jnp.where(inside, moved, packed)
            pz[v] = packed[0]
        for side, k in ((0, 1), (1, -1)):
            remote(pz, qz.at[side], 2, 6, step(2, k)).start()

    sides_x = len(first_sides)

    def share_blend():
        bs[...] = blend
        for side, k in first_sides:
            there = bc.at[pl.ds(side * EX, EX)]
            remote(bs, there, 3, 7, step(0, k)).start()
        for side, k in ((0, 1), (1, -1)):
            there = bc.at[pl.ds((sides_x + 1 + side) * EX, EX)]
            remote(bs, there, 3, 7, step(2, k)).start()
            rows = pl.ds(Y - P_SIZE, P_SIZE) if side == 0 else pl.ds(0, P_SIZE)
            there = bc.at[pl.ds(sides_x * EX, EX), rows]
            remote(bs.at[:, rows], there, 3, 7, step(1, k)).start()

    def trial_of(low, d, low_sigma, blend):
        weight = None if blend is None else nodes(blend)
        trial = [a + (b if weight is None else weight * b) for a, b in zip(low, d)]
        safe, speeds, p = state_of(trial[0], trial[1:4], trial[4])
        residual = entropy(trial[0], safe, p) - low_sigma
        return trial[0], speeds, p, residual * residual

    def scales_of(d, speeds, square):
        cross = speeds[0] * d[1] + speeds[1] * d[2] + speeds[2] * d[3]
        speed2 = speeds[0] * speeds[0] + speeds[1] * speeds[1] + speeds[2] * speeds[2]
        slope = (GAMMA - 1.0) * (d[4] - cross + 0.5 * speed2 * d[0])
        mean_square = element(square, jnp.add) * (1.0 / (P_SIZE**3))
        return 1.0 / jnp.maximum(-slope, SLOPE_FLOOR), mean_square

    def sigma_of(low):
        safe, _, p = state_of(low[0], low[1:4], low[4])
        return entropy(low[0], safe, p)

    def neighbour_low(layer):
        low = [layer(i * X, (i + 1) * X) for i in range(5)]
        d = [layer(i * X, (i + 1) * X) for i in range(5, 10)]
        bounds = [layer(10 * X + i * EX, 10 * X + (i + 1) * EX) for i in range(2)]
        scale = 1.0 / jnp.maximum(-d[0], SLOPE_FLOOR)
        return low, d, sigma_of(low), scale, bounds

    def neighbour_fields(known, blend):
        low, d, sigma, scale, bounds = known
        density, speeds, p, square = trial_of(low, d, sigma, blend)
        p_scale, mean_square = scales_of(d, speeds, square)
        return density, scale, p, p_scale, bounds[0], bounds[1], mean_square, blend

    low_sigma = sigma_of(low_five)
    blend = None
    for newton in range(ITERS):
        t_density, t_vel, t_p, square = trial_of(low_five, d_five, low_sigma, blend)
        stats = jnp.where(
            stat_lane == 0,
            total(t_density, jnp.minimum),
            jnp.where(stat_lane == 1, total(t_p, jnp.minimum), total(square, jnp.add)),
        )
        spread_start(newton + 1, 0, stats)
        if newton == ITERS - 2:
            for key in ("x", "y", "z", "e"):
                sent_all(key)
            share((*low_five, *d_five, rho_bound, p_bound))
        p_scale, mean_square = scales_of(d_five, t_vel, square)
        base = jnp.ones((EX, Y, Z), jnp.float32) if blend is None else blend
        beside = {}
        if newton == ITERS - 1:
            for d in (1, 2, 0):
                arrive(("b", d))
            known = {1: neighbour_low(lambda a, b: pny[a:b])}
            near = (lane_index & (2 * P_SIZE - 1)) < P_SIZE
            edges = [
                jnp.where(near, qz[0, v][None], qz[1, v][None]) for v in range(pz.shape[0])
            ]
            items = [
                roll(edges[j // per_edge], -(2 * P_SIZE * (j % per_edge) + P_SIZE), 2)
                for j in range(depth)
            ]
            known[2] = neighbour_low(lambda a, b: jnp.concatenate(items[a:b], axis=0))
            for side in range(sides_x):
                known[0, side] = neighbour_low(lambda a, b: pnx[side, a:b])
            for d in range(3):
                sent_all(("b", d))
            sent_all("c")
            arrive("c")
            at = sides_x * EX
            weights = {(0, side): bc[side * EX : (side + 1) * EX] for side in range(sides_x)}
            weights[1] = bc[at : at + EX]
            weights[2] = jnp.where(
                lane_index < P_SIZE, bc[at + 2 * EX : at + 3 * EX], bc[at + EX : at + 2 * EX]
            )
            beside = {key: neighbour_fields(known[key], weights[key]) for key in known}
        got = broadcast_stats(spread_end(newton + 1, combine_stats))
        blend = next_blend(
            got, (t_density, rho_scale, t_p, p_scale, rho_bound, p_bound, mean_square, base)
        )
        if newton == ITERS - 2:
            share_blend()

    beside = {key: next_blend(got, packed) for key, packed in beside.items()}
    beside.setdefault((0, 1), beside[0, 0])

    theta = []
    for d in (2, 1):
        above = roll(jnp.where(index[d] == 0, beside[d], blend), -1, d)
        below = roll(jnp.where(index[d] == extent[d] - 1, beside[d], blend), 1, d)
        theta.append((nodes(jnp.minimum(blend, above)), nodes(jnp.minimum(blend, below))))
    x_blend = joined(beside[0, 0][EX - 1 : EX], nodes(blend), beside[0, 1][0:1])
    x_theta = jnp.minimum(x_blend[:-1], x_blend[1:])
    for c in range(COMPS):
        faces = x_theta * dx[c]
        change = lows[c] + (faces[1:] - faces[:-1])
        for number in range(2):
            upper, lower = theta[number]
            change += upper * du[number, c] - lower * dw[number, c]
        out[c] = cons[c] - ratio * change

    chosen = (lax.broadcasted_iota(jnp.int32, (Y, Z), 1) * P_SIZE) & (Z - 1)
    for e in range(EX):
        few = jnp.take_along_axis(blend[e], chosen, axis=1, mode="promise_in_bounds")[:, :EZ]
        bl[e] = jnp.concatenate([few[j * P_SIZE : j * P_SIZE + 1] for j in range(EY)], axis=0)

    spread_sent(ITERS, len(groups) - 1)


def store(state, weights, state_hbm, weights_hbm, sem):
    copies = [
        pltpu.make_async_copy(state, state_hbm, sem.at[0]),
        pltpu.make_async_copy(weights, weights_hbm, sem.at[1]),
    ]
    for copy in copies:
        copy.start()
    for copy in copies:
        copy.wait()


def solution(mesh):
    sizes = tuple(mesh.shape[name] for name in AXES)

    def local(species, velocity_in, pressure_in, wall_types):
        X, Y, Z = pressure_in.shape
        EX, EY, EZ = wall_types.shape[1:]
        packs = -(-COMPS // (Z // (4 * X)))
        depth = 10 * X + 2 * EX
        edge_packs = -(-depth // (Z // (2 * P_SIZE)))
        vmem = lambda *shape: pltpu.VMEM(shape, jnp.float32)
        groups = reduce_groups(sizes)
        dma = pltpu.SemaphoreType.DMA
        sides = 1 if sizes[0] == 2 else 2
        rows_scratch = []
        for _ in range(ITERS + 1):
            for group in groups:
                rows_scratch += [vmem(1, ROW), vmem(len(group_offsets(sizes, group)), ROW)]
        state, weights = (
            pl.pallas_call(
                functools.partial(kernel, sizes),
                out_shape=[
                    pltpu.VMEM((COMPS, X, Y, Z), jnp.float32),
                    pltpu.VMEM((EX, EY, EZ), jnp.float32),
                ],
                in_specs=[pl.BlockSpec(memory_space=pltpu.HBM)] * 4,
                out_specs=[pl.BlockSpec(memory_space=pltpu.VMEM)] * 2,
                scratch_shapes=[
                    vmem(COMPS, X, Y, Z),
                    pltpu.VMEM((3, EX, EY, EZ), jnp.int32),
                    dma((2,)),
                    vmem(2, COMPS, 2, Y, Z),
                    vmem(2, COMPS * 2 * X + EX * Y, Z),
                    vmem(2, COMPS * 2 * X + EX * Y, Z),
                    vmem(COMPS, X, Y, Z),
                    vmem(packs + EX, Y, Z),
                    vmem(2, packs + EX, Y, Z),
                    vmem(EX, Y, Z),
                    vmem(sides, EX, Y, Z),
                    vmem(depth, Y, Z),
                    vmem(sides, depth, Y, Z),
                    vmem(depth, Y, Z),
                    vmem(edge_packs, Y, Z),
                    vmem(2, edge_packs, Y, Z),
                    vmem(EX, Y, Z),
                    vmem((sides + 3) * EX, Y, Z),
                    vmem(COMPS, X + 1, Y, Z),
                    vmem(2, COMPS, X, Y, Z),
                    vmem(2, COMPS, X, Y, Z),
                    vmem(COMPS, X, Y, Z),
                    vmem(COMPS - SPECIES + 1, X, Y, Z),
                    dma((4,)),
                    dma((8,)),
                    pltpu.SemaphoreType.REGULAR((len(halo_links(sizes)),)),
                    pltpu.SemaphoreType.REGULAR,
                    vmem(1, ROW),
                    dma(()),
                    dma(()),
                    dma((2 * len(groups),)),
                ]
                + rows_scratch,
                compiler_params=pltpu.CompilerParams(collective_id=0, has_side_effects=True),
            )(species, velocity_in, pressure_in, wall_types)
        )
        return tuple(
            pl.pallas_call(
                store,
                out_shape=[
                    jax.ShapeDtypeStruct((COMPS, X, Y, Z), jnp.float32),
                    jax.ShapeDtypeStruct((EX, EY, EZ), jnp.float32),
                ],
                in_specs=[pl.BlockSpec(memory_space=pltpu.VMEM)] * 2,
                out_specs=[pl.BlockSpec(memory_space=pltpu.HBM)] * 2,
                scratch_shapes=[pltpu.SemaphoreType.DMA((2,))],
            )(*[pltpu.with_memory_space_constraint(v, pltpu.VMEM) for v in (state, weights)])
        )

    in_specs = (
        P(None, "gx", "gy", "gz"),
        P(None, "gx", "gy", "gz"),
        P("gx", "gy", "gz"),
        P(None, "gx", "gy", "gz"),
    )
    out_specs = (P(None, "gx", "gy", "gz"), P("gx", "gy", "gz"))
    return jax.shard_map(local, mesh=mesh, in_specs=in_specs, out_specs=out_specs, check_vma=False)
```

```python
import functools
import itertools

import jax
import jax.numpy as jnp
from jax import lax
from jax.experimental import pallas as pl
from jax.experimental.pallas import tpu as pltpu
from jax.sharding import PartitionSpec as P

SPECIES = 5
P_SIZE = 4
ITERS = 2
GAMMA = 1.4
COURANT = 0.4
FLOOR = 0.1
SLOPE_FLOOR = 0.01
SPREAD = 0.002
RELAX = 0.1

COMPS = SPECIES + 4
AXES = ("gx", "gy", "gz")
ROW = 128
DIRECT = 64
MESH = pl.DeviceIdType.MESH


def reduce_groups(sizes):
    if sizes[0] * sizes[1] * sizes[2] <= DIRECT:
        return [(0, 1, 2)]
    return [(2,), (1,), (0,)]


def group_offsets(sizes, group):
    spans = [range(sizes[d]) if d in group else (0,) for d in range(3)]
    far = lambda off: sum(min(off[d], sizes[d] - off[d]) for d in range(3))
    return sorted(itertools.product(*spans), key=far)


def halo_links(sizes):
    return [(d, k) for d in range(3) for k in ((1,) if sizes[d] == 2 else (1, -1))]


def conserved_of(inputs):
    species, velocity, pressure = inputs[:SPECIES], inputs[SPECIES : SPECIES + 3], inputs[-1]
    density = sum(species[1:], species[0])
    square = velocity[0] * velocity[0] + velocity[1] * velocity[1] + velocity[2] * velocity[2]
    energy = pressure * (1.0 / (GAMMA - 1.0)) + 0.5 * density * square
    return list(species) + [density * v for v in velocity] + [energy]


def primitives(cons):
    density = sum(cons[1:SPECIES], cons[0])
    safe = jnp.maximum(density, FLOOR)
    inverse = 1.0 / safe
    momentum = cons[SPECIES : SPECIES + 3]
    velocity = [m * inverse for m in momentum]
    kinetic = momentum[0] * velocity[0] + momentum[1] * velocity[1] + momentum[2] * velocity[2]
    pressure = (GAMMA - 1.0) * (cons[SPECIES + 3] - 0.5 * kinetic)
    return density, safe, inverse, velocity, pressure


def state_of(density, momentum, energy):
    safe = jnp.maximum(density, FLOOR)
    inverse = 1.0 / safe
    velocity = [m * inverse for m in momentum]
    kinetic = momentum[0] * velocity[0] + momentum[1] * velocity[1] + momentum[2] * velocity[2]
    pressure = (GAMMA - 1.0) * (energy - 0.5 * kinetic)
    return safe, velocity, pressure


def sound_of(inverse, pressure):
    return jnp.sqrt(GAMMA * jnp.maximum(pressure, FLOOR) * inverse)


def entropy(density, safe, pressure):
    return density * (jnp.log(jnp.maximum(pressure, FLOOR)) - GAMMA * jnp.log(safe))


def flux_term(cons, velocity, pressure, comp, d):
    term = cons[comp] * velocity[d]
    if comp == SPECIES + d:
        term = term + pressure
    if comp == SPECIES + 3:
        term = term + pressure * velocity[d]
    return term


def face_pair(mm, left, right, pp, jump, rate, wall, wall_value):
    both = left + right
    high = (7.0 * both - (mm + pp)) * (1.0 / 12.0)
    low = 0.5 * both - rate * jump
    keep = 0.0 if wall_value is None else wall_value
    diff = jnp.where(wall, 0.0, high - low)
    return jnp.where(wall, keep, low), diff


def kernel(
    sizes, sp_hbm, ve_hbm, pr_hbm, wa_hbm, out, bl, inp, wa, load_sem,
    xh, ys, yr, hy, zs, zr, es, er, pk, nb, pz, bs, bc, dx, du, dw, lows, deltas,
    sent_sem, came_sem, near_sem, all_sem, relay, relay_sem, row_sent, row_came, *rows_scratch
):
    X, Y, Z = inp.shape[1:]
    EX, EY, EZ = wa.shape[1:]
    loads = [
        pltpu.make_async_copy(sp_hbm, inp.at[:SPECIES], load_sem.at[0]),
        pltpu.make_async_copy(ve_hbm, inp.at[SPECIES : SPECIES + 3], load_sem.at[0]),
        pltpu.make_async_copy(pr_hbm, inp.at[SPECIES + 3], load_sem.at[0]),
        pltpu.make_async_copy(wa_hbm, wa, load_sem.at[1]),
    ]
    for copy in loads:
        copy.start()
    me = [lax.axis_index(name) for name in AXES]
    groups = reduce_groups(sizes)

    place = [[me[d]] + [lax.rem(me[d] + k, sizes[d]) for k in range(1, sizes[d])] for d in range(3)]

    def device(off):
        return tuple(place[d][off[d]] for d in range(3))

    def step(d, k):
        return tuple(k % sizes[d] if a == d else 0 for a in range(3))

    relayed = len(groups) == 1
    if relayed:
        rows_scratch[1][...] = jnp.zeros_like(rows_scratch[1])

    def traced(flag):
        return jnp.where(flag, 1, 0).astype(jnp.int32)

    links = halo_links(sizes)
    near = {link: near_sem.at[i] for i, link in enumerate(links)}

    def later(d, k):
        return me[d] != sizes[d] - 1 if k == 1 else me[d] == 0

    def neighbour(d, k):
        return device(step(d, k))

    corner = tuple(n - 1 for n in sizes)
    is_corner = (me[0] == corner[0]) & (me[1] == corner[1]) & (me[2] == corner[2])
    devices = sizes[0] * sizes[1] * sizes[2]
    barrier = pltpu.get_barrier_semaphore()

    @pl.when(jnp.logical_not(is_corner))
    def _():
        pl.semaphore_signal(barrier, inc=1, device_id=corner, device_id_type=MESH)

    expected = jnp.where(is_corner, devices - 1, 0).astype(jnp.int32)
    for d, k in links:

        @pl.when(later(d, k))
        def _(d=d, k=k):
            pl.semaphore_signal(barrier, inc=1, device_id=neighbour(d, k), device_id_type=MESH)

        expected = expected + 1 - traced(later(d, k))

    @pl.when(expected > 0)
    def _():
        pl.semaphore_wait(barrier, expected)

    for d, k in links:
        back = (d, k if sizes[d] == 2 else -k)

        @pl.when(jnp.logical_not(later(d, k)))
        def _(d=d, k=k, back=back):
            pl.semaphore_signal(
                near[back], inc=1, device_id=neighbour(d, k), device_id_type=MESH
            )

    @pl.when(is_corner)
    def _():
        def tell(i, carry):
            z = lax.rem(i, sizes[2])
            y = lax.rem(lax.div(i, sizes[2]), sizes[1])
            x = lax.div(i, sizes[2] * sizes[1])
            pl.semaphore_signal(all_sem, inc=1, device_id=(x, y, z), device_id_type=MESH)
            return carry

        if devices <= DIRECT:
            for at in itertools.product(*[range(n) for n in sizes]):
                if at != corner:
                    pl.semaphore_signal(all_sem, inc=1, device_id=at, device_id_type=MESH)
        else:
            lax.fori_loop(0, devices - 1, tell, 0)

    def await_near(d, k):
        @pl.when(later(d, k))
        def _():
            pl.semaphore_wait(near[d, k], 1)

    def await_all():
        @pl.when(jnp.logical_not(is_corner))
        def _():
            pl.semaphore_wait(all_sem, 1)

    pltpu.make_async_copy(inp, inp, load_sem.at[0]).wait()
    loads[3].wait()

    origin = (me[0] == 0) & (me[1] <= 1)
    next_up = origin & (me[2] == 1)
    origin = origin & (me[2] == 0)
    plane_rows = ((origin, devices - 2), (jnp.logical_not(origin), devices - 3))
    if relayed:
        relay_copy = pltpu.make_async_remote_copy(
            src_ref=rows_scratch[0],
            dst_ref=relay,
            send_sem=row_sent,
            recv_sem=relay_sem,
            device_id=neighbour(2, 1),
            device_id_type=MESH,
        )

    def speed_out():
        await_all()
        if not relayed:
            spread_start(0, 0, speed_row)
            return

        @pl.when(next_up)
        def _():
            relay_copy.wait_recv()
            spread_start(0, 0, jnp.maximum(speed_row, relay[...]))

        @pl.when(jnp.logical_not(origin | next_up))
        def _():
            spread_start(0, 0, speed_row)

    def row_parts(turn, stage):
        base = 2 * (turn * len(groups) + stage)
        mine, buf = rows_scratch[base : base + 2]
        return mine, buf, row_came.at[turn % 2 * len(groups) + stage]

    def spread_copy(turn, stage, i):
        mine, buf, came = row_parts(turn, stage)
        group = groups[stage]
        off = group_offsets(sizes, group)[i]
        there = tuple(
            lax.rem(sizes[d] - 1 - me[d] + off[d], sizes[d]) if d in group else me[d]
            for d in range(3)
        )
        can_be_me = all((off[d] + 1 - sizes[d]) % 2 == 0 or sizes[d] % 2 for d in group)
        copy = pltpu.make_async_remote_copy(
            src_ref=mine,
            dst_ref=buf.at[pl.ds(i, 1)],
            send_sem=row_sent,
            recv_sem=came,
            device_id=there,
            device_id_type=MESH,
        )
        return copy, can_be_me, functools.reduce(lambda a, b: a & b, [t == m for t, m in zip(there, me)])

    def spread_start(turn, stage, row):
        if turn or stage:
            before = turn * len(groups) + stage - 1
            spread_sent(before // len(groups), before % len(groups))
        mine, buf, _ = row_parts(turn, stage)
        mine[...] = row
        for i in range(buf.shape[0]):
            copy, can_be_me, is_me = spread_copy(turn, stage, i)
            if not can_be_me:
                copy.start()
                continue

            @pl.when(jnp.logical_not(is_me))
            def _(copy=copy):
                copy.start()

            @pl.when(is_me)
            def _(i=i):
                buf[i : i + 1] = row

    def spread_whole(turn, stage, rows=None):
        _, buf, came = row_parts(turn, stage)
        rows = buf.at[pl.ds(0, rows or buf.shape[0] - 1)]
        return pltpu.make_async_remote_copy(
            src_ref=rows,
            dst_ref=rows,
            send_sem=row_sent,
            recv_sem=came,
            device_id=device((1, 1, 1)),
            device_id_type=MESH,
        )

    def spread_end(turn, combine):
        for stage in range(len(groups)):
            if stage > 0:
                spread_start(turn, stage, row)
            if turn == 0 and relayed:
                for flag, rows in plane_rows:

                    @pl.when(flag)
                    def _(rows=rows):
                        spread_whole(turn, stage, rows).wait_recv()
            else:
                spread_whole(turn, stage).wait_recv()
            row = combine(row_parts(turn, stage)[1][...])
        return row

    def spread_sent(turn, stage):
        if turn == 0 and relayed:

            @pl.when(jnp.logical_not(origin))
            def _():
                spread_whole(turn, stage).wait_send()

            @pl.when(origin)
            def _():
                relay_copy.wait_send()

        else:
            spread_whole(turn, stage).wait_send()

    row_index = lax.broadcasted_iota(jnp.int32, (1, Y, Z), 1)
    lane_index = lax.broadcasted_iota(jnp.int32, (1, Y, Z), 2)
    index = {1: row_index, 2: lane_index}
    extent = {1: Y, 2: Z}

    def roll(value, shift, axis):
        return pltpu.roll(value, shift % value.shape[axis], axis)

    def mesh_group(value, axis, op):
        for s in (1, 2):
            low = (index[axis] & s) == 0
            value = op(value, jnp.where(low, roll(value, -s, axis), roll(value, s, axis)))
        return value

    def lane_group(value, op):
        place = lane_index & (P_SIZE - 1)
        for s in range(1, P_SIZE):
            ahead = roll(value, -s, 2)
            behind = roll(value, P_SIZE - s, 2)
            turned = jnp.where(place < P_SIZE - s, ahead, behind)
            whole = turned if s == 1 else op(whole, turned)
        return op(value, whole)

    def element(value, op):
        parts = value.reshape(EX, P_SIZE, Y, Z)
        value = op(op(parts[:, 0], parts[:, 1]), op(parts[:, 2], parts[:, 3]))
        return lane_group(mesh_group(value, 1, op), op)

    def nodes(value):
        return jnp.broadcast_to(value[:, None], (EX, P_SIZE, Y, Z)).reshape(X, Y, Z)

    def total(value, op):
        value = functools.reduce(op, [value[x] for x in range(X)])
        value = {jnp.minimum: jnp.min, jnp.maximum: jnp.max, jnp.add: jnp.sum}[op](
            value, axis=0, keepdims=True
        )
        return {jnp.minimum: jnp.min, jnp.maximum: jnp.max, jnp.add: jnp.sum}[op](
            value, axis=1, keepdims=True
        )

    late = me[2] == corner[2]
    last_x = me[0] == corner[0]
    last_chip = last_x & (me[1] >= corner[1] - 1) & late
    first_sides = ((0, 1),) if sizes[0] == 2 else ((0, 1), (1, -1))
    packs = zs.shape[0] - EX
    body = COMPS * 2 * X

    def remote(src, dst, sent, came, off):
        return pltpu.make_async_remote_copy(
            src_ref=src,
            dst_ref=dst,
            send_sem=sent_sem.at[sent],
            recv_sem=came_sem.at[came],
            device_id=device(off),
            device_id_type=MESH,
        )

    landing = {
        "x": (xh, 0, 0),
        "y": (yr, 1, 1),
        "z": (zr, 2, 2),
        "e": (er, 3, 3),
        "b": (nb, 0, 4),
        "c": (bc, 3, 5),
    }

    def whole(key):
        ref, sent, came = landing[key]
        return remote(ref, ref, sent, came, step(2, 1))

    def arrive(key):
        whole(key).wait_recv()

    def sent_all(key):
        whole(key).wait_send()

    def send_x():
        for d, k in links:
            if d == 0:
                await_near(d, k)
        for side, k in ((0, 1), (1, -1)):
            at = X - 2 if side == 0 else 0
            remote(inp.at[:, at : at + 2], xh.at[side], 0, 0, step(0, k)).start()

    def send_e():
        for side, k in first_sides:
            remote(es, er.at[side], 3, 3, step(0, k)).start()

    def send_y():
        for side, k in ((0, 1), (1, -1)):
            if (1, k) in links:
                await_near(1, k)
            remote(ys.at[side], yr.at[side], 1, 1, step(1, k)).start()

    def send_z():
        for side, k in ((0, 1), (1, -1)):
            if (2, k) in links:
                await_near(2, k)
            remote(zs, zr.at[side], 2, 2, step(2, k)).start()
            if side == 0 and relayed:

                @pl.when(origin)
                def _():
                    rows_scratch[0][...] = speed_row
                    relay_copy.start()

    @pl.when(last_x & jnp.logical_not(last_chip))
    def _():
        send_x()

    own_inputs = [inp[c] for c in range(COMPS)]

    cons = conserved_of(own_inputs)
    density, _, inverse, velocity, pressure = primitives(cons)
    sound = sound_of(inverse, pressure)
    speed = jnp.abs(velocity[0]) + jnp.abs(velocity[1]) + jnp.abs(velocity[2]) + 3.0 * sound
    speed_row = jnp.broadcast_to(total(speed, jnp.maximum), (1, ROW))

    @pl.when(last_chip)
    def _():
        speed_out()
        send_x()

    for c in range(COMPS):
        for x in range(X):
            at = 2 * (c * X + x)
            ys[0, at : at + 2, :] = own_inputs[c][x, Y - 2 : Y, :]
            ys[1, at : at + 2, :] = own_inputs[c][x, 0:2, :]
    per_pack = Z // (4 * X)
    for v in range(packs):
        packed = jnp.zeros((1, Y, Z), jnp.float32)
        for c in range(v * per_pack, min((v + 1) * per_pack, COMPS)):
            for x in range(X):
                at = ((c - v * per_pack) * X + x) * 4
                moved = roll(own_inputs[c][x : x + 1], at + 2, 2)
                packed = jnp.where((lane_index >= at) & (lane_index < at + 4), moved, packed)
        zs[v] = packed[0]

    rho_min = element(density, jnp.minimum)
    p_min = element(pressure, jnp.minimum)
    widen = (
        lax.broadcasted_iota(jnp.int32, (EZ, Z), 1) // P_SIZE
        == lax.broadcasted_iota(jnp.int32, (EZ, Z), 0)
    ).astype(jnp.float32)
    heighten = (
        lax.broadcasted_iota(jnp.int32, (Y, EY), 0) // P_SIZE
        == lax.broadcasted_iota(jnp.int32, (Y, EY), 1)
    ).astype(jnp.float32)
    walls = []
    for d in range(3):
        layers = []
        for e in range(EX):
            flags = wa[d, e].astype(jnp.float32)
            flags = jnp.dot(flags, widen, preferred_element_type=jnp.float32)
            layers.append(jnp.dot(heighten, flags, preferred_element_type=jnp.float32)[None])
        walls.append(jnp.concatenate(layers, axis=0))
        turn_row = row_index & (P_SIZE - 1)
        fields = jnp.where(turn_row == 0, rho_min, jnp.where(turn_row == 1, p_min, walls[d]))
        if d == 0:
            es[...] = fields
        elif d == 1:
            for side in (0, 1):
                ys[side, body : body + EX * Y, :] = fields.reshape(EX * Y, Z)
        else:
            zs[packs : packs + EX] = fields

    def spread_rows(value, which):
        value = jnp.where((row_index & (P_SIZE - 1)) == which, value, jnp.inf)
        return mesh_group(value, 1, jnp.minimum)

    def edge(side, d, which):
        if d == 0:
            fields = er[0 if sizes[0] == 2 else side]
        elif d == 1:
            fields = yr[side, body : body + EX * Y, :].reshape(EX, Y, Z)
        else:
            fields = zr[side, packs : packs + EX]
        return spread_rows(fields, which)

    @pl.when(jnp.logical_not(late | last_x))
    def _():
        send_x()

    @pl.when(jnp.logical_not(late))
    def _():
        send_e()
        send_y()

    send_z()

    @pl.when(late & jnp.logical_not(last_x))
    def _():
        send_x()

    @pl.when(late)
    def _():
        send_e()
        send_y()

    @pl.when(jnp.logical_not(last_chip))
    def _():
        speed_out()

    def cyclic_fluxes(d, halo_inputs, number, first):
        n = extent[d]
        ix = index[d]
        halo = conserved_of(halo_inputs)
        _, _, h_inv, h_vel, h_p = primitives(halo)
        h_rate = jnp.abs(h_vel[d]) + sound_of(h_inv, h_p)
        rate = jnp.abs(velocity[d]) + sound

        def beside(value, beyond, k):
            edge_of = ix < k if k > 0 else ix >= n + k
            return roll(jnp.where(edge_of, beyond, value), -k, d)

        shifts = (-2, -1, 1, 2)
        along = {k: {d: beside(velocity[d], h_vel[d], k)} for k in shifts}
        p_at = {k: beside(pressure, h_p, k) for k in shifts}
        flag = roll(jnp.where(ix == 0, edge(1, d, 2), walls[d]), -1, d)
        ends = ix & (P_SIZE - 1)
        wall = nodes(jnp.where(ends == P_SIZE - 1, flag, 0.0)) > 0.5
        wall_low = nodes(jnp.where(ends == 0, walls[d], 0.0)) > 0.5
        half_rate = 0.5 * jnp.maximum(rate, beside(rate, h_rate, 1))
        half_low = 0.5 * jnp.maximum(beside(rate, h_rate, -1), rate)
        wall_p = 0.5 * (pressure + p_at[1])
        wall_p_low = 0.5 * (p_at[-1] + pressure)
        for c in range(COMPS):
            u_at = {k: beside(cons[c], halo[c], k) for k in shifts}
            f_at = {k: flux_term({c: u_at[k]}, along[k], p_at[k], c, d) for k in shifts}
            f = flux_term(cons, velocity, pressure, c, d)
            is_normal = c == SPECIES + d
            low, diff = face_pair(
                f_at[-1],
                f,
                f_at[1],
                f_at[2],
                u_at[1] - cons[c],
                half_rate,
                wall,
                wall_p if is_normal else None,
            )
            before_low, before_diff = face_pair(
                f_at[-2],
                f_at[-1],
                f,
                f_at[1],
                cons[c] - u_at[-1],
                half_low,
                wall_low,
                wall_p_low if is_normal else None,
            )
            du[number, c] = diff
            dw[number, c] = before_diff
            slot = max(c - SPECIES + 1, 0)
            if first:
                lows[c] = low - before_low
            else:
                lows[c] += low - before_low
            if first and c in (0, *range(SPECIES, COMPS)):
                deltas[slot] = diff - before_diff
            else:
                deltas[slot] += diff - before_diff

    arrive("y")
    for c in range(COMPS):
        hy[c] = own_inputs[c]
        for x in range(X):
            at = 2 * (c * X + x)
            hy[c, x, Y - 2 : Y, :] = yr[0, at : at + 2, :]
            hy[c, x, 0:2, :] = yr[1, at : at + 2, :]
    cyclic_fluxes(1, [hy[c] for c in range(COMPS)], 1, True)

    arrive("z")
    merged = [
        jnp.where((lane_index & 3) < 2, zr[0, v][None], zr[1, v][None]) for v in range(packs)
    ]
    z_halo = []
    for c in range(COMPS):
        layers = []
        for x in range(X):
            at = ((c % per_pack) * X + x) * 4
            layers.append(roll(merged[c // per_pack], -(at + 2), 2))
        z_halo.append(jnp.concatenate(layers, axis=0))
    cyclic_fluxes(2, z_halo, 0, False)

    arrive("x")
    arrive("e")
    sides = []
    for side in (0, 1):
        halo = conserved_of([xh[side, c] for c in range(COMPS)])
        _, _, h_inv, h_vel, h_p = primitives(halo)
        sides.append((halo, h_vel, h_p, jnp.abs(h_vel[0]) + sound_of(h_inv, h_p)))

    def joined(below, own, above):
        return jnp.concatenate([below, own, above], axis=0)

    rate = joined(sides[0][3], jnp.abs(velocity[0]) + sound, sides[1][3])
    p_ext = joined(sides[0][2], pressure, sides[1][2])
    half_rate = 0.5 * jnp.maximum(rate[1 : X + 2], rate[2 : X + 3])
    wall_p = 0.5 * (p_ext[1 : X + 2] + p_ext[2 : X + 3])
    planes = []
    for x in range(-1, X):
        if (x + 1) % P_SIZE:
            planes.append(jnp.zeros((1, Y, Z), jnp.float32))
        elif x == X - 1:
            planes.append(edge(1, 0, 2)[0:1])
        else:
            e = (x + 1) // P_SIZE
            planes.append(walls[0][e : e + 1])
    wall = jnp.concatenate(planes, axis=0) > 0.5
    for c in range(COMPS):
        f = joined(
            flux_term(sides[0][0], sides[0][1], sides[0][2], c, 0),
            flux_term(cons, velocity, pressure, c, 0),
            flux_term(sides[1][0], sides[1][1], sides[1][2], c, 0),
        )
        u = joined(sides[0][0][c], cons[c], sides[1][0][c])
        low, diff = face_pair(
            f[0 : X + 1],
            f[1 : X + 2],
            f[2 : X + 3],
            f[3 : X + 4],
            u[2 : X + 3] - u[1 : X + 2],
            half_rate,
            wall,
            wall_p if c == SPECIES else None,
        )
        dx[c] = diff
        lows[c] += low[1:] - low[:-1]
        deltas[max(c - SPECIES + 1, 0)] += diff[1:] - diff[:-1]

    def bound(own, which):
        best = own
        for d in (1, 2):
            n = extent[d]
            up = jnp.where(index[d] < P_SIZE, edge(1, d, which), own)
            down = jnp.where(index[d] >= n - P_SIZE, edge(0, d, which), own)
            best = jnp.minimum(best, jnp.minimum(roll(up, -P_SIZE, d), roll(down, P_SIZE, d)))
        chain = joined(edge(0, 0, which)[EX - 1 : EX], own, edge(1, 0, which)[0:1])
        return jnp.minimum(best, jnp.minimum(chain[:EX], chain[2:]))

    rho_bound = bound(rho_min, 0)
    p_bound = bound(p_min, 1)

    fluxes = [sum([lows[c] for c in range(1, SPECIES)], lows[0])]
    fluxes += [lows[c] for c in range(SPECIES, COMPS)]
    jumps = [deltas[i] for i in range(COMPS - SPECIES + 1)]

    speed_max = spread_end(0, lambda rows: jnp.max(rows, axis=0, keepdims=True))
    ratio = (COURANT / speed_max).reshape(1, 1, ROW)

    def five(values):
        return [sum([values[c] for c in range(1, SPECIES)], values[0])] + [
            values[c] for c in range(SPECIES, COMPS)
        ]

    low_five = [u - ratio * f for u, f in zip(five(cons), fluxes)]
    d_five = [-(ratio * d) for d in jumps]
    d_rho = d_five[0]
    rho_scale = 1.0 / jnp.maximum(-d_rho, SLOPE_FLOOR)
    count = X * Y * Z * sizes[0] * sizes[1] * sizes[2]
    stat_lane = lax.broadcasted_iota(jnp.int32, (1, ROW), 1)

    def combine_stats(rows):
        return jnp.where(
            stat_lane < 2,
            jnp.min(rows, axis=0, keepdims=True),
            jnp.sum(rows, axis=0, keepdims=True),
        )

    def broadcast_stats(got):
        lowest_rho = got[0:1, 0:1].reshape(1, 1, 1)
        lowest_p = got[0:1, 1:2].reshape(1, 1, 1)
        spread = got[0:1, 2:3].reshape(1, 1, 1) * (1.0 / count) + SPREAD
        return lowest_rho, lowest_p, spread

    def next_blend(got, packed):
        t_density, rho_scale, t_p, p_scale, rho_bound, p_bound, mean_square, base = packed
        lowest_rho, lowest_p, spread = got
        rho_target = rho_bound - RELAX * jnp.maximum(rho_bound - lowest_rho, 0.0)
        p_target = p_bound - RELAX * jnp.maximum(p_bound - lowest_p, 0.0)
        step_rho = jnp.minimum(t_density - nodes(rho_target), 0.0) * rho_scale
        step_p = jnp.minimum(t_p - nodes(p_target), 0.0) * p_scale
        lowered = element(jnp.minimum(step_rho, step_p), jnp.minimum)
        cap = spread / (spread + mean_square)
        return jnp.maximum(jnp.minimum(cap, base + lowered), 0.0)

    per_edge = Z // (2 * P_SIZE)
    depth = 10 * X + 2 * EX
    sides_x = len(first_sides)

    def share(fields):
        at = 0
        for value in fields:
            pk[at : at + value.shape[0]] = value
            at += value.shape[0]
        for side, k in first_sides:
            remote(pk, nb.at[pl.ds(side * depth, depth)], 0, 4, step(0, k)).start()
        for side, k in ((0, 1), (1, -1)):
            rows = pl.ds(Y - P_SIZE, P_SIZE) if side == 0 else pl.ds(0, P_SIZE)
            there = nb.at[pl.ds(sides_x * depth, depth), rows]
            remote(pk.at[:, rows], there, 0, 4, step(1, k)).start()
        items = [value[x : x + 1] for value in fields for x in range(value.shape[0])]
        for v in range(pz.shape[0]):
            packed = jnp.zeros((1, Y, Z), jnp.float32)
            for j, item in enumerate(items[v * per_edge : (v + 1) * per_edge]):
                at = 2 * P_SIZE * j
                moved = roll(item, at + P_SIZE, 2)
                inside = (lane_index >= at) & (lane_index < at + 2 * P_SIZE)
                packed = jnp.where(inside, moved, packed)
            pz[v] = packed[0]
        for side, k in ((0, 1), (1, -1)):
            there = nb.at[pl.ds((sides_x + 1) * depth + side * pz.shape[0], pz.shape[0])]
            remote(pz, there, 0, 4, step(2, k)).start()

    def share_blend():
        bs[...] = blend
        for side, k in first_sides:
            there = bc.at[pl.ds(side * EX, EX)]
            remote(bs, there, 3, 5, step(0, k)).start()
        for side, k in ((0, 1), (1, -1)):
            there = bc.at[pl.ds((sides_x + 1 + side) * EX, EX)]
            remote(bs, there, 3, 5, step(2, k)).start()
            rows = pl.ds(Y - P_SIZE, P_SIZE) if side == 0 else pl.ds(0, P_SIZE)
            there = bc.at[pl.ds(sides_x * EX, EX), rows]
            remote(bs.at[:, rows], there, 3, 5, step(1, k)).start()

    def trial_of(low, d, low_sigma, blend):
        weight = None if blend is None else nodes(blend)
        trial = [a + (b if weight is None else weight * b) for a, b in zip(low, d)]
        safe, speeds, p = state_of(trial[0], trial[1:4], trial[4])
        residual = entropy(trial[0], safe, p) - low_sigma
        return trial[0], speeds, p, residual * residual

    def scales_of(d, speeds, square):
        cross = speeds[0] * d[1] + speeds[1] * d[2] + speeds[2] * d[3]
        speed2 = speeds[0] * speeds[0] + speeds[1] * speeds[1] + speeds[2] * speeds[2]
        slope = (GAMMA - 1.0) * (d[4] - cross + 0.5 * speed2 * d[0])
        mean_square = element(square, jnp.add) * (1.0 / (P_SIZE**3))
        return 1.0 / jnp.maximum(-slope, SLOPE_FLOOR), mean_square

    def sigma_of(low):
        safe, _, p = state_of(low[0], low[1:4], low[4])
        return entropy(low[0], safe, p)

    def neighbour_low(layer):
        low = [layer(i * X, (i + 1) * X) for i in range(5)]
        d = [layer(i * X, (i + 1) * X) for i in range(5, 10)]
        bounds = [layer(10 * X + i * EX, 10 * X + (i + 1) * EX) for i in range(2)]
        scale = 1.0 / jnp.maximum(-d[0], SLOPE_FLOOR)
        return low, d, sigma_of(low), scale, bounds

    def neighbour_fields(known, blend):
        low, d, sigma, scale, bounds = known
        density, speeds, p, square = trial_of(low, d, sigma, blend)
        p_scale, mean_square = scales_of(d, speeds, square)
        return density, scale, p, p_scale, bounds[0], bounds[1], mean_square, blend

    low_sigma = sigma_of(low_five)
    blend = None
    for newton in range(ITERS):
        t_density, t_vel, t_p, square = trial_of(low_five, d_five, low_sigma, blend)
        stats = jnp.where(
            stat_lane == 0,
            total(t_density, jnp.minimum),
            jnp.where(stat_lane == 1, total(t_p, jnp.minimum), total(square, jnp.add)),
        )
        spread_start(newton + 1, 0, stats)
        if newton == ITERS - 2:
            for key in ("x", "y", "z", "e"):
                sent_all(key)
            share((*low_five, *d_five, rho_bound, p_bound))
        p_scale, mean_square = scales_of(d_five, t_vel, square)
        base = jnp.ones((EX, Y, Z), jnp.float32) if blend is None else blend
        beside = {}
        if newton == ITERS - 1:
            arrive("b")
            at = sides_x * depth
            known = {1: neighbour_low(lambda a, b: nb[at + a : at + b])}
            ends = [
                nb[at + depth + i * pz.shape[0] : at + depth + (i + 1) * pz.shape[0]] for i in (0, 1)
            ]
            near = (lane_index & (2 * P_SIZE - 1)) < P_SIZE
            edges = [
                jnp.where(near, ends[0][v][None], ends[1][v][None]) for v in range(pz.shape[0])
            ]
            items = [
                roll(edges[j // per_edge], -(2 * P_SIZE * (j % per_edge) + P_SIZE), 2)
                for j in range(depth)
            ]
            known[2] = neighbour_low(lambda a, b: jnp.concatenate(items[a:b], axis=0))
            for side in range(sides_x):
                start = side * depth
                known[0, side] = neighbour_low(lambda a, b: nb[start + a : start + b])
            sent_all("b")
            sent_all("c")
            arrive("c")
            at = sides_x * EX
            weights = {(0, side): bc[side * EX : (side + 1) * EX] for side in range(sides_x)}
            weights[1] = bc[at : at + EX]
            weights[2] = jnp.where(
                lane_index < P_SIZE, bc[at + 2 * EX : at + 3 * EX], bc[at + EX : at + 2 * EX]
            )
            beside = {key: neighbour_fields(known[key], weights[key]) for key in known}
        got = broadcast_stats(spread_end(newton + 1, combine_stats))
        blend = next_blend(
            got, (t_density, rho_scale, t_p, p_scale, rho_bound, p_bound, mean_square, base)
        )
        if newton == ITERS - 2:
            share_blend()

    beside = {key: next_blend(got, packed) for key, packed in beside.items()}
    beside.setdefault((0, 1), beside[0, 0])

    theta = []
    for d in (2, 1):
        above = roll(jnp.where(index[d] == 0, beside[d], blend), -1, d)
        below = roll(jnp.where(index[d] == extent[d] - 1, beside[d], blend), 1, d)
        theta.append((nodes(jnp.minimum(blend, above)), nodes(jnp.minimum(blend, below))))
    x_blend = joined(beside[0, 0][EX - 1 : EX], nodes(blend), beside[0, 1][0:1])
    x_theta = jnp.minimum(x_blend[:-1], x_blend[1:])
    for c in range(COMPS):
        faces = x_theta * dx[c]
        change = lows[c] + (faces[1:] - faces[:-1])
        for number in range(2):
            upper, lower = theta[number]
            change += upper * du[number, c] - lower * dw[number, c]
        out[c] = cons[c] - ratio * change

    chosen = (lax.broadcasted_iota(jnp.int32, (Y, Z), 1) * P_SIZE) & (Z - 1)
    for e in range(EX):
        few = jnp.take_along_axis(blend[e], chosen, axis=1, mode="promise_in_bounds")[:, :EZ]
        bl[e] = jnp.concatenate([few[j * P_SIZE : j * P_SIZE + 1] for j in range(EY)], axis=0)

    spread_sent(ITERS, len(groups) - 1)


def store(state, weights, state_hbm, weights_hbm, sem):
    small = pltpu.make_async_copy(weights, weights_hbm, sem.at[1])
    small.start()
    for c in range(0, COMPS, 3):
        pltpu.make_async_copy(state.at[c : c + 3], state_hbm.at[c : c + 3], sem.at[0]).start()
    pltpu.make_async_copy(state, state_hbm, sem.at[0]).wait()
    small.wait()


def solution(mesh):
    sizes = tuple(mesh.shape[name] for name in AXES)

    def local(species, velocity_in, pressure_in, wall_types):
        X, Y, Z = pressure_in.shape
        EX, EY, EZ = wall_types.shape[1:]
        packs = -(-COMPS // (Z // (4 * X)))
        depth = 10 * X + 2 * EX
        edge_packs = -(-depth // (Z // (2 * P_SIZE)))
        vmem = lambda *shape: pltpu.VMEM(shape, jnp.float32)
        groups = reduce_groups(sizes)
        dma = pltpu.SemaphoreType.DMA
        sides = 1 if sizes[0] == 2 else 2
        rows_scratch = []
        for _ in range(ITERS + 1):
            for group in groups:
                rows_scratch += [vmem(1, ROW), vmem(len(group_offsets(sizes, group)), ROW)]
        state, weights = (
            pl.pallas_call(
                functools.partial(kernel, sizes),
                out_shape=[
                    pltpu.VMEM((COMPS, X, Y, Z), jnp.float32),
                    pltpu.VMEM((EX, EY, EZ), jnp.float32),
                ],
                in_specs=[pl.BlockSpec(memory_space=pltpu.HBM)] * 4,
                out_specs=[pl.BlockSpec(memory_space=pltpu.VMEM)] * 2,
                scratch_shapes=[
                    vmem(COMPS, X, Y, Z),
                    pltpu.VMEM((3, EX, EY, EZ), jnp.int32),
                    dma((2,)),
                    vmem(2, COMPS, 2, Y, Z),
                    vmem(2, COMPS * 2 * X + EX * Y, Z),
                    vmem(2, COMPS * 2 * X + EX * Y, Z),
                    vmem(COMPS, X, Y, Z),
                    vmem(packs + EX, Y, Z),
                    vmem(2, packs + EX, Y, Z),
                    vmem(EX, Y, Z),
                    vmem(sides, EX, Y, Z),
                    vmem(depth, Y, Z),
                    vmem((sides + 1) * depth + 2 * edge_packs, Y, Z),
                    vmem(edge_packs, Y, Z),
                    vmem(EX, Y, Z),
                    vmem((sides + 3) * EX, Y, Z),
                    vmem(COMPS, X + 1, Y, Z),
                    vmem(2, COMPS, X, Y, Z),
                    vmem(2, COMPS, X, Y, Z),
                    vmem(COMPS, X, Y, Z),
                    vmem(COMPS - SPECIES + 1, X, Y, Z),
                    dma((4,)),
                    dma((6,)),
                    pltpu.SemaphoreType.REGULAR((len(halo_links(sizes)),)),
                    pltpu.SemaphoreType.REGULAR,
                    vmem(1, ROW),
                    dma(()),
                    dma(()),
                    dma((2 * len(groups),)),
                ]
                + rows_scratch,
                compiler_params=pltpu.CompilerParams(collective_id=0, has_side_effects=True),
            )(species, velocity_in, pressure_in, wall_types)
        )
        return tuple(
            pl.pallas_call(
                store,
                out_shape=[
                    jax.ShapeDtypeStruct((COMPS, X, Y, Z), jnp.float32),
                    jax.ShapeDtypeStruct((EX, EY, EZ), jnp.float32),
                ],
                in_specs=[pl.BlockSpec(memory_space=pltpu.VMEM)] * 2,
                out_specs=[pl.BlockSpec(memory_space=pltpu.HBM)] * 2,
                scratch_shapes=[pltpu.SemaphoreType.DMA((2,))],
            )(*[pltpu.with_memory_space_constraint(v, pltpu.VMEM) for v in (state, weights)])
        )

    in_specs = (
        P(None, "gx", "gy", "gz"),
        P(None, "gx", "gy", "gz"),
        P("gx", "gy", "gz"),
        P(None, "gx", "gy", "gz"),
    )
    out_specs = (P(None, "gx", "gy", "gz"), P("gx", "gy", "gz"))
    return jax.shard_map(local, mesh=mesh, in_specs=in_specs, out_specs=out_specs, check_vma=False)
```

```python
import functools
import itertools

import jax
import jax.numpy as jnp
from jax import lax
from jax.experimental import pallas as pl
from jax.experimental.pallas import tpu as pltpu
from jax.sharding import PartitionSpec as P

SPECIES = 5
P_SIZE = 4
ITERS = 2
GAMMA = 1.4
COURANT = 0.4
FLOOR = 0.1
SLOPE_FLOOR = 0.01
SPREAD = 0.002
RELAX = 0.1

COMPS = SPECIES + 4
AXES = ("gx", "gy", "gz")
ROW = 128
DIRECT = 64
MESH = pl.DeviceIdType.MESH


def reduce_groups(sizes):
    if sizes[0] * sizes[1] * sizes[2] <= DIRECT:
        return [(0, 1, 2)]
    return [(2,), (1,), (0,)]


def group_offsets(sizes, group):
    spans = [range(sizes[d]) if d in group else (0,) for d in range(3)]
    far = lambda off: sum(min(off[d], sizes[d] - off[d]) for d in range(3))
    return sorted(itertools.product(*spans), key=far)


def halo_links(sizes):
    return [(d, k) for d in range(3) for k in ((1,) if sizes[d] == 2 else (1, -1))]


def conserved_of(inputs):
    species, velocity, pressure = inputs[:SPECIES], inputs[SPECIES : SPECIES + 3], inputs[-1]
    density = sum(species[1:], species[0])
    square = velocity[0] * velocity[0] + velocity[1] * velocity[1] + velocity[2] * velocity[2]
    energy = pressure * (1.0 / (GAMMA - 1.0)) + 0.5 * density * square
    return list(species) + [density * v for v in velocity] + [energy]


def primitives(cons):
    density = sum(cons[1:SPECIES], cons[0])
    safe = jnp.maximum(density, FLOOR)
    inverse = 1.0 / safe
    momentum = cons[SPECIES : SPECIES + 3]
    velocity = [m * inverse for m in momentum]
    kinetic = momentum[0] * velocity[0] + momentum[1] * velocity[1] + momentum[2] * velocity[2]
    pressure = (GAMMA - 1.0) * (cons[SPECIES + 3] - 0.5 * kinetic)
    return density, safe, inverse, velocity, pressure


def state_of(density, momentum, energy):
    safe = jnp.maximum(density, FLOOR)
    inverse = 1.0 / safe
    velocity = [m * inverse for m in momentum]
    kinetic = momentum[0] * velocity[0] + momentum[1] * velocity[1] + momentum[2] * velocity[2]
    pressure = (GAMMA - 1.0) * (energy - 0.5 * kinetic)
    return safe, velocity, pressure


def sound_of(inverse, pressure):
    return jnp.sqrt(GAMMA * jnp.maximum(pressure, FLOOR) * inverse)


def entropy(density, safe, pressure):
    return density * (jnp.log(jnp.maximum(pressure, FLOOR)) - GAMMA * jnp.log(safe))


def flux_term(cons, velocity, pressure, comp, d):
    term = cons[comp] * velocity[d]
    if comp == SPECIES + d:
        term = term + pressure
    if comp == SPECIES + 3:
        term = term + pressure * velocity[d]
    return term


def face_pair(mm, left, right, pp, jump, rate, wall, wall_value):
    both = left + right
    high = (7.0 * both - (mm + pp)) * (1.0 / 12.0)
    low = 0.5 * both - rate * jump
    keep = 0.0 if wall_value is None else wall_value
    diff = jnp.where(wall, 0.0, high - low)
    return jnp.where(wall, keep, low), diff


def kernel(
    sizes, sp_hbm, ve_hbm, pr_hbm, wa_hbm, out, bl, inp, wa, load_sem,
    xh, ys, yr, hy, zs, zr, es, er, pk, nb, pz, bs, bc, dx, du, dw, lows, deltas,
    sent_sem, came_sem, near_sem, all_sem, row_sent, row_came, *rows_scratch
):
    X, Y, Z = inp.shape[1:]
    EX, EY, EZ = wa.shape[1:]
    loads = [
        pltpu.make_async_copy(sp_hbm, inp.at[:SPECIES], load_sem.at[0]),
        pltpu.make_async_copy(ve_hbm, inp.at[SPECIES : SPECIES + 3], load_sem.at[0]),
        pltpu.make_async_copy(pr_hbm, inp.at[SPECIES + 3], load_sem.at[0]),
        pltpu.make_async_copy(wa_hbm, wa, load_sem.at[1]),
    ]
    for copy in loads:
        copy.start()
    me = [lax.axis_index(name) for name in AXES]
    groups = reduce_groups(sizes)

    place = [[me[d]] + [lax.rem(me[d] + k, sizes[d]) for k in range(1, sizes[d])] for d in range(3)]

    def device(off):
        return tuple(place[d][off[d]] for d in range(3))

    def step(d, k):
        return tuple(k % sizes[d] if a == d else 0 for a in range(3))

    relayed = False
    relay = relay_sem = None
    if relayed:
        rows_scratch[1][...] = jnp.zeros_like(rows_scratch[1])

    def traced(flag):
        return jnp.where(flag, 1, 0).astype(jnp.int32)

    links = halo_links(sizes)
    near = {link: near_sem.at[i] for i, link in enumerate(links)}

    def later(d, k):
        return me[d] != sizes[d] - 1 if k == 1 else me[d] == 0

    def neighbour(d, k):
        return device(step(d, k))

    corner = tuple(n - 1 for n in sizes)
    is_corner = (me[0] == corner[0]) & (me[1] == corner[1]) & (me[2] == corner[2])
    devices = sizes[0] * sizes[1] * sizes[2]
    barrier = pltpu.get_barrier_semaphore()

    @pl.when(jnp.logical_not(is_corner))
    def _():
        pl.semaphore_signal(barrier, inc=1, device_id=corner, device_id_type=MESH)

    expected = jnp.where(is_corner, devices - 1, 0).astype(jnp.int32)
    for d, k in links:

        @pl.when(later(d, k))
        def _(d=d, k=k):
            pl.semaphore_signal(barrier, inc=1, device_id=neighbour(d, k), device_id_type=MESH)

        expected = expected + 1 - traced(later(d, k))

    @pl.when(expected > 0)
    def _():
        pl.semaphore_wait(barrier, expected)

    for d, k in links:
        back = (d, k if sizes[d] == 2 else -k)

        @pl.when(jnp.logical_not(later(d, k)))
        def _(d=d, k=k, back=back):
            pl.semaphore_signal(
                near[back], inc=1, device_id=neighbour(d, k), device_id_type=MESH
            )

    @pl.when(is_corner)
    def _():
        def tell(i, carry):
            z = lax.rem(i, sizes[2])
            y = lax.rem(lax.div(i, sizes[2]), sizes[1])
            x = lax.div(i, sizes[2] * sizes[1])
            pl.semaphore_signal(all_sem, inc=1, device_id=(x, y, z), device_id_type=MESH)
            return carry

        if devices <= DIRECT:
            for at in itertools.product(*[range(n) for n in sizes]):
                if at != corner:
                    pl.semaphore_signal(all_sem, inc=1, device_id=at, device_id_type=MESH)
        else:
            lax.fori_loop(0, devices - 1, tell, 0)

    def await_near(d, k):
        @pl.when(later(d, k))
        def _():
            pl.semaphore_wait(near[d, k], 1)

    def await_all():
        @pl.when(jnp.logical_not(is_corner))
        def _():
            pl.semaphore_wait(all_sem, 1)

    pltpu.make_async_copy(inp, inp, load_sem.at[0]).wait()
    loads[3].wait()

    origin = (me[0] == 0) & (me[1] <= 1)
    next_up = origin & (me[2] == 1)
    origin = origin & (me[2] == 0)
    plane_rows = ((origin, devices - 2), (jnp.logical_not(origin), devices - 3))
    if relayed:
        relay_copy = pltpu.make_async_remote_copy(
            src_ref=rows_scratch[0],
            dst_ref=relay,
            send_sem=row_sent,
            recv_sem=relay_sem,
            device_id=neighbour(2, 1),
            device_id_type=MESH,
        )

    def speed_out():
        await_all()
        if not relayed:
            spread_start(0, 0, speed_row)
            return

        @pl.when(next_up)
        def _():
            relay_copy.wait_recv()
            spread_start(0, 0, jnp.maximum(speed_row, relay[...]))

        @pl.when(jnp.logical_not(origin | next_up))
        def _():
            spread_start(0, 0, speed_row)

    def row_parts(turn, stage):
        base = 2 * (turn * len(groups) + stage)
        mine, buf = rows_scratch[base : base + 2]
        return mine, buf, row_came.at[turn % 2 * len(groups) + stage]

    def spread_copy(turn, stage, i):
        mine, buf, came = row_parts(turn, stage)
        group = groups[stage]
        off = group_offsets(sizes, group)[i]
        there = tuple(
            lax.rem(sizes[d] - 1 - me[d] + off[d], sizes[d]) if d in group else me[d]
            for d in range(3)
        )
        can_be_me = all((off[d] + 1 - sizes[d]) % 2 == 0 or sizes[d] % 2 for d in group)
        copy = pltpu.make_async_remote_copy(
            src_ref=mine,
            dst_ref=buf.at[pl.ds(i, 1)],
            send_sem=row_sent,
            recv_sem=came,
            device_id=there,
            device_id_type=MESH,
        )
        return copy, can_be_me, functools.reduce(lambda a, b: a & b, [t == m for t, m in zip(there, me)])

    def spread_start(turn, stage, row):
        if turn or stage:
            before = turn * len(groups) + stage - 1
            spread_sent(before // len(groups), before % len(groups))
        mine, buf, _ = row_parts(turn, stage)
        mine[...] = row
        for i in range(buf.shape[0]):
            copy, can_be_me, is_me = spread_copy(turn, stage, i)
            if not can_be_me:
                copy.start()
                continue

            @pl.when(jnp.logical_not(is_me))
            def _(copy=copy):
                copy.start()

            @pl.when(is_me)
            def _(i=i):
                buf[i : i + 1] = row

    def spread_whole(turn, stage, rows=None):
        _, buf, came = row_parts(turn, stage)
        rows = buf.at[pl.ds(0, rows or buf.shape[0] - 1)]
        return pltpu.make_async_remote_copy(
            src_ref=rows,
            dst_ref=rows,
            send_sem=row_sent,
            recv_sem=came,
            device_id=device((1, 1, 1)),
            device_id_type=MESH,
        )

    def spread_end(turn, combine):
        for stage in range(len(groups)):
            if stage > 0:
                spread_start(turn, stage, row)
            if turn == 0 and relayed:
                for flag, rows in plane_rows:

                    @pl.when(flag)
                    def _(rows=rows):
                        spread_whole(turn, stage, rows).wait_recv()
            else:
                spread_whole(turn, stage).wait_recv()
            row = combine(row_parts(turn, stage)[1][...])
        return row

    def spread_sent(turn, stage):
        if turn == 0 and relayed:

            @pl.when(jnp.logical_not(origin))
            def _():
                spread_whole(turn, stage).wait_send()

            @pl.when(origin)
            def _():
                relay_copy.wait_send()

        else:
            spread_whole(turn, stage).wait_send()

    row_index = lax.broadcasted_iota(jnp.int32, (1, Y, Z), 1)
    lane_index = lax.broadcasted_iota(jnp.int32, (1, Y, Z), 2)
    index = {1: row_index, 2: lane_index}
    extent = {1: Y, 2: Z}

    def roll(value, shift, axis):
        return pltpu.roll(value, shift % value.shape[axis], axis)

    def mesh_group(value, axis, op):
        for s in (1, 2):
            low = (index[axis] & s) == 0
            value = op(value, jnp.where(low, roll(value, -s, axis), roll(value, s, axis)))
        return value

    def lane_group(value, op):
        place = lane_index & (P_SIZE - 1)
        for s in range(1, P_SIZE):
            ahead = roll(value, -s, 2)
            behind = roll(value, P_SIZE - s, 2)
            turned = jnp.where(place < P_SIZE - s, ahead, behind)
            whole = turned if s == 1 else op(whole, turned)
        return op(value, whole)

    def element(value, op):
        parts = value.reshape(EX, P_SIZE, Y, Z)
        value = op(op(parts[:, 0], parts[:, 1]), op(parts[:, 2], parts[:, 3]))
        return lane_group(mesh_group(value, 1, op), op)

    def nodes(value):
        return jnp.broadcast_to(value[:, None], (EX, P_SIZE, Y, Z)).reshape(X, Y, Z)

    def total(value, op):
        value = functools.reduce(op, [value[x] for x in range(X)])
        value = {jnp.minimum: jnp.min, jnp.maximum: jnp.max, jnp.add: jnp.sum}[op](
            value, axis=0, keepdims=True
        )
        return {jnp.minimum: jnp.min, jnp.maximum: jnp.max, jnp.add: jnp.sum}[op](
            value, axis=1, keepdims=True
        )

    late = me[2] == corner[2]
    last_x = me[0] == corner[0]
    last_chip = last_x & (me[1] >= corner[1] - 1) & late
    first_sides = ((0, 1),) if sizes[0] == 2 else ((0, 1), (1, -1))
    packs = zs.shape[0] - EX
    body = COMPS * 2 * X

    def remote(src, dst, sent, came, off):
        return pltpu.make_async_remote_copy(
            src_ref=src,
            dst_ref=dst,
            send_sem=sent_sem.at[sent],
            recv_sem=came_sem.at[came],
            device_id=device(off),
            device_id_type=MESH,
        )

    landing = {
        "x": (xh, 0, 0),
        "y": (yr, 1, 1),
        "z": (zr, 2, 2),
        "e": (er, 3, 3),
        "b": (nb, 0, 4),
        "c": (bc, 3, 5),
    }

    def whole(key):
        ref, sent, came = landing[key]
        return remote(ref, ref, sent, came, step(2, 1))

    def arrive(key):
        whole(key).wait_recv()

    def sent_all(key):
        whole(key).wait_send()

    def send_x():
        for d, k in links:
            if d == 0:
                await_near(d, k)
        for side, k in ((0, 1), (1, -1)):
            at = X - 2 if side == 0 else 0
            remote(inp.at[:, at : at + 2], xh.at[side], 0, 0, step(0, k)).start()

    def send_e():
        for side, k in first_sides:
            remote(es, er.at[side], 3, 3, step(0, k)).start()

    def send_y():
        for side, k in ((0, 1), (1, -1)):
            if (1, k) in links:
                await_near(1, k)
            remote(ys.at[side], yr.at[side], 1, 1, step(1, k)).start()

    def send_z():
        for side, k in ((0, 1), (1, -1)):
            if (2, k) in links:
                await_near(2, k)
            remote(zs, zr.at[side], 2, 2, step(2, k)).start()
            if side == 0 and relayed:

                @pl.when(origin)
                def _():
                    rows_scratch[0][...] = speed_row
                    relay_copy.start()

    @pl.when(last_x & jnp.logical_not(last_chip))
    def _():
        send_x()

    own_inputs = [inp[c] for c in range(COMPS)]

    cons = conserved_of(own_inputs)
    density, _, inverse, velocity, pressure = primitives(cons)
    sound = sound_of(inverse, pressure)
    speed = jnp.abs(velocity[0]) + jnp.abs(velocity[1]) + jnp.abs(velocity[2]) + 3.0 * sound
    speed_row = jnp.broadcast_to(total(speed, jnp.maximum), (1, ROW))

    @pl.when(last_chip)
    def _():
        speed_out()
        send_x()

    for c in range(COMPS):
        for x in range(X):
            at = 2 * (c * X + x)
            ys[0, at : at + 2, :] = own_inputs[c][x, Y - 2 : Y, :]
            ys[1, at : at + 2, :] = own_inputs[c][x, 0:2, :]
    per_pack = Z // (4 * X)
    for v in range(packs):
        packed = jnp.zeros((1, Y, Z), jnp.float32)
        for c in range(v * per_pack, min((v + 1) * per_pack, COMPS)):
            for x in range(X):
                at = ((c - v * per_pack) * X + x) * 4
                moved = roll(own_inputs[c][x : x + 1], at + 2, 2)
                packed = jnp.where((lane_index >= at) & (lane_index < at + 4), moved, packed)
        zs[v] = packed[0]

    rho_min = element(density, jnp.minimum)
    p_min = element(pressure, jnp.minimum)
    widen = (
        lax.broadcasted_iota(jnp.int32, (EZ, Z), 1) // P_SIZE
        == lax.broadcasted_iota(jnp.int32, (EZ, Z), 0)
    ).astype(jnp.float32)
    heighten = (
        lax.broadcasted_iota(jnp.int32, (Y, EY), 0) // P_SIZE
        == lax.broadcasted_iota(jnp.int32, (Y, EY), 1)
    ).astype(jnp.float32)
    walls = []
    for d in range(3):
        layers = []
        for e in range(EX):
            flags = wa[d, e].astype(jnp.float32)
            flags = jnp.dot(flags, widen, preferred_element_type=jnp.float32)
            layers.append(jnp.dot(heighten, flags, preferred_element_type=jnp.float32)[None])
        walls.append(jnp.concatenate(layers, axis=0))
        turn_row = row_index & (P_SIZE - 1)
        fields = jnp.where(turn_row == 0, rho_min, jnp.where(turn_row == 1, p_min, walls[d]))
        if d == 0:
            es[...] = fields
        elif d == 1:
            for side in (0, 1):
                ys[side, body : body + EX * Y, :] = fields.reshape(EX * Y, Z)
        else:
            zs[packs : packs + EX] = fields

    def spread_rows(value, which):
        value = jnp.where((row_index & (P_SIZE - 1)) == which, value, jnp.inf)
        return mesh_group(value, 1, jnp.minimum)

    def edge(side, d, which):
        if d == 0:
            fields = er[0 if sizes[0] == 2 else side]
        elif d == 1:
            fields = yr[side, body : body + EX * Y, :].reshape(EX, Y, Z)
        else:
            fields = zr[side, packs : packs + EX]
        return spread_rows(fields, which)

    @pl.when(jnp.logical_not(late | last_x))
    def _():
        send_x()

    @pl.when(jnp.logical_not(late))
    def _():
        send_e()
        send_y()

    send_z()

    @pl.when(late & jnp.logical_not(last_x))
    def _():
        send_x()

    @pl.when(late)
    def _():
        send_e()
        send_y()

    @pl.when(jnp.logical_not(last_chip))
    def _():
        speed_out()

    def cyclic_fluxes(d, halo_inputs, number, first):
        n = extent[d]
        ix = index[d]
        halo = conserved_of(halo_inputs)
        _, _, h_inv, h_vel, h_p = primitives(halo)
        h_rate = jnp.abs(h_vel[d]) + sound_of(h_inv, h_p)
        rate = jnp.abs(velocity[d]) + sound

        def beside(value, beyond, k):
            edge_of = ix < k if k > 0 else ix >= n + k
            return roll(jnp.where(edge_of, beyond, value), -k, d)

        shifts = (-2, -1, 1, 2)
        along = {k: {d: beside(velocity[d], h_vel[d], k)} for k in shifts}
        p_at = {k: beside(pressure, h_p, k) for k in shifts}
        flag = roll(jnp.where(ix == 0, edge(1, d, 2), walls[d]), -1, d)
        ends = ix & (P_SIZE - 1)
        wall = nodes(jnp.where(ends == P_SIZE - 1, flag, 0.0)) > 0.5
        wall_low = nodes(jnp.where(ends == 0, walls[d], 0.0)) > 0.5
        half_rate = 0.5 * jnp.maximum(rate, beside(rate, h_rate, 1))
        half_low = 0.5 * jnp.maximum(beside(rate, h_rate, -1), rate)
        wall_p = 0.5 * (pressure + p_at[1])
        wall_p_low = 0.5 * (p_at[-1] + pressure)
        for c in range(COMPS):
            u_at = {k: beside(cons[c], halo[c], k) for k in shifts}
            f_at = {k: flux_term({c: u_at[k]}, along[k], p_at[k], c, d) for k in shifts}
            f = flux_term(cons, velocity, pressure, c, d)
            is_normal = c == SPECIES + d
            low, diff = face_pair(
                f_at[-1],
                f,
                f_at[1],
                f_at[2],
                u_at[1] - cons[c],
                half_rate,
                wall,
                wall_p if is_normal else None,
            )
            before_low, before_diff = face_pair(
                f_at[-2],
                f_at[-1],
                f,
                f_at[1],
                cons[c] - u_at[-1],
                half_low,
                wall_low,
                wall_p_low if is_normal else None,
            )
            du[number, c] = diff
            dw[number, c] = before_diff
            slot = max(c - SPECIES + 1, 0)
            if first:
                lows[c] = low - before_low
            else:
                lows[c] += low - before_low
            if first and c in (0, *range(SPECIES, COMPS)):
                deltas[slot] = diff - before_diff
            else:
                deltas[slot] += diff - before_diff

    arrive("y")
    for c in range(COMPS):
        hy[c] = own_inputs[c]
        for x in range(X):
            at = 2 * (c * X + x)
            hy[c, x, Y - 2 : Y, :] = yr[0, at : at + 2, :]
            hy[c, x, 0:2, :] = yr[1, at : at + 2, :]
    cyclic_fluxes(1, [hy[c] for c in range(COMPS)], 1, True)

    arrive("z")
    merged = [
        jnp.where((lane_index & 3) < 2, zr[0, v][None], zr[1, v][None]) for v in range(packs)
    ]
    z_halo = []
    for c in range(COMPS):
        layers = []
        for x in range(X):
            at = ((c % per_pack) * X + x) * 4
            layers.append(roll(merged[c // per_pack], -(at + 2), 2))
        z_halo.append(jnp.concatenate(layers, axis=0))
    cyclic_fluxes(2, z_halo, 0, False)

    arrive("x")
    arrive("e")
    sides = []
    for side in (0, 1):
        halo = conserved_of([xh[side, c] for c in range(COMPS)])
        _, _, h_inv, h_vel, h_p = primitives(halo)
        sides.append((halo, h_vel, h_p, jnp.abs(h_vel[0]) + sound_of(h_inv, h_p)))

    def joined(below, own, above):
        return jnp.concatenate([below, own, above], axis=0)

    rate = joined(sides[0][3], jnp.abs(velocity[0]) + sound, sides[1][3])
    p_ext = joined(sides[0][2], pressure, sides[1][2])
    half_rate = 0.5 * jnp.maximum(rate[1 : X + 2], rate[2 : X + 3])
    wall_p = 0.5 * (p_ext[1 : X + 2] + p_ext[2 : X + 3])
    planes = []
    for x in range(-1, X):
        if (x + 1) % P_SIZE:
            planes.append(jnp.zeros((1, Y, Z), jnp.float32))
        elif x == X - 1:
            planes.append(edge(1, 0, 2)[0:1])
        else:
            e = (x + 1) // P_SIZE
            planes.append(walls[0][e : e + 1])
    wall = jnp.concatenate(planes, axis=0) > 0.5
    for c in range(COMPS):
        f = joined(
            flux_term(sides[0][0], sides[0][1], sides[0][2], c, 0),
            flux_term(cons, velocity, pressure, c, 0),
            flux_term(sides[1][0], sides[1][1], sides[1][2], c, 0),
        )
        u = joined(sides[0][0][c], cons[c], sides[1][0][c])
        low, diff = face_pair(
            f[0 : X + 1],
            f[1 : X + 2],
            f[2 : X + 3],
            f[3 : X + 4],
            u[2 : X + 3] - u[1 : X + 2],
            half_rate,
            wall,
            wall_p if c == SPECIES else None,
        )
        dx[c] = diff
        lows[c] += low[1:] - low[:-1]
        deltas[max(c - SPECIES + 1, 0)] += diff[1:] - diff[:-1]

    def bound(own, which):
        best = own
        for d in (1, 2):
            n = extent[d]
            up = jnp.where(index[d] < P_SIZE, edge(1, d, which), own)
            down = jnp.where(index[d] >= n - P_SIZE, edge(0, d, which), own)
            best = jnp.minimum(best, jnp.minimum(roll(up, -P_SIZE, d), roll(down, P_SIZE, d)))
        chain = joined(edge(0, 0, which)[EX - 1 : EX], own, edge(1, 0, which)[0:1])
        return jnp.minimum(best, jnp.minimum(chain[:EX], chain[2:]))

    rho_bound = bound(rho_min, 0)
    p_bound = bound(p_min, 1)

    fluxes = [sum([lows[c] for c in range(1, SPECIES)], lows[0])]
    fluxes += [lows[c] for c in range(SPECIES, COMPS)]
    jumps = [deltas[i] for i in range(COMPS - SPECIES + 1)]

    speed_max = spread_end(0, lambda rows: jnp.max(rows, axis=0, keepdims=True))
    ratio = (COURANT / speed_max).reshape(1, 1, ROW)

    def five(values):
        return [sum([values[c] for c in range(1, SPECIES)], values[0])] + [
            values[c] for c in range(SPECIES, COMPS)
        ]

    low_five = [u - ratio * f for u, f in zip(five(cons), fluxes)]
    d_five = [-(ratio * d) for d in jumps]
    d_rho = d_five[0]
    rho_scale = 1.0 / jnp.maximum(-d_rho, SLOPE_FLOOR)
    count = X * Y * Z * sizes[0] * sizes[1] * sizes[2]
    stat_lane = lax.broadcasted_iota(jnp.int32, (1, ROW), 1)

    def combine_stats(rows):
        return jnp.where(
            stat_lane < 2,
            jnp.min(rows, axis=0, keepdims=True),
            jnp.sum(rows, axis=0, keepdims=True),
        )

    def broadcast_stats(got):
        lowest_rho = got[0:1, 0:1].reshape(1, 1, 1)
        lowest_p = got[0:1, 1:2].reshape(1, 1, 1)
        spread = got[0:1, 2:3].reshape(1, 1, 1) * (1.0 / count) + SPREAD
        return lowest_rho, lowest_p, spread

    def next_blend(got, packed):
        t_density, rho_scale, t_p, p_scale, rho_bound, p_bound, mean_square, base = packed
        lowest_rho, lowest_p, spread = got
        rho_target = rho_bound - RELAX * jnp.maximum(rho_bound - lowest_rho, 0.0)
        p_target = p_bound - RELAX * jnp.maximum(p_bound - lowest_p, 0.0)
        step_rho = jnp.minimum(t_density - nodes(rho_target), 0.0) * rho_scale
        step_p = jnp.minimum(t_p - nodes(p_target), 0.0) * p_scale
        lowered = element(jnp.minimum(step_rho, step_p), jnp.minimum)
        cap = spread / (spread + mean_square)
        return jnp.maximum(jnp.minimum(cap, base + lowered), 0.0)

    per_edge = Z // (2 * P_SIZE)
    depth = 10 * X + 2 * EX
    sides_x = len(first_sides)

    def share(fields):
        at = 0
        for value in fields:
            pk[at : at + value.shape[0]] = value
            at += value.shape[0]
        for side, k in first_sides:
            remote(pk, nb.at[pl.ds(side * depth, depth)], 0, 4, step(0, k)).start()
        for side, k in ((0, 1), (1, -1)):
            rows = pl.ds(Y - P_SIZE, P_SIZE) if side == 0 else pl.ds(0, P_SIZE)
            there = nb.at[pl.ds(sides_x * depth, depth), rows]
            remote(pk.at[:, rows], there, 0, 4, step(1, k)).start()
        items = [value[x : x + 1] for value in fields for x in range(value.shape[0])]
        for v in range(pz.shape[0]):
            packed = jnp.zeros((1, Y, Z), jnp.float32)
            for j, item in enumerate(items[v * per_edge : (v + 1) * per_edge]):
                at = 2 * P_SIZE * j
                moved = roll(item, at + P_SIZE, 2)
                inside = (lane_index >= at) & (lane_index < at + 2 * P_SIZE)
                packed = jnp.where(inside, moved, packed)
            pz[v] = packed[0]
        for side, k in ((0, 1), (1, -1)):
            there = nb.at[pl.ds((sides_x + 1) * depth + side * pz.shape[0], pz.shape[0])]
            remote(pz, there, 0, 4, step(2, k)).start()

    def share_blend():
        bs[...] = blend
        for side, k in first_sides:
            there = bc.at[pl.ds(side * EX, EX)]
            remote(bs, there, 3, 5, step(0, k)).start()
        for side, k in ((0, 1), (1, -1)):
            there = bc.at[pl.ds((sides_x + 1 + side) * EX, EX)]
            remote(bs, there, 3, 5, step(2, k)).start()
            rows = pl.ds(Y - P_SIZE, P_SIZE) if side == 0 else pl.ds(0, P_SIZE)
            there = bc.at[pl.ds(sides_x * EX, EX), rows]
            remote(bs.at[:, rows], there, 3, 5, step(1, k)).start()

    def trial_of(low, d, low_sigma, blend):
        weight = None if blend is None else nodes(blend)
        trial = [a + (b if weight is None else weight * b) for a, b in zip(low, d)]
        safe, speeds, p = state_of(trial[0], trial[1:4], trial[4])
        residual = entropy(trial[0], safe, p) - low_sigma
        return trial[0], speeds, p, residual * residual

    def scales_of(d, speeds, square):
        cross = speeds[0] * d[1] + speeds[1] * d[2] + speeds[2] * d[3]
        speed2 = speeds[0] * speeds[0] + speeds[1] * speeds[1] + speeds[2] * speeds[2]
        slope = (GAMMA - 1.0) * (d[4] - cross + 0.5 * speed2 * d[0])
        mean_square = element(square, jnp.add) * (1.0 / (P_SIZE**3))
        return 1.0 / jnp.maximum(-slope, SLOPE_FLOOR), mean_square

    def sigma_of(low):
        safe, _, p = state_of(low[0], low[1:4], low[4])
        return entropy(low[0], safe, p)

    def neighbour_low(layer):
        low = [layer(i * X, (i + 1) * X) for i in range(5)]
        d = [layer(i * X, (i + 1) * X) for i in range(5, 10)]
        bounds = [layer(10 * X + i * EX, 10 * X + (i + 1) * EX) for i in range(2)]
        scale = 1.0 / jnp.maximum(-d[0], SLOPE_FLOOR)
        return low, d, sigma_of(low), scale, bounds

    def neighbour_fields(known, blend):
        low, d, sigma, scale, bounds = known
        density, speeds, p, square = trial_of(low, d, sigma, blend)
        p_scale, mean_square = scales_of(d, speeds, square)
        return density, scale, p, p_scale, bounds[0], bounds[1], mean_square, blend

    low_sigma = sigma_of(low_five)
    blend = None
    for newton in range(ITERS):
        t_density, t_vel, t_p, square = trial_of(low_five, d_five, low_sigma, blend)
        stats = jnp.where(
            stat_lane == 0,
            total(t_density, jnp.minimum),
            jnp.where(stat_lane == 1, total(t_p, jnp.minimum), total(square, jnp.add)),
        )
        spread_start(newton + 1, 0, stats)
        if newton == ITERS - 2:
            for key in ("x", "y", "z", "e"):
                sent_all(key)
            share((*low_five, *d_five, rho_bound, p_bound))
        p_scale, mean_square = scales_of(d_five, t_vel, square)
        base = jnp.ones((EX, Y, Z), jnp.float32) if blend is None else blend
        beside = {}
        if newton == ITERS - 1:
            arrive("b")
            at = sides_x * depth
            known = {1: neighbour_low(lambda a, b: nb[at + a : at + b])}
            ends = [
                nb[at + depth + i * pz.shape[0] : at + depth + (i + 1) * pz.shape[0]] for i in (0, 1)
            ]
            near = (lane_index & (2 * P_SIZE - 1)) < P_SIZE
            edges = [
                jnp.where(near, ends[0][v][None], ends[1][v][None]) for v in range(pz.shape[0])
            ]
            items = [
                roll(edges[j // per_edge], -(2 * P_SIZE * (j % per_edge) + P_SIZE), 2)
                for j in range(depth)
            ]
            known[2] = neighbour_low(lambda a, b: jnp.concatenate(items[a:b], axis=0))
            for side in range(sides_x):
                start = side * depth
                known[0, side] = neighbour_low(lambda a, b: nb[start + a : start + b])
            sent_all("b")
            sent_all("c")
            arrive("c")
            at = sides_x * EX
            weights = {(0, side): bc[side * EX : (side + 1) * EX] for side in range(sides_x)}
            weights[1] = bc[at : at + EX]
            weights[2] = jnp.where(
                lane_index < P_SIZE, bc[at + 2 * EX : at + 3 * EX], bc[at + EX : at + 2 * EX]
            )
            beside = {key: neighbour_fields(known[key], weights[key]) for key in known}
        got = broadcast_stats(spread_end(newton + 1, combine_stats))
        blend = next_blend(
            got, (t_density, rho_scale, t_p, p_scale, rho_bound, p_bound, mean_square, base)
        )
        if newton == ITERS - 2:
            share_blend()

    beside = {key: next_blend(got, packed) for key, packed in beside.items()}
    beside.setdefault((0, 1), beside[0, 0])

    theta = []
    for d in (2, 1):
        above = roll(jnp.where(index[d] == 0, beside[d], blend), -1, d)
        below = roll(jnp.where(index[d] == extent[d] - 1, beside[d], blend), 1, d)
        theta.append((nodes(jnp.minimum(blend, above)), nodes(jnp.minimum(blend, below))))
    x_blend = joined(beside[0, 0][EX - 1 : EX], nodes(blend), beside[0, 1][0:1])
    x_theta = jnp.minimum(x_blend[:-1], x_blend[1:])
    for c in range(COMPS):
        faces = x_theta * dx[c]
        change = lows[c] + (faces[1:] - faces[:-1])
        for number in range(2):
            upper, lower = theta[number]
            change += upper * du[number, c] - lower * dw[number, c]
        out[c] = cons[c] - ratio * change

    chosen = (lax.broadcasted_iota(jnp.int32, (Y, Z), 1) * P_SIZE) & (Z - 1)
    for e in range(EX):
        few = jnp.take_along_axis(blend[e], chosen, axis=1, mode="promise_in_bounds")[:, :EZ]
        bl[e] = jnp.concatenate([few[j * P_SIZE : j * P_SIZE + 1] for j in range(EY)], axis=0)

    spread_sent(ITERS, len(groups) - 1)


def store(state, weights, state_hbm, weights_hbm, sem):
    small = pltpu.make_async_copy(weights, weights_hbm, sem.at[1])
    small.start()
    for c in range(0, COMPS, 3):
        pltpu.make_async_copy(state.at[c : c + 3], state_hbm.at[c : c + 3], sem.at[0]).start()
    pltpu.make_async_copy(state, state_hbm, sem.at[0]).wait()
    small.wait()


def solution(mesh):
    sizes = tuple(mesh.shape[name] for name in AXES)

    def local(species, velocity_in, pressure_in, wall_types):
        X, Y, Z = pressure_in.shape
        EX, EY, EZ = wall_types.shape[1:]
        packs = -(-COMPS // (Z // (4 * X)))
        depth = 10 * X + 2 * EX
        edge_packs = -(-depth // (Z // (2 * P_SIZE)))
        vmem = lambda *shape: pltpu.VMEM(shape, jnp.float32)
        groups = reduce_groups(sizes)
        dma = pltpu.SemaphoreType.DMA
        sides = 1 if sizes[0] == 2 else 2
        rows_scratch = []
        for _ in range(ITERS + 1):
            for group in groups:
                rows_scratch += [vmem(1, ROW), vmem(len(group_offsets(sizes, group)), ROW)]
        state, weights = (
            pl.pallas_call(
                functools.partial(kernel, sizes),
                out_shape=[
                    pltpu.VMEM((COMPS, X, Y, Z), jnp.float32),
                    pltpu.VMEM((EX, EY, EZ), jnp.float32),
                ],
                in_specs=[pl.BlockSpec(memory_space=pltpu.HBM)] * 4,
                out_specs=[pl.BlockSpec(memory_space=pltpu.VMEM)] * 2,
                scratch_shapes=[
                    vmem(COMPS, X, Y, Z),
                    pltpu.VMEM((3, EX, EY, EZ), jnp.int32),
                    dma((2,)),
                    vmem(2, COMPS, 2, Y, Z),
                    vmem(2, COMPS * 2 * X + EX * Y, Z),
                    vmem(2, COMPS * 2 * X + EX * Y, Z),
                    vmem(COMPS, X, Y, Z),
                    vmem(packs + EX, Y, Z),
                    vmem(2, packs + EX, Y, Z),
                    vmem(EX, Y, Z),
                    vmem(sides, EX, Y, Z),
                    vmem(depth, Y, Z),
                    vmem((sides + 1) * depth + 2 * edge_packs, Y, Z),
                    vmem(edge_packs, Y, Z),
                    vmem(EX, Y, Z),
                    vmem((sides + 3) * EX, Y, Z),
                    vmem(COMPS, X + 1, Y, Z),
                    vmem(2, COMPS, X, Y, Z),
                    vmem(2, COMPS, X, Y, Z),
                    vmem(COMPS, X, Y, Z),
                    vmem(COMPS - SPECIES + 1, X, Y, Z),
                    dma((4,)),
                    dma((6,)),
                    pltpu.SemaphoreType.REGULAR((len(halo_links(sizes)),)),
                    pltpu.SemaphoreType.REGULAR,
                    dma(()),
                    dma((2 * len(groups),)),
                ]
                + rows_scratch,
                compiler_params=pltpu.CompilerParams(collective_id=0, has_side_effects=True),
            )(species, velocity_in, pressure_in, wall_types)
        )
        return tuple(
            pl.pallas_call(
                store,
                out_shape=[
                    jax.ShapeDtypeStruct((COMPS, X, Y, Z), jnp.float32),
                    jax.ShapeDtypeStruct((EX, EY, EZ), jnp.float32),
                ],
                in_specs=[pl.BlockSpec(memory_space=pltpu.VMEM)] * 2,
                out_specs=[pl.BlockSpec(memory_space=pltpu.HBM)] * 2,
                scratch_shapes=[pltpu.SemaphoreType.DMA((2,))],
            )(*[pltpu.with_memory_space_constraint(v, pltpu.VMEM) for v in (state, weights)])
        )

    in_specs = (
        P(None, "gx", "gy", "gz"),
        P(None, "gx", "gy", "gz"),
        P("gx", "gy", "gz"),
        P(None, "gx", "gy", "gz"),
    )
    out_specs = (P(None, "gx", "gy", "gz"), P("gx", "gy", "gz"))
    return jax.shard_map(local, mesh=mesh, in_specs=in_specs, out_specs=out_specs, check_vma=False)
```
